128 devices in a mesh: flow: 128 (over y, z, x, core).
Axes of the slice: x: 4, y: 4, z: 4, core: 2. Of those that a mesh axis runs over, the one named last changes fastest.
Arguments:
- forcing: float32 [2, 12, 3072, 1024], P(None, None, 'flow'), may hold values from -1000 to 1000
- viscosity: float32 [3072, 1024], P('flow'), may hold values from 0.5 to 4
- friction: float32 [3072, 1024], P('flow'), may hold values from 1 to 30
- rotation: float32 [3072, 1024], P('flow'), may hold values from -2 to 2
- vertical: float32 [11, 3072, 1024], P(None, 'flow'), may hold values from 2 to 20
- ice_mask: int32 [3072, 1024], P('flow'), may hold values 0 or 1
- grounded: int32 [3072, 1024], P('flow'), may hold values 0 or 1
Outputs:
- solution: float32 [2, 12, 3072, 1024], P(None, None, 'flow')
- residual: float32 [2, 12, 3072, 1024], P(None, None, 'flow')
The draws below stay inside these ranges and needn't reach their ends.
All inputs are finite; a program needn't handle non-finite values. No bound on the sum of `ice_mask` or of `grounded` on one device may be relied on, other than what follows from the above.
Results may differ from the reference program's by a relative error of at most 0.0003.
Values sent between devices are 32-bit elements; how exact they have to be, the bound alone decides.
No kernel may reach another device: no remote copies, remote signals or barrier semaphores. Data moves between devices by JAX's collectives and lax.ppermute only.
A program may use at most 192 MiB of HBM per device.

```python
import math
import jax
import jax.numpy as jnp

NY = 1024
L = 12
ITERS = 3
NX = 3072


def draw_forcing(key, part):
    noise_key = jax.random.fold_in(key, 11)
    column_key = jax.random.fold_in(key, 12)
    position = jnp.arange(NX, dtype=jnp.float32) / NX
    column_scale = jnp.exp(jax.random.uniform(column_key, (NY,), jnp.float32, 0.0, math.log(10.0)))
    noise_base = jnp.clip(jax.random.normal(noise_key, (2, L, NX, NY), jnp.float32), -5.0, 5.0)
    row_scale = 3.0 ** position
    return 4.0 * noise_base * row_scale[:, None] * column_scale[None, :]


def touch_ends(result, key, least, top_value):
    place = [jax.random.randint(jax.random.fold_in(key, axis), (), 0, length) for axis, length in enumerate(result.shape)]
    longest = result.shape.index(max(result.shape))
    neighbour = place[:longest] + [(place[longest] + 1) % result.shape[longest]] + place[longest + 1:]
    return result.at[tuple(place)].set(least).at[tuple(neighbour)].set(top_value)


def level_of(key, dims, split, smallest, largest):
    def one(dim, parts):
        steps = jax.random.uniform(jax.random.fold_in(jax.random.fold_in(key, 6), dim), (parts,), jnp.float32, smallest / len(split), largest / len(split))
        return jnp.repeat(jnp.exp(steps), dims[dim] // parts).reshape((-1,) + (1,) * (len(dims) - dim - 1))

    level = one(*split[0])
    for cut in split[1:]:
        level = level * one(*cut)
    return level


def setup_inputs(seed: int = 0) -> dict:
    arg_keys = jax.random.split(jax.random.key(seed), 8)
    forcing = draw_forcing(jax.random.fold_in(arg_keys[7], 71), 0)
    viscosity = jnp.clip(jnp.exp(math.log(4.0) - 2.0794415 * jax.random.uniform(arg_keys[1], (NX, NY), jnp.float32) ** level_of(arg_keys[1], (NX, NY), ((0, 128),), -0.2, 0.2)), 0.5, 4.0)
    friction = jnp.clip(jnp.exp(math.log(30.0) - 3.4011974 * jax.random.uniform(arg_keys[2], (NX, NY), jnp.float32) ** level_of(arg_keys[2], (NX, NY), ((0, 128),), -0.2, 0.2)), 1.0, 30.0)
    rotation = jnp.clip(jax.random.uniform(arg_keys[3], (NX, NY), jnp.float32, -2.0, 2.0) * level_of(arg_keys[3], (NX, NY), ((0, 128),), -0.4, 0.0), -2.0, 2.0)
    vertical = jnp.clip(jnp.exp(math.log(20.0) - 2.3025851 * jax.random.uniform(arg_keys[4], (L - 1, NX, NY), jnp.float32) ** level_of(arg_keys[4], (L - 1, NX, NY), ((1, 128),), -0.2, 0.2)), 2.0, 20.0)
    ice_mask = touch_ends((jax.random.randint(arg_keys[5], (NX, NY), 0, 16) < 15).astype(jnp.int32), jax.random.fold_in(arg_keys[5], 1), 0, 1)
    grounded = touch_ends((jax.random.randint(arg_keys[6], (NX, NY), 0, 4) < 3).astype(jnp.int32), jax.random.fold_in(arg_keys[6], 1), 0, 1)
    return {"forcing": forcing, "viscosity": viscosity, "friction": friction, "rotation": rotation, "vertical": vertical, "ice_mask": ice_mask, "grounded": grounded}


epsilon = 1e-06
relaxation = 0.5
reach_weights = (1.0, 0.6, 0.35, 0.2)

def layer_coefs(basal_drag, vertical):
    zero_plane = jnp.zeros_like(vertical[:1])
    upper_coef = jnp.concatenate([vertical, zero_plane], 0)
    lower_coef = jnp.concatenate([zero_plane, vertical], 0)
    bottom = jnp.concatenate([basal_drag[None], jnp.zeros_like(vertical)], 0)
    return (upper_coef, lower_coef, bottom)

def stencil_apply(padded, viscosity, basal_drag, rotation, ice_cover, vertical):
    row_count = padded.shape[2] - 8
    values = padded[:, :, 4:4 + row_count]
    horizontal = jnp.zeros_like(values)
    for order, weight in enumerate(reach_weights):
        offset = order + 1
        forward_cells = padded[:, :, 4 + offset:4 + offset + row_count]
        backward_cells = padded[:, :, 4 - offset:4 - offset + row_count]
        horizontal = horizontal + weight * (2.0 * values - forward_cells - backward_cells)
    padded_cross = jnp.pad(values, ((0, 0), (0, 0), (0, 0), (1, 1)))
    horizontal = horizontal + (2.0 * values - padded_cross[..., 2:] - padded_cross[..., :-2])
    upper_coef, lower_coef, bottom = layer_coefs(basal_drag, vertical)
    diagonal = upper_coef + lower_coef + bottom + relaxation * viscosity
    shifted_up = jnp.concatenate([values[:, 1:], jnp.zeros_like(values[:, :1])], 1)
    shifted_down = jnp.concatenate([jnp.zeros_like(values[:, :1]), values[:, :-1]], 1)
    turned = jnp.stack([values[1], -values[0]])
    stencil = diagonal * values - upper_coef * shifted_up - lower_coef * shifted_down + rotation * turned + viscosity * horizontal
    return jnp.where(ice_cover > 0.5, stencil, values)

def precondition(vector, viscosity, basal_drag, rotation, ice_cover, vertical):
    active = ice_cover > 0.5
    horiz_total = 2.0 * sum(reach_weights) + 2.0
    upper_coef, lower_coef, bottom = layer_coefs(basal_drag, vertical)
    real_part = upper_coef + lower_coef + bottom + relaxation * viscosity + horiz_total * viscosity
    real_part = jnp.where(active, real_part, jnp.ones_like(real_part))
    imag_part = jnp.where(active, rotation, jnp.zeros_like(rotation))
    coupling = jnp.where(active, vertical, jnp.zeros_like(vertical))
    layer_total = vector.shape[1]
    inv_real, inv_imag, carry_former, carry_latter = ([], [], [], [])
    for layer in range(layer_total):
        pivot_real = real_part[layer]
        pivot_imag = imag_part
        source_former = vector[0, layer]
        source_latter = vector[1, layer]
        if layer > 0:
            link = coupling[layer - 1]
            pivot_real = pivot_real - link * link * inv_real[layer - 1]
            pivot_imag = pivot_imag - link * link * inv_imag[layer - 1]
            source_former = source_former + link * carry_former[layer - 1]
            source_latter = source_latter + link * carry_latter[layer - 1]
        inverse_det = 1.0 / (pivot_real * pivot_real + pivot_imag * pivot_imag)
        entry_real = pivot_real * inverse_det
        entry_imag = -pivot_imag * inverse_det
        inv_real.append(entry_real)
        inv_imag.append(entry_imag)
        carry_former.append(entry_real * source_former + entry_imag * source_latter)
        carry_latter.append(entry_real * source_latter - entry_imag * source_former)
    result_former = [None] * layer_total
    result_latter = [None] * layer_total
    result_former[layer_total - 1] = carry_former[layer_total - 1]
    result_latter[layer_total - 1] = carry_latter[layer_total - 1]
    for layer in range(layer_total - 2, -1, -1):
        link = coupling[layer]
        pushed_former = link * result_former[layer + 1]
        pushed_latter = link * result_latter[layer + 1]
        result_former[layer] = carry_former[layer] + inv_real[layer] * pushed_former + inv_imag[layer] * pushed_latter
        result_latter[layer] = carry_latter[layer] + inv_real[layer] * pushed_latter - inv_imag[layer] * pushed_former
    solved = jnp.stack([jnp.stack(result_former), jnp.stack(result_latter)])
    return jnp.where(active, solved, vector)

def least_squares(columns, start):
    count_cols = len(columns)
    givens_rhs = [start] + [start * 0.0 for index in range(count_cols)]
    cosines, sines, upper_cols = ([], [], [])
    for column_index, column_in in enumerate(columns):
        column = list(column_in)
        for row_index in range(column_index):
            rotated_a = cosines[row_index] * column[row_index] + sines[row_index] * column[row_index + 1]
            rotated_b = -sines[row_index] * column[row_index] + cosines[row_index] * column[row_index + 1]
            column[row_index] = rotated_a
            column[row_index + 1] = rotated_b
        radius = jnp.sqrt(column[column_index] * column[column_index] + column[column_index + 1] * column[column_index + 1])
        cosine = column[column_index] / radius
        sine_value = column[column_index + 1] / radius
        column[column_index] = radius
        cosines.append(cosine)
        sines.append(sine_value)
        upper_cols.append(column)
        next_rhs = -sine_value * givens_rhs[column_index]
        givens_rhs[column_index] = cosine * givens_rhs[column_index]
        givens_rhs[column_index + 1] = next_rhs
    factors = [None] * count_cols
    for column_index in range(count_cols - 1, -1, -1):
        accum = givens_rhs[column_index]
        for later in range(column_index + 1, count_cols):
            accum = accum - upper_cols[later][column_index] * factors[later]
        factors[column_index] = accum / upper_cols[column_index][column_index]
    return factors

def operate(values, coefs):
    padded = jnp.pad(values, ((0, 0), (0, 0), (4, 4), (0, 0)))
    return stencil_apply(padded, *coefs)

def reference(forcing, viscosity, friction, rotation, vertical, ice_mask, grounded):
    ice_cover = jnp.where(ice_mask > 0, jnp.ones_like(viscosity), jnp.zeros_like(viscosity))
    basal_drag = jnp.where(grounded > 0, friction, jnp.zeros_like(friction))
    coefs = (viscosity, basal_drag, rotation, ice_cover, vertical)
    load_norm = jnp.sqrt(jnp.sum(forcing * forcing) + epsilon)
    krylov = [forcing / load_norm]
    searches = []
    columns = []
    for iteration in range(ITERS):
        search = precondition(krylov[iteration], *coefs)
        searches.append(search)
        image = operate(search, coefs)
        column = []
        for vector in krylov:
            weight_now = jnp.sum(image * vector)
            image = image - weight_now * vector
            column.append(weight_now)
        new_norm = jnp.sqrt(jnp.sum(image * image) + epsilon)
        column.append(new_norm)
        columns.append(column)
        if iteration + 1 < ITERS:
            krylov.append(image / new_norm)
    factors = least_squares(columns, load_norm)
    solution = factors[0] * searches[0]
    for index in range(1, ITERS):
        solution = solution + factors[index] * searches[index]
    residual = forcing - operate(solution, coefs)
    return (solution, residual)
```

```python
import jax
import jax.numpy as jnp
from jax import lax
from jax.experimental import pallas as pl
from jax.experimental.pallas import tpu as pltpu
from jax.sharding import Mesh
from jax.sharding import PartitionSpec as P


FLOW = ("flow_0", "flow_1", "flow_2", "flow_3")
CORE = "flow_3"
epsilon = 1e-06
relaxation = 0.5
reach_weights = (1.0, 0.6, 0.35, 0.2)
horiz_total = 2.0 * sum(reach_weights) + 2.0

L = 12
ROWS = 24
REACH = 4
EDGE = 2 * REACH
INNER = ROWS - EDGE
F32 = jnp.float32
TILE = (8, 128)

VM = pl.BlockSpec(memory_space=pltpu.VMEM)
HB = pl.BlockSpec(memory_space=pltpu.HBM)


def vmem(*lead):
    return pltpu.VMEM((*lead, *TILE), F32)


def edge_order(index):
    return index if index < REACH else ROWS - 1 - (index - REACH)


def place_of(core, t):
    tile, sub = t // 8, t % 8
    return (
        jnp.where(core == 1, tile, 2 - tile),
        jnp.where(core == 1, sub, 7 - sub),
    )


def row(ref, plane, place):
    tile, sub = place
    return ref[plane, tile, pl.ds(sub, 8, stride=8), :]


def rows(ref, plane, places):
    return jnp.stack([row(ref, plane, place) for place in places])


def factor(places, raws, inv_real, inv_imag, link_out, nu_out, start):
    vraw, nuraw, fricraw, rotraw, iceraw, groundraw = raws
    span = pl.ds(start, len(places))
    active = rows(iceraw, 0, places) > 0
    nu = rows(nuraw, 0, places)
    drag = jnp.where(rows(groundraw, 0, places) > 0, rows(fricraw, 0, places), 0.0)
    imag = jnp.where(active, rows(rotraw, 0, places), 0.0)
    base = (relaxation + horiz_total) * nu
    nu_out[span] = jnp.where(active, nu, 0.0)
    below = None
    for k in range(L):
        real = base
        if k == 0:
            real = real + drag
        else:
            real = real + below
        if k < L - 1:
            above = rows(vraw, k, places)
            real = real + above
        real = jnp.where(active, real, 1.0)
        pivot_imag = imag
        if k > 0:
            link = jnp.where(active, below, 0.0)
            link_out[k - 1, span] = link
            square = link * link
            real = real - square * er
            pivot_imag = imag - square * ei
        inverse = 1.0 / (real * real + pivot_imag * pivot_imag)
        er = real * inverse
        ei = -(pivot_imag * inverse)
        inv_real[k, span] = er
        inv_imag[k, span] = ei
        if k < L - 1:
            below = above


def solve(source, inv_real, inv_imag, link, span, put, get):
    cf = cg = None
    for k in range(L):
        sf, sg = source(k), source(L + k)
        if k > 0:
            ln = link[k - 1, span]
            sf = sf + ln * cf
            sg = sg + ln * cg
        er, ei = inv_real[k, span], inv_imag[k, span]
        cf, cg = er * sf + ei * sg, er * sg - ei * sf
        put(k, cf)
        put(L + k, cg)
    xf, xg = cf, cg
    for k in range(L - 2, -1, -1):
        ln = link[k, span]
        pf, pg = ln * xf, ln * xg
        er, ei = inv_real[k, span], inv_imag[k, span]
        xf = get(k) + (er * pf + ei * pg)
        xg = get(L + k) + (er * pg - ei * pf)
        put(k, xf)
        put(L + k, xg)


def edge_put(sa, sb):
    def put(plane, value):
        sa[plane] = value[:REACH]
        sb[plane] = value[REACH:]

    def get(plane):
        return jnp.concatenate([sa[plane], sb[plane]], 0)

    return put, get


def lanes():
    return lax.broadcasted_iota(jnp.int32, TILE, 1)


def cross(s, masks):
    first, last, first_end, last_end = masks
    up = jnp.where(first, pltpu.roll(s, 7, 0), s)
    up = jnp.where(first_end, 0.0, up)
    down = jnp.where(last, pltpu.roll(s, 1, 0), s)
    down = jnp.where(last_end, 0.0, down)
    return pltpu.roll(up, 127, 1) + pltpu.roll(down, 1, 1)


def cross_masks():
    lane = lanes()
    sub = lax.broadcasted_iota(jnp.int32, TILE, 0)
    first, last = lane == 0, lane == 127
    return first, last, first & (sub == 7), last & (sub == 0)


def apply_stencil(sa, sb, si, nu_i, u_edges, u_inners, u_new, nsum, extra=None):
    masks = cross_masks()
    count = len(u_inners)
    pairs = count + 1
    zero = jnp.zeros(TILE, F32)

    def step(plane, sums):
        sums = list(sums)
        s = (
            [sa[plane, d] for d in range(REACH)]
            + [si[plane, d] for d in range(INNER)]
            + [sb[plane, REACH - 1 - d] for d in range(REACH)]
        )
        for t in range(ROWS):
            total = cross(s[t], masks)
            for m in range(1, REACH + 1):
                weight = reach_weights[m - 1]
                near = [s[q] for q in (t - m, t + m) if 0 <= q < ROWS]
                both = near[0] + near[1] if len(near) == 2 else near[0]
                total = total + (both if weight == 1.0 else weight * both)
            if REACH <= t < ROWS - REACH:
                i = t - REACH
                new = nu_i[i] * total
                u_new[plane, i] = new
                for a in range(count):
                    sums[a] = sums[a] + new * u_inners[a][plane, i]
                sums[count] = sums[count] + new * new
            else:
                nsum[plane, t if t < REACH else REACH + ROWS - 1 - t] = total
        for e in range(EDGE):
            now = u_edges[-1][plane, e]
            for a in range(count):
                other = now if a == count - 1 else u_edges[a][plane, e]
                sums[pairs + a] = sums[pairs + a] + now * other
        if extra is not None:
            for i in range(INNER):
                now = u_inners[0][plane, i]
                sums[pairs + count] = sums[pairs + count] + now * now
        return tuple(sums)

    size = pairs + count + (extra is not None)
    return lax.fori_loop(0, 2 * L, step, (zero,) * size)


def first_edge_kernel(f, v, nu, fric, rot, ice, ground, *rest):
    (inv_real, inv_imag, link, nu_e, sa, sb) = rest[:6]
    raws = rest[6:13]
    sems = rest[13]
    fraw, vraw = raws[0], raws[1]
    small = [
        pltpu.make_async_copy(src, dst, sems.at[i])
        for i, (src, dst) in enumerate(zip((nu, fric, rot, ice, ground), raws[2:]))
    ]
    v_edge = [pltpu.make_async_copy(v.at[:, i], vraw.at[:, i], sems.at[5 + i]) for i in (0, 2)]
    f_edge = [pltpu.make_async_copy(f.at[:, i], fraw.at[:, i], sems.at[8 + i]) for i in (0, 2)]
    middle = [
        pltpu.make_async_copy(v.at[:, 1], vraw.at[:, 1], sems.at[6]),
        pltpu.make_async_copy(f.at[:, 1], fraw.at[:, 1], sems.at[9]),
    ]
    for copy in small + v_edge + f_edge + middle:
        copy.start()
    core = lax.axis_index(CORE)
    places = [place_of(core, edge_order(e)) for e in range(EDGE)]
    for copy in small + v_edge:
        copy.wait()
    factor(places, raws[1:], inv_real, inv_imag, link, nu_e, 0)
    for copy in f_edge:
        copy.wait()
    put, get = edge_put(sa, sb)
    span = pl.ds(0, EDGE)
    solve(lambda plane: rows(fraw, plane, places), inv_real, inv_imag, link, span, put, get)
    for copy in middle:
        copy.wait()


def first_inner_kernel(fraw, vraw, nuraw, fricraw, rotraw, iceraw, groundraw, sa, sb, *rest):
    (inv_real, inv_imag, link, nu_i, si, f_e, f_i, u_new, nsum, sums_out) = rest
    raws = (vraw, nuraw, fricraw, rotraw, iceraw, groundraw)
    core = lax.axis_index(CORE)
    edge_places = [place_of(core, edge_order(e)) for e in range(EDGE)]
    places = [place_of(core, REACH + i) for i in range(INNER)]

    def spread(plane, carry):
        for e in range(EDGE):
            f_e[plane, e] = row(fraw, plane, edge_places[e])
        for i in range(INNER):
            f_i[plane, i] = row(fraw, plane, places[i])
        return carry

    lax.fori_loop(0, 2 * L, spread, 0)
    for start in (0, 8):
        factor(places[start : start + 8], raws, inv_real, inv_imag, link, nu_i, start)
    inner_solve(f_i, inv_real, inv_imag, link, si)
    sums = apply_stencil(sa, sb, si, nu_i, [f_e], [f_i], u_new, nsum, extra=True)
    for a, value in enumerate(sums):
        sums_out[a] = value


def inner_solve(u_i, inv_real, inv_imag, link, si):
    def batch(b, carry):
        span = pl.ds(b * 8, 8)

        def put(plane, value):
            si[plane, span] = value

        solve(
            lambda plane: u_i[plane, span],
            inv_real,
            inv_imag,
            link,
            span,
            put,
            lambda plane: si[plane, span],
        )
        return carry

    lax.fori_loop(0, INNER // 8, batch, 0)


def edge_source(halo, nsum, nu_e):
    def of_side(plane, side):
        parts = []
        for d in range(REACH):
            total = nsum[plane, side * REACH + d]
            for q in range(1, REACH + 1 - d):
                weight = reach_weights[d + q - 1]
                value = halo[side][plane, q - 1]
                total = total + (value if weight == 1.0 else weight * value)
            parts.append(nu_e[side * REACH + d] * total)
        return parts

    return lambda plane: jnp.stack(of_side(plane, 0) + of_side(plane, 1))


def edge_kernel(ha, hb, nsum, nu_e, inv_real, inv_imag, link, u_e, sa, sb):
    finish = edge_source((ha, hb), nsum, nu_e)

    def source(plane):
        value = finish(plane)
        u_e[plane] = value
        return value

    put, get = edge_put(sa, sb)
    solve(source, inv_real, inv_imag, link, pl.ds(0, EDGE), put, get)


def inner_kernel(order, *refs):
    sa, sb, inv_real, inv_imag, link, nu_i = refs[:6]
    u_edges = refs[6 : 7 + order]
    u_inners = refs[7 + order : 8 + 2 * order]
    si, u_new, nsum, sums_out = refs[8 + 2 * order :]
    inner_solve(u_inners[-1], inv_real, inv_imag, link, si)
    sums = apply_stencil(sa, sb, si, nu_i, u_edges, u_inners, u_new, nsum)
    for a, value in enumerate(sums):
        sums_out[a] = value


GRAM = [(a, b) for b in range(4) for a in range(b + 1)]


def last_edge_kernel(ha, hb, nsum, nu_e, u0, u1, u2, s0, s1, s2, u_e, payload):
    finish = edge_source((ha, hb), nsum, nu_e)
    zero = jnp.zeros(TILE, F32)

    def step(plane, sums):
        sums = list(sums)
        value = finish(plane)
        u_e[plane] = value
        for a, ref in enumerate((u0, u1, u2)):
            other = ref[plane]
            for e in range(EDGE):
                sums[a] = sums[a] + value[e] * other[e]
        for e in range(EDGE):
            sums[3] = sums[3] + value[e] * value[e]
        return tuple(sums)

    last = lax.fori_loop(0, 2 * L, step, (zero,) * 4)
    gram = {
        (0, 0): s0[2] + s0[3],
        (0, 1): s0[0] + s1[3],
        (1, 1): s0[1] + s1[4],
        (0, 2): s1[0] + s2[4],
        (1, 2): s1[1] + s2[5],
        (2, 2): s1[2] + s2[6],
        (0, 3): s2[0] + last[0],
        (1, 3): s2[1] + last[1],
        (2, 3): s2[2] + last[2],
        (3, 3): s2[3] + last[3],
    }
    lane = lanes()
    out = zero
    for i, pair in enumerate(GRAM):
        value = jnp.sum(jnp.sum(gram[pair], axis=0, keepdims=True), axis=1, keepdims=True)
        out = out + jnp.where(lane == i, value, 0.0)
    for r in range(payload.shape[0] // 8):
        payload[pl.ds(8 * r, 8), :] = out


def least_squares(columns, start):
    count_cols = len(columns)
    givens_rhs = [start] + [start * 0.0 for index in range(count_cols)]
    cosines, sines, upper_cols = ([], [], [])
    for column_index, column_in in enumerate(columns):
        column = list(column_in)
        for row_index in range(column_index):
            rotated_a = (
                cosines[row_index] * column[row_index] + sines[row_index] * column[row_index + 1]
            )
            rotated_b = (
                -sines[row_index] * column[row_index] + cosines[row_index] * column[row_index + 1]
            )
            column[row_index] = rotated_a
            column[row_index + 1] = rotated_b
        radius = jnp.sqrt(
            column[column_index] * column[column_index]
            + column[column_index + 1] * column[column_index + 1]
        )
        inverse = 1.0 / radius
        cosine = column[column_index] * inverse
        sine_value = column[column_index + 1] * inverse
        column[column_index] = inverse
        cosines.append(cosine)
        sines.append(sine_value)
        upper_cols.append(column)
        next_rhs = -sine_value * givens_rhs[column_index]
        givens_rhs[column_index] = cosine * givens_rhs[column_index]
        givens_rhs[column_index + 1] = next_rhs
    factors = [None] * count_cols
    for column_index in range(count_cols - 1, -1, -1):
        accum = givens_rhs[column_index]
        for later in range(column_index + 1, count_cols):
            accum = accum - upper_cols[later][column_index] * factors[later]
        factors[column_index] = accum * upper_cols[column_index][column_index]
    return factors


def dot(left, right):
    total = left[0] * right[0]
    for a, b in zip(left[1:], right[1:]):
        total = total + a * b
    return total


def coefficients(gram):
    size = 4
    upper = {}
    for a in range(size):
        square = gram[(a, a)]
        for p in range(a):
            square = square - upper[(p, a)] * upper[(p, a)]
        square = jnp.maximum(square, 0.0)
        length = jnp.sqrt(square)
        inverse = jnp.where(length > 0.0, 1.0 / jnp.where(length > 0.0, length, 1.0), 0.0)
        upper[(a, a)] = length
        for b in range(a + 1, size):
            value = gram[(a, b)]
            for p in range(a):
                value = value - upper[(p, a)] * upper[(p, b)]
            upper[(a, b)] = value * inverse
    beta = jnp.sqrt(gram[(0, 0)] + epsilon)
    inverse = 1.0 / beta
    basis = [[inverse]]
    ortho = [[upper[(0, 0)] * inverse]]
    columns = []
    for j in range(3):
        current = basis[j]
        w = [current[0]]
        for i in range(1, j + 1):
            w.append(current[i] - current[i - 1])
        w.append(-current[j])
        q = [dot([upper[(i, m)] for m in range(i, j + 2)], w[i:]) for i in range(j + 2)]
        column = []
        for i in range(j + 1):
            h = dot(q[: i + 1], ortho[i])
            for m in range(i + 1):
                q[m] = q[m] - h * ortho[i][m]
                w[m] = w[m] - h * basis[i][m]
            column.append(h)
        length = jnp.sqrt(dot(q, q) + epsilon)
        column.append(length)
        columns.append(column)
        if j < 2:
            inverse = 1.0 / length
            basis.append([value * inverse for value in w])
            ortho.append([value * inverse for value in q])
    y = least_squares(columns, beta)
    return [dot(y[i:], [basis[j][i] for j in range(i, 3)]) for i in range(3)]


def final_kernel(gathered, *refs):
    u_edges, u_inners = refs[0:4], refs[4:8]
    sas, sbs, sis = refs[8:11], refs[11:14], refs[14:17]
    out_s, out_r, buf_s, buf_r, sem_s, sem_r = refs[17:]
    total = gathered[pl.ds(0, 8), :]
    for r in range(1, gathered.shape[0] // 8):
        total = total + gathered[pl.ds(8 * r, 8), :]
    total = jnp.sum(total, axis=0, keepdims=True)
    total = jnp.broadcast_to(total, TILE)
    lane = lanes()
    gram = {}
    for i, pair in enumerate(GRAM):
        value = jnp.sum(jnp.where(lane == i, total, 0.0), axis=1, keepdims=True)
        gram[pair] = jnp.broadcast_to(value, TILE)
    c0, c1, c2 = coefficients(gram)
    e0, e1, e2 = 1.0 - c0, c0 - c1, c1 - c2
    core = lax.axis_index(CORE)
    places = [place_of(core, t) for t in range(ROWS)]

    def copies(plane):
        return (
            pltpu.make_async_copy(buf_s.at[plane], out_s.at[plane], sem_s),
            pltpu.make_async_copy(buf_r.at[plane], out_r.at[plane], sem_r),
        )

    def step(plane, carry):
        for t in range(ROWS):
            if t < REACH:
                s = [ref[plane, t] for ref in sas]
                u = [ref[plane, t] for ref in u_edges]
            elif t < ROWS - REACH:
                s = [ref[plane, t - REACH] for ref in sis]
                u = [ref[plane, t - REACH] for ref in u_inners]
            else:
                s = [ref[plane, ROWS - 1 - t] for ref in sbs]
                u = [ref[plane, REACH + ROWS - 1 - t] for ref in u_edges]
            tile, sub = places[t]
            buf_s[plane, tile, pl.ds(sub, 8, stride=8), :] = c0 * s[0] + c1 * s[1] + c2 * s[2]
            buf_r[plane, tile, pl.ds(sub, 8, stride=8), :] = (
                e0 * u[0] + e1 * u[1] + (e2 * u[2] + c2 * u[3])
            )
        for copy in copies(plane):
            copy.start()
        return carry

    lax.fori_loop(0, 2 * L, step, 0)
    pltpu.make_async_copy(buf_s, out_s, sem_s).wait()
    pltpu.make_async_copy(buf_r, out_r, sem_r).wait()


def tiled(x):
    x = x.reshape(-1, ROWS // 8, 8, 8, 128)
    return x.transpose(0, 1, 3, 2, 4).reshape(-1, ROWS // 8, 64, 128)


def untiled(x):
    x = x.reshape(2 * L, ROWS // 8, 8, 8, 128).transpose(0, 1, 3, 2, 4)
    return x.reshape(2, L, ROWS, 1024)


def call(kernel, name, out_shape, args, in_specs=None, out_specs=None, scratch=(), limit=None):
    return pl.pallas_call(
        kernel,
        out_shape=out_shape,
        in_specs=in_specs or [VM] * len(args),
        out_specs=out_specs or [VM] * len(out_shape),
        scratch_shapes=scratch,
        compiler_params=pltpu.CompilerParams(vmem_limit_bytes=limit or (4 << 20)),
        name=name,
    )(*args)


def exchange(sa, sb):
    count = 128
    across = [(i, i + 1) for i in range(1, count - 1, 2)]
    across = across + [(b, a) for a, b in across]
    within = [(i, i ^ 1) for i in range(count)]
    hb = lax.ppermute(sb, FLOW, across)
    ha = lax.ppermute(sa, FLOW, within)
    return ha, hb


def body(forcing, viscosity, friction, rotation, vertical, ice_mask, grounded):
    raw = [tiled(x) for x in (forcing, vertical, viscosity, friction, rotation, ice_mask, grounded)]
    raw = [pltpu.with_memory_space_constraint(x, pltpu.HBM) for x in raw]
    planes = 2 * L

    def rawtype(x):
        return pltpu.VMEM(x.shape, x.dtype)

    out = call(
        first_edge_kernel,
        "edge0",
        [vmem(L, EDGE), vmem(L, EDGE), vmem(L - 1, EDGE), vmem(EDGE)]
        + [vmem(planes, REACH)] * 2
        + [rawtype(x) for x in raw],
        raw,
        in_specs=[HB] * 7,
        scratch=[pltpu.SemaphoreType.DMA((11,))],
    )
    ier, iei, ie_link, nu_e, sa, sb = out[:6]
    sas, sbs, sis = [sa], [sb], []
    inner_vec = vmem(planes, INNER)
    edge_vec = vmem(planes, EDGE)
    halo = exchange(sa, sb)
    ir, ii, i_link, nu_i, si, f_e, f_i, u_i, nsum, sums = call(
        first_inner_kernel,
        "inner0",
        [vmem(L, INNER), vmem(L, INNER), vmem(L - 1, INNER), vmem(INNER)]
        + [inner_vec, edge_vec, inner_vec, inner_vec, edge_vec, vmem(4)],
        list(out[6:]) + [sa, sb],
    )
    sis.append(si)
    u_edges, u_inners, all_sums = [f_e], [f_i, u_i], [sums]
    for order in (1, 2):
        u_e, sa, sb = call(
            edge_kernel,
            f"edge{order}",
            [edge_vec] + [vmem(planes, REACH)] * 2,
            [*halo, nsum, nu_e, ier, iei, ie_link],
        )
        u_edges.append(u_e)
        sas.append(sa)
        sbs.append(sb)
        halo = exchange(sa, sb)

        def kernel(*refs, order=order):
            inner_kernel(order, *refs)

        si, u_i, nsum, sums = call(
            kernel,
            f"inner{order}",
            [inner_vec, inner_vec, edge_vec, vmem(2 * order + 3)],
            [sa, sb, ir, ii, i_link, nu_i, *u_edges, *u_inners],
        )
        sis.append(si)
        u_inners.append(u_i)
        all_sums.append(sums)
    u_e, payload = call(
        last_edge_kernel,
        "edge3",
        [edge_vec, jax.ShapeDtypeStruct((128, 128), F32)],
        [*halo, nsum, nu_e, *u_edges, *all_sums],
    )
    u_edges.append(u_e)
    gathered = lax.all_to_all(payload, FLOW, split_axis=0, concat_axis=0, tiled=True)
    shape = (planes, ROWS // 8, 64, 128)
    outs = call(
        final_kernel,
        "combine",
        [jax.ShapeDtypeStruct(shape, F32)] * 2,
        [gathered, *u_edges, *u_inners, *sas, *sbs, *sis],
        out_specs=[HB] * 2,
        scratch=[pltpu.VMEM(shape, F32)] * 2 + [pltpu.SemaphoreType.DMA] * 2,
        limit=8 << 20,
    )
    return untiled(outs[0]), untiled(outs[1])


def solution(mesh):
    finer = Mesh(mesh.devices.reshape(4, 4, 4, 2), FLOW)
    return jax.shard_map(
        body,
        mesh=finer,
        in_specs=(
            P(None, None, FLOW, None),
            P(FLOW, None),
            P(FLOW, None),
            P(FLOW, None),
            P(None, FLOW, None),
            P(FLOW, None),
            P(FLOW, None),
        ),
        out_specs=(P(None, None, FLOW, None), P(None, None, FLOW, None)),
        check_vma=False,
    )
```

```python
import jax
import jax.numpy as jnp
from jax import lax
from jax.experimental import pallas as pl
from jax.experimental.pallas import tpu as pltpu
from jax.sharding import Mesh
from jax.sharding import PartitionSpec as P


FLOW = ("flow_0", "flow_1", "flow_2", "flow_3")
CORE = "flow_3"
epsilon = 1e-06
relaxation = 0.5
reach_weights = (1.0, 0.6, 0.35, 0.2)
horiz_total = 2.0 * sum(reach_weights) + 2.0

L = 12
PLANES = 2 * L
ROWS = 24
REACH = 4
HALF = 12
F32 = jnp.float32
TILE = (8, 128)
GRAM = [(a, b) for b in range(4) for a in range(b + 1)]

VM = pl.BlockSpec(memory_space=pltpu.VMEM)
HB = pl.BlockSpec(memory_space=pltpu.HBM)


def vmem(*lead):
    return pltpu.VMEM((*lead, *TILE), F32)


def span(start, stop):
    return list(range(start, stop))


def place_of(core, t):
    tile, sub = t // 8, t % 8
    return (
        jnp.where(core == 1, tile, 2 - tile),
        jnp.where(core == 1, sub, 7 - sub),
    )


def raw_row(ref, plane, place):
    tile, sub = place
    return ref[plane, tile, pl.ds(sub, 8, stride=8), :]


class Field:
    def __init__(self, *parts):
        self.parts = parts

    def find(self, t):
        for ref, first, index in self.parts:
            if t in index:
                return ref, first, index[t]
        raise KeyError(t)

    def row(self, plane, t):
        ref, first, i = self.find(t)
        return ref[first + plane, i]

    def get(self, plane, ts):
        return jnp.stack([self.row(plane, t) for t in ts])

    def put(self, plane, ts, value):
        for i, t in enumerate(ts):
            ref, first, j = self.find(t)
            ref[first + plane, j] = value[i]


def part(ref, start, stop, first=0):
    return (ref, first, {t: t - start for t in range(start, stop)})


def mirrored(ref, start, stop, first=0):
    return (ref, first, {ROWS - 1 - d: d - start for d in range(start, stop)})


def factor(ts, read, inv_real, inv_imag, link, nu_out):
    vert, active, nu, drag, rot = read
    imag = jnp.where(active, rot, 0.0)
    base = (relaxation + horiz_total) * nu
    if nu_out is not None:
        nu_out.put(0, ts, jnp.where(active, nu, 0.0))
    below = er = ei = None
    for k in range(L):
        real = base + (drag if k == 0 else below)
        if k < L - 1:
            above = vert(k)
            real = real + above
        real = jnp.where(active, real, 1.0)
        pivot_imag = imag
        if k > 0:
            ln = jnp.where(active, below, 0.0)
            link.put(k - 1, ts, ln)
            square = ln * ln
            real = real - square * er
            pivot_imag = imag - square * ei
        inverse = 1.0 / (real * real + pivot_imag * pivot_imag)
        er = real * inverse
        ei = -(pivot_imag * inverse)
        inv_real.put(k, ts, er)
        inv_imag.put(k, ts, ei)
        if k < L - 1:
            below = above


def solve(ts, source, inv_real, inv_imag, link, result, also=None):
    cf = cg = None
    for k in range(L):
        sf, sg = source(k, ts), source(L + k, ts)
        if k > 0:
            ln = link.get(k - 1, ts)
            sf = sf + ln * cf
            sg = sg + ln * cg
        er, ei = inv_real.get(k, ts), inv_imag.get(k, ts)
        cf, cg = er * sf + ei * sg, er * sg - ei * sf
        result.put(k, ts, cf)
        result.put(L + k, ts, cg)
    xf, xg = cf, cg
    for k in range(L - 1, -1, -1):
        if k < L - 1:
            ln = link.get(k, ts)
            pf, pg = ln * xf, ln * xg
            er, ei = inv_real.get(k, ts), inv_imag.get(k, ts)
            xf = result.get(k, ts) + (er * pf + ei * pg)
            xg = result.get(L + k, ts) + (er * pg - ei * pf)
            result.put(k, ts, xf)
            result.put(L + k, ts, xg)
        if also is not None:
            copy, rows = also
            for i, t in enumerate(ts):
                if t in rows:
                    copy.put(k, [t], xf[i : i + 1])
                    copy.put(L + k, [t], xg[i : i + 1])


def lanes():
    return lax.broadcasted_iota(jnp.int32, TILE, 1)


def cross_masks():
    lane = lanes()
    sub = lax.broadcasted_iota(jnp.int32, TILE, 0)
    first, last = lane == 0, lane == 127
    return first, last, first & (sub == 7), last & (sub == 0)


def cross(s, masks):
    first, last, first_end, last_end = masks
    up = jnp.where(first, pltpu.roll(s, 7, 0), s)
    up = jnp.where(first_end, 0.0, up)
    down = jnp.where(last, pltpu.roll(s, 1, 0), s)
    down = jnp.where(last_end, 0.0, down)
    return pltpu.roll(up, 127, 1) + pltpu.roll(down, 1, 1)


def stencil(ts, known, s, masks):
    for t in ts:
        total = cross(s[t], masks)
        for m in range(1, REACH + 1):
            near = [s[q] for q in (t - m, t + m) if q in known]
            if near:
                both = near[0] + near[1] if len(near) == 2 else near[0]
                weight = reach_weights[m - 1]
                total = total + (both if weight == 1.0 else weight * both)
        yield t, total


def halo_sum(total, distance, halo):
    for q in range(1, REACH + 1 - distance):
        weight = reach_weights[distance + q - 1]
        value = halo(q - 1)
        total = total + (value if weight == 1.0 else weight * value)
    return total


def loop_sums(pairs, step):
    pairs = list(pairs)

    def run(plane, carry):
        sums = dict(zip(pairs, carry))

        def add(pair, value):
            sums[pair] = sums[pair] + value

        step(plane, add)
        return tuple(sums[pair] for pair in pairs)

    zero = jnp.zeros(TILE, F32)
    return dict(zip(pairs, lax.fori_loop(0, PLANES, run, (zero,) * len(pairs))))


def with_all(add, b, value, plane, t, us):
    for a in range(b):
        add((a, b), value * us[a].row(plane, t))
    add((b, b), value * value)


def pairs_of(*bs):
    return [(a, b) for a, b in GRAM if b in bs]


def raw_reader(r, core, ts):
    places = [place_of(core, t) for t in ts]

    def rows(ref, plane):
        return jnp.stack([raw_row(ref, plane, place) for place in places])

    active = rows(r.iceraw, 0) > 0
    drag = jnp.where(rows(r.groundraw, 0) > 0, rows(r.fricraw, 0), 0.0)
    return (
        lambda k: rows(r.vraw, k),
        active,
        rows(r.nuraw, 0),
        drag,
        rows(r.rotraw, 0),
    )


def raw_source(fraw, core):
    return lambda plane, ts: jnp.stack([raw_row(fraw, plane, place_of(core, t)) for t in ts])


def load_kernel(r):
    core = lax.axis_index(CORE)
    edge = jnp.where(core == 1, 2, 0)
    small = [
        pltpu.make_async_copy(getattr(r, n), getattr(r, n + "raw"), r.sems.at[i])
        for i, n in enumerate(("nu", "fric", "rot", "ice", "ground"))
    ]
    v_copy = [
        pltpu.make_async_copy(r.v.at[:, tile], r.vraw.at[:, tile], r.sems.at[5 + i])
        for i, tile in enumerate((edge, 1, 2 - edge))
    ]
    f_copy = [
        pltpu.make_async_copy(r.f.at[:, tile], r.fraw.at[:, tile], r.sems.at[8 + i])
        for i, tile in enumerate((edge, 1, 2 - edge))
    ]
    for copy in small + v_copy[:2] + f_copy[:2] + [v_copy[2], f_copy[2]]:
        copy.start()
    for copy in small + v_copy[:2]:
        copy.wait()
    er, ei, link, nu = (Field(part(x, HALF, ROWS)) for x in (r.er, r.ei, r.link, r.nuh))
    packed = Field(mirrored(r.p1, 0, REACH))
    for start in (12, 18):
        ts = span(start, start + 6)
        read = raw_reader(r, core, ts)
        factor(ts, read, er, ei, link, nu)
        vert, active, nu_row, drag, rot = read
        for i, t in enumerate(ts):
            if t >= ROWS - REACH:
                for k in range(L - 1):
                    packed.put(PLANES + k, [t], vert(k)[i : i + 1])
                packed.put(PLANES + L - 1, [t], jnp.where(active, nu_row, 0.0)[i : i + 1])
                packed.put(PLANES + L, [t], drag[i : i + 1])
                packed.put(PLANES + L + 1, [t], rot[i : i + 1])
    for copy in f_copy[:2]:
        copy.wait()
    source = raw_source(r.fraw, core)
    s0 = Field(part(r.s0, HALF, ROWS))
    for start in (12, 18):
        ts = span(start, start + 6)
        solve(ts, source, er, ei, link, s0, (packed, span(ROWS - REACH, ROWS)))
    v_copy[2].wait()
    f_copy[2].wait()


def ahead_kernel(r):
    masks = cross_masks()
    s0 = Field(part(r.s0, HALF, ROWS))
    nu = Field(part(r.nuh, HALF, ROWS))
    sums = Field(mirrored(r.p2, 0, REACH))
    known = span(HALF, ROWS)
    u1 = Field(part(r.u1, 16, 20))

    def step(plane, carry):
        s = {t: s0.row(plane, t) for t in known}
        for t, total in stencil(span(16, 24), known, s, masks):
            if t < 20:
                u1.put(plane, [t], (nu.row(0, t) * total)[None])
            else:
                sums.put(plane, [t], total[None])
        return carry

    lax.fori_loop(0, PLANES, step, 0)
    er, ei, link = (Field(part(x, HALF, ROWS)) for x in (r.er, r.ei, r.link))
    packed = Field(mirrored(r.p2, REACH, 2 * REACH, PLANES))
    solve(span(16, 20), u1.get, er, ei, link, Field(part(r.s1, 16, 20)), (packed, span(16, 20)))


def rest_kernel(r):
    core = lax.axis_index(CORE)
    er, ei, link, nu = (Field(part(x, 0, HALF)) for x in (r.er, r.ei, r.link, r.nuh))
    for start in (0, 6):
        ts = span(start, start + 6)
        factor(ts, raw_reader(r, core, ts), er, ei, link, nu)
    places = [place_of(core, t) for t in range(ROWS)]

    def spread(plane, carry):
        for t in range(ROWS):
            r.u0[plane, t] = raw_row(r.fraw, plane, places[t])
        return carry

    lax.fori_loop(0, PLANES, spread, 0)
    u0 = Field(part(r.u0, 0, ROWS))
    s0 = Field(part(r.s0, 0, HALF))
    for start in (0, 6):
        solve(span(start, start + 6), u0.get, er, ei, link, s0, (Field(part(r.sa, 0, REACH)), span(0, REACH)))


def both_halves(r, name):
    return Field(part(getattr(r, name + "_a"), 0, HALF), part(getattr(r, name + "_b"), HALF, ROWS))


def inner1_kernel(r):
    masks = cross_masks()
    s0, nu = both_halves(r, "s0"), both_halves(r, "nuh")
    known = span(0, 20)

    def step(plane, carry):
        s = {t: s0.row(plane, t) for t in known}
        for t, total in stencil(span(0, 16), known, s, masks):
            if t < REACH:
                r.nsum[plane, t] = total
            else:
                r.u1[plane, t - REACH] = nu.row(0, t) * total
        return carry

    lax.fori_loop(0, PLANES, step, 0)


def edge_a_kernel(r):
    nu = Field(part(r.nuh_a, 0, HALF))
    er, ei, link = (both_halves(r, n) for n in ("er", "ei", "link"))
    edge = Field(part(r.u_edge, 0, REACH))
    inner = Field(part(r.u_in, REACH, 16))

    def source(plane, ts):
        rows = []
        for t in ts:
            if t < REACH:
                value = halo_sum(r.nsum[plane, t], t, lambda q: r.ha[plane, q])
                value = nu.row(0, t) * value
                edge.put(plane, [t], value[None])
            else:
                value = inner.row(plane, t)
            rows.append(value)
        return jnp.stack(rows)

    result = Field(part(r.s, 0, 16))
    sa = Field(part(r.sa, 0, REACH))
    for start in (0, 8):
        solve(span(start, start + 8), source, er, ei, link, result, (sa, span(0, REACH)))


def write_sums(ref, sums):
    zero = jnp.zeros(TILE, F32)
    for i, pair in enumerate(GRAM):
        ref[i] = sums.get(pair, zero)


def inner2_kernel(r):
    masks = cross_masks()
    s1 = Field(part(r.s1_a, 0, 16), part(r.s1_m, 16, 20))
    nu = both_halves(r, "nuh")
    u0 = Field(part(r.u0, 0, ROWS))
    u1 = Field(part(r.u1_e, 0, REACH), part(r.u1_i, REACH, 16), part(r.u1_m, 16, 20))
    known = span(0, 20)

    def step(plane, add):
        s = {t: s1.row(plane, t) for t in known}
        for t, total in stencil(span(0, 16), known, s, masks):
            if t < REACH:
                r.nsum[plane, t] = total
            else:
                value = nu.row(0, t) * total
                r.u2[plane, t - REACH] = value
                with_all(add, 2, value, plane, t, (u0, u1))
        for t in span(0, ROWS):
            value = u0.row(plane, t)
            add((0, 0), value * value)
            if t < 20:
                with_all(add, 1, u1.row(plane, t), plane, t, (u0,))

    write_sums(r.sums, loop_sums(pairs_of(0, 1, 2), step))


def inner3_kernel(r):
    masks = cross_masks()
    s2 = Field(part(r.s2, 0, 16))
    nu = Field(part(r.nuh_a, 0, HALF))
    u0 = Field(part(r.u0, 0, ROWS))
    u1 = Field(part(r.u1_e, 0, REACH), part(r.u1_i, REACH, 16))
    u2 = Field(part(r.u2_e, 0, REACH), part(r.u2_i, REACH, 16))
    known = span(0, 16)

    def step(plane, add):
        s = {t: s2.row(plane, t) for t in known}
        for t, total in stencil(span(0, HALF), known, s, masks):
            if t < REACH:
                r.nsum[plane, t] = total
                with_all(add, 2, u2.row(plane, t), plane, t, (u0, u1))
            else:
                value = nu.row(0, t) * total
                r.u3[plane, t - REACH] = value
                with_all(add, 3, value, plane, t, (u0, u1, u2))

    write_sums(r.sums, loop_sums(pairs_of(2, 3), step))


def beyond_kernel(r):
    nu_a = Field(part(r.nuh_a, 0, HALF))
    nu_b = Field(part(r.nuh_b, HALF, ROWS))
    u0 = Field(part(r.u0, 0, ROWS))
    u1 = Field(part(r.u1_e, 0, REACH))
    u2 = Field(part(r.u2_e, 0, REACH))
    ts = span(ROWS, ROWS + REACH)
    nu = r.p1[PLANES + L - 1]
    read = (
        lambda k: r.p1[PLANES + k],
        nu > 0.0,
        nu,
        r.p1[PLANES + L],
        r.p1[PLANES + L + 1],
    )
    er, ei, link = (Field(part(x, ROWS, ROWS + REACH)) for x in (r.er, r.ei, r.link))
    factor(ts, read, er, ei, link, None)

    def step(plane, add):
        for t in range(REACH):
            value = halo_sum(r.nsum[plane, t], t, lambda q: r.ha[plane, q])
            value = nu_a.row(0, t) * value
            r.u3[plane, t] = value
            with_all(add, 3, value, plane, t, (u0, u1, u2))
        for d in range(REACH):
            t = ROWS - 1 - d
            value = nu_b.row(0, t) * halo_sum(r.p2s[plane, d], d, lambda q: r.p1[plane, q])
            r.u1[plane, t - 20] = value
            with_all(add, 1, value, plane, t, (u0,))

    write_sums(r.sums, loop_sums(pairs_of(1, 3), step))


def band_kernel(r):
    masks = cross_masks()
    nu_b = Field(part(r.nuh_b, HALF, ROWS))
    nu = Field(part(r.nuh_b, HALF, ROWS), part(r.p1, ROWS, ROWS + REACH, PLANES + L - 1))
    er, ei, link = (
        Field(part(getattr(r, n + "_b"), HALF, ROWS), part(getattr(r, n + "_h"), ROWS, ROWS + REACH))
        for n in ("er", "ei", "link")
    )
    s0 = Field(part(r.s0_b, HALF, ROWS))
    u1 = Field(part(r.u1_i, REACH, 16), part(r.u1_m, 16, 20), part(r.u1_b, 20, ROWS))

    def source(plane, ts):
        rows = []
        for t in ts:
            if t < ROWS:
                rows.append(u1.row(plane, t))
            else:
                j = t - ROWS
                value = halo_sum(r.p2[plane, j], j, lambda q: s0.row(plane, ROWS - 1 - q))
                rows.append(nu.row(0, t) * value)
        return jnp.stack(rows)

    s1_b = part(r.s1, 20, 28)
    solve(span(20, 28), source, er, ei, link, Field(s1_b))
    s1 = Field(
        part(r.s1_a, 0, 16), part(r.s1_m, 16, 20), s1_b, part(r.p2, 28, 32, PLANES)
    )
    u0 = Field(part(r.u0, 0, ROWS))
    u2_b = part(r.u2, 16, 28)
    u2 = Field(part(r.u2_i, REACH, 16), u2_b)
    known = span(12, 32)

    def step(plane, add):
        s = {t: s1.row(plane, t) for t in known}
        for t, total in stencil(span(16, 28), known, s, masks):
            value = nu.row(0, t) * total
            u2.put(plane, [t], value[None])
            if t < ROWS:
                with_all(add, 2, value, plane, t, (u0, u1))

    sums = loop_sums(pairs_of(2), step)
    s2_b = part(r.s2, 16, 28)
    for start in (16, 22):
        solve(span(start, start + 6), u2.get, er, ei, link, Field(s2_b))
    s2 = Field(part(r.s2_a, 0, 16), s2_b)
    known3 = span(8, 28)

    def last(plane, add):
        s = {t: s2.row(plane, t) for t in known3}
        for t, total in stencil(span(12, 24), known3, s, masks):
            value = nu_b.row(0, t) * total
            r.u3[plane, t - 12] = value
            with_all(add, 3, value, plane, t, (u0, u1, u2))

    sums.update(loop_sums(pairs_of(3), last))
    lane = lanes()
    out = jnp.zeros(TILE, F32)
    for i, pair in enumerate(GRAM):
        value = r.sums2[i] + r.sums3[i] + r.sums4[i]
        if pair in sums:
            value = value + sums[pair]
        value = jnp.sum(jnp.sum(value, axis=0, keepdims=True), axis=1, keepdims=True)
        out = out + jnp.where(lane == i, value, 0.0)
    for i in range(r.payload.shape[0] // 8):
        r.payload[pl.ds(8 * i, 8), :] = out


def least_squares(columns, start):
    count_cols = len(columns)
    givens_rhs = [start] + [start * 0.0 for index in range(count_cols)]
    cosines, sines, upper_cols = ([], [], [])
    for column_index, column_in in enumerate(columns):
        column = list(column_in)
        for row_index in range(column_index):
            rotated_a = (
                cosines[row_index] * column[row_index] + sines[row_index] * column[row_index + 1]
            )
            rotated_b = (
                -sines[row_index] * column[row_index] + cosines[row_index] * column[row_index + 1]
            )
            column[row_index] = rotated_a
            column[row_index + 1] = rotated_b
        radius = jnp.sqrt(
            column[column_index] * column[column_index]
            + column[column_index + 1] * column[column_index + 1]
        )
        inverse = 1.0 / radius
        cosine = column[column_index] * inverse
        sine_value = column[column_index + 1] * inverse
        column[column_index] = inverse
        cosines.append(cosine)
        sines.append(sine_value)
        upper_cols.append(column)
        next_rhs = -sine_value * givens_rhs[column_index]
        givens_rhs[column_index] = cosine * givens_rhs[column_index]
        givens_rhs[column_index + 1] = next_rhs
    factors = [None] * count_cols
    for column_index in range(count_cols - 1, -1, -1):
        accum = givens_rhs[column_index]
        for later in range(column_index + 1, count_cols):
            accum = accum - upper_cols[later][column_index] * factors[later]
        factors[column_index] = accum * upper_cols[column_index][column_index]
    return factors


def dot(left, right):
    total = left[0] * right[0]
    for a, b in zip(left[1:], right[1:]):
        total = total + a * b
    return total


def coefficients(gram):
    size = 4
    upper = {}
    for a in range(size):
        square = gram[(a, a)]
        for p in range(a):
            square = square - upper[(p, a)] * upper[(p, a)]
        square = jnp.maximum(square, 0.0)
        length = jnp.sqrt(square)
        inverse = jnp.where(length > 0.0, 1.0 / jnp.where(length > 0.0, length, 1.0), 0.0)
        upper[(a, a)] = length
        for b in range(a + 1, size):
            value = gram[(a, b)]
            for p in range(a):
                value = value - upper[(p, a)] * upper[(p, b)]
            upper[(a, b)] = value * inverse
    beta = jnp.sqrt(gram[(0, 0)] + epsilon)
    inverse = 1.0 / beta
    basis = [[inverse]]
    ortho = [[upper[(0, 0)] * inverse]]
    columns = []
    for j in range(3):
        current = basis[j]
        w = [current[0]]
        for i in range(1, j + 1):
            w.append(current[i] - current[i - 1])
        w.append(-current[j])
        q = [dot([upper[(i, m)] for m in range(i, j + 2)], w[i:]) for i in range(j + 2)]
        column = []
        for i in range(j + 1):
            h = dot(q[: i + 1], ortho[i])
            for m in range(i + 1):
                q[m] = q[m] - h * ortho[i][m]
                w[m] = w[m] - h * basis[i][m]
            column.append(h)
        length = jnp.sqrt(dot(q, q) + epsilon)
        column.append(length)
        columns.append(column)
        if j < 2:
            inverse = 1.0 / length
            basis.append([value * inverse for value in w])
            ortho.append([value * inverse for value in q])
    y = least_squares(columns, beta)
    return [dot(y[i:], [basis[j][i] for j in range(i, 3)]) for i in range(3)]


def final_kernel(r):
    total = r.gathered[pl.ds(0, 8), :]
    for i in range(1, r.gathered.shape[0] // 8):
        total = total + r.gathered[pl.ds(8 * i, 8), :]
    total = jnp.sum(total, axis=0, keepdims=True)
    total = jnp.broadcast_to(total, TILE)
    lane = lanes()
    gram = {}
    for i, pair in enumerate(GRAM):
        value = jnp.sum(jnp.where(lane == i, total, 0.0), axis=1, keepdims=True)
        gram[pair] = jnp.broadcast_to(value, TILE)
    c0, c1, c2 = coefficients(gram)
    e0, e1, e2 = 1.0 - c0, c0 - c1, c1 - c2
    core = lax.axis_index(CORE)
    places = [place_of(core, t) for t in range(ROWS)]
    s0 = both_halves(r, "s0")
    s1 = Field(part(r.s1_a, 0, 16), part(r.s1_m, 16, 20), part(r.s1_b, 20, 28))
    s2 = Field(part(r.s2_a, 0, 16), part(r.s2_b, 16, 28))
    u0 = Field(part(r.u0, 0, ROWS))
    u1 = Field(
        part(r.u1_e, 0, 4), part(r.u1_i, 4, 16), part(r.u1_m, 16, 20), part(r.u1_b, 20, 24)
    )
    u2 = Field(part(r.u2_e, 0, 4), part(r.u2_i, 4, 16), part(r.u2_b, 16, 28))
    u3 = Field(part(r.u3_e, 0, 4), part(r.u3_i, 4, 12), part(r.u3_b, 12, 24))

    def step(plane, carry):
        for t in range(ROWS):
            s = [x.row(plane, t) for x in (s0, s1, s2)]
            u = [x.row(plane, t) for x in (u0, u1, u2, u3)]
            tile, sub = places[t]
            r.buf_s[plane, tile, pl.ds(sub, 8, stride=8), :] = c0 * s[0] + c1 * s[1] + c2 * s[2]
            r.buf_r[plane, tile, pl.ds(sub, 8, stride=8), :] = (
                e0 * u[0] + e1 * u[1] + (e2 * u[2] + c2 * u[3])
            )
        pltpu.make_async_copy(r.buf_s.at[plane], r.out_s.at[plane], r.sem_s).start()
        pltpu.make_async_copy(r.buf_r.at[plane], r.out_r.at[plane], r.sem_r).start()
        return carry

    lax.fori_loop(0, PLANES, step, 0)
    pltpu.make_async_copy(r.buf_s, r.out_s, r.sem_s).wait()
    pltpu.make_async_copy(r.buf_r, r.out_r, r.sem_r).wait()


def tiled(x):
    x = x.reshape(-1, ROWS // 8, 8, 8, 128)
    return x.transpose(0, 1, 3, 2, 4).reshape(-1, ROWS // 8, 64, 128)


def untiled(x):
    x = x.reshape(PLANES, ROWS // 8, 8, 8, 128).transpose(0, 1, 3, 2, 4)
    return x.reshape(2, L, ROWS, 1024)


class Refs:
    def __init__(self, names, refs):
        self.__dict__.update(zip(names, refs))


def call(kernel, name, ins, outs, scratch={}, in_specs=None, out_specs=None, limit=4 << 20):
    names = [*ins, *outs, *scratch]

    def run(*refs):
        kernel(Refs(names, refs))

    results = pl.pallas_call(
        run,
        out_shape=list(outs.values()),
        in_specs=[in_specs or VM] * len(ins),
        out_specs=[out_specs or VM] * len(outs),
        scratch_shapes=list(scratch.values()),
        compiler_params=pltpu.CompilerParams(vmem_limit_bytes=limit),
        name=name,
    )(*ins.values())
    return dict(zip(outs, results))


def within(x):
    return lax.ppermute(x, FLOW, [(i, i ^ 1) for i in range(128)])


def across(x):
    pairs = [(i, i + 1) for i in range(1, 127, 2)]
    return lax.ppermute(x, FLOW, pairs + [(b, a) for a, b in pairs])


def body(forcing, viscosity, friction, rotation, vertical, ice_mask, grounded):
    names = ("f", "v", "nu", "fric", "rot", "ice", "ground")
    arrays = (forcing, vertical, viscosity, friction, rotation, ice_mask, grounded)
    ins = {
        n: pltpu.with_memory_space_constraint(tiled(x), pltpu.HBM) for n, x in zip(names, arrays)
    }
    raws = {n + "raw": pltpu.VMEM(x.shape, x.dtype) for n, x in ins.items()}

    def factors(rows):
        return {"er": vmem(L, rows), "ei": vmem(L, rows), "link": vmem(L - 1, rows)}

    def pick(src, tag, *keys):
        return {k + tag: src[k] for k in keys}

    edge = vmem(PLANES, REACH)
    k0 = call(
        load_kernel,
        "load",
        ins,
        {
            **factors(HALF),
            "nuh": vmem(1, HALF),
            "s0": vmem(PLANES, HALF),
            "p1": vmem(PLANES + L + 2, REACH),
            **raws,
        },
        {"sems": pltpu.SemaphoreType.DMA((11,))},
        in_specs=HB,
    )
    p1 = across(k0["p1"])
    ahead = call(
        ahead_kernel,
        "ahead",
        pick(k0, "", "s0", "nuh", "er", "ei", "link"),
        {"u1": edge, "s1": edge, "p2": vmem(2 * PLANES, REACH)},
    )
    p2 = across(ahead["p2"])
    k1 = call(
        rest_kernel,
        "rest",
        {**pick(k0, "", *raws), "order": ahead["p2"]},
        {
            **factors(HALF),
            "nuh": vmem(1, HALF),
            "s0": vmem(PLANES, HALF),
            "u0": vmem(PLANES, ROWS),
            "sa": edge,
        },
    )
    halves = {}
    for key in ("er", "ei", "link", "nuh", "s0"):
        halves[key + "_a"], halves[key + "_b"] = k1[key], k0[key]
    u0 = {"u0": k1["u0"]}

    def some(*keys):
        return {k: halves[k] for k in keys}

    operator = some("er_a", "er_b", "ei_a", "ei_b", "link_a", "link_b", "nuh_a")
    solved = {"u_edge": edge, "s": vmem(PLANES, 16), "sa": edge}
    ha = within(k1["sa"])
    n1 = call(
        inner1_kernel,
        "inner1",
        some("s0_a", "s0_b", "nuh_a", "nuh_b"),
        {"nsum": edge, "u1": vmem(PLANES, HALF)},
    )
    e1 = call(
        edge_a_kernel,
        "edge1",
        {"ha": ha, "nsum": n1["nsum"], "u_in": n1["u1"], **operator},
        solved,
    )
    ha = within(e1["sa"])
    first = {"u1_e": e1["u_edge"], "u1_i": n1["u1"]}
    middle = {"u1_m": ahead["u1"]}
    s1 = {"s1_a": e1["s"], "s1_m": ahead["s1"]}
    n2 = call(
        inner2_kernel,
        "inner2",
        {**s1, **some("nuh_a", "nuh_b"), **u0, **first, **middle},
        {"nsum": edge, "u2": vmem(PLANES, HALF), "sums": vmem(10)},
    )
    e2 = call(
        edge_a_kernel,
        "edge2",
        {"ha": ha, "nsum": n2["nsum"], "u_in": n2["u2"], **operator},
        solved,
    )
    ha = within(e2["sa"])
    second = {"u2_e": e2["u_edge"], "u2_i": n2["u2"]}
    n3 = call(
        inner3_kernel,
        "inner3",
        {"s2": e2["s"], **some("nuh_a"), **u0, **first, **second},
        {"nsum": edge, "u3": vmem(PLANES, 8), "sums": vmem(10)},
    )
    b1 = call(
        beyond_kernel,
        "beyond",
        {
            "ha": ha,
            "nsum": n3["nsum"],
            "p1": p1,
            "p2s": ahead["p2"],
            **some("nuh_a", "nuh_b"),
            **u0,
            "u1_e": first["u1_e"],
            "u2_e": second["u2_e"],
        },
        {**factors(REACH), "u1": edge, "u3": edge, "sums": vmem(10)},
    )
    b2 = call(
        band_kernel,
        "band",
        {
            "p1": p1,
            "p2": p2,
            **some("er_b", "ei_b", "link_b", "nuh_b", "s0_b"),
            **pick(b1, "_h", "er", "ei", "link"),
            **u0,
            "u1_i": n1["u1"],
            **middle,
            "u1_b": b1["u1"],
            **s1,
            "u2_i": n2["u2"],
            "s2_a": e2["s"],
            "sums2": n2["sums"],
            "sums3": n3["sums"],
            "sums4": b1["sums"],
        },
        {
            "s1": vmem(PLANES, 8),
            "u2": vmem(PLANES, HALF),
            "s2": vmem(PLANES, HALF),
            "u3": vmem(PLANES, HALF),
            "payload": jax.ShapeDtypeStruct((128, 128), F32),
        },
    )
    gathered = lax.all_to_all(b2["payload"], FLOW, split_axis=0, concat_axis=0, tiled=True)
    shape = (PLANES, ROWS // 8, 64, 128)
    outs = call(
        final_kernel,
        "combine",
        {
            "gathered": gathered,
            **some("s0_a", "s0_b"),
            **s1,
            "s1_b": b2["s1"],
            "s2_a": e2["s"],
            "s2_b": b2["s2"],
            **u0,
            **first,
            **middle,
            "u1_b": b1["u1"],
            **second,
            "u2_b": b2["u2"],
            "u3_e": b1["u3"],
            "u3_i": n3["u3"],
            "u3_b": b2["u3"],
        },
        {"out_s": jax.ShapeDtypeStruct(shape, F32), "out_r": jax.ShapeDtypeStruct(shape, F32)},
        {
            "buf_s": pltpu.VMEM(shape, F32),
            "buf_r": pltpu.VMEM(shape, F32),
            "sem_s": pltpu.SemaphoreType.DMA,
            "sem_r": pltpu.SemaphoreType.DMA,
        },
        out_specs=HB,
        limit=8 << 20,
    )
    return untiled(outs["out_s"]), untiled(outs["out_r"])


def solution(mesh):
    finer = Mesh(mesh.devices.reshape(4, 4, 4, 2), FLOW)
    return jax.shard_map(
        body,
        mesh=finer,
        in_specs=(
            P(None, None, FLOW, None),
            P(FLOW, None),
            P(FLOW, None),
            P(FLOW, None),
            P(None, FLOW, None),
            P(FLOW, None),
            P(FLOW, None),
        ),
        out_specs=(P(None, None, FLOW, None), P(None, None, FLOW, None)),
        check_vma=False,
    )
```

```python
import jax
import jax.numpy as jnp
from jax import lax
from jax.experimental import pallas as pl
from jax.experimental.pallas import tpu as pltpu
from jax.sharding import Mesh
from jax.sharding import PartitionSpec as P


FLOW = ("flow_0", "flow_1", "flow_2", "flow_3")
CORE = "flow_3"
epsilon = 1e-06
relaxation = 0.5
reach_weights = (1.0, 0.6, 0.35, 0.2)
horiz_total = 2.0 * sum(reach_weights) + 2.0

L = 12
PLANES = 2 * L
ROWS = 24
REACH = 4
HALF = 12
F32 = jnp.float32
TILE = (8, 128)
GRAM = [(a, b) for b in range(4) for a in range(b + 1)]

VM = pl.BlockSpec(memory_space=pltpu.VMEM)
HB = pl.BlockSpec(memory_space=pltpu.HBM)


def vmem(*lead):
    return pltpu.VMEM((*lead, *TILE), F32)


def span(start, stop):
    return list(range(start, stop))


def place_of(core, t):
    tile, sub = t // 8, t % 8
    return (
        jnp.where(core == 1, tile, 2 - tile),
        jnp.where(core == 1, sub, 7 - sub),
    )


def raw_row(ref, plane, place):
    tile, sub = place
    return ref[plane, tile, pl.ds(sub, 8, stride=8), :]


class Field:
    def __init__(self, *parts):
        self.parts = parts

    def find(self, t):
        for ref, first, index in self.parts:
            if t in index:
                return ref, first, index[t]
        raise KeyError(t)

    def row(self, plane, t):
        ref, first, i = self.find(t)
        return ref[first + plane, i]

    def get(self, plane, ts):
        return jnp.stack([self.row(plane, t) for t in ts])

    def put(self, plane, ts, value):
        for i, t in enumerate(ts):
            ref, first, j = self.find(t)
            ref[first + plane, j] = value[i]


def part(ref, start, stop, first=0):
    return (ref, first, {t: t - start for t in range(start, stop)})


def mirrored(ref, start, stop, first=0):
    return (ref, first, {ROWS - 1 - d: d - start for d in range(start, stop)})


def factor(ts, read, inv_real, inv_imag, link, nu_out):
    vert, active, nu, drag, rot = read
    imag = jnp.where(active, rot, 0.0)
    base = (relaxation + horiz_total) * nu
    if nu_out is not None:
        nu_out.put(0, ts, jnp.where(active, nu, 0.0))
    below = er = ei = None
    for k in range(L):
        real = base + (drag if k == 0 else below)
        if k < L - 1:
            above = vert(k)
            real = real + above
        real = jnp.where(active, real, 1.0)
        pivot_imag = imag
        if k > 0:
            ln = jnp.where(active, below, 0.0)
            link.put(k - 1, ts, ln)
            square = ln * ln
            real = real - square * er
            pivot_imag = imag - square * ei
        inverse = 1.0 / (real * real + pivot_imag * pivot_imag)
        er = real * inverse
        ei = -(pivot_imag * inverse)
        inv_real.put(k, ts, er)
        inv_imag.put(k, ts, ei)
        if k < L - 1:
            below = above


def solve(ts, source, inv_real, inv_imag, link, result, also=None):
    cf = cg = None
    for k in range(L):
        sf, sg = source(k, ts), source(L + k, ts)
        if k > 0:
            ln = link.get(k - 1, ts)
            sf = sf + ln * cf
            sg = sg + ln * cg
        er, ei = inv_real.get(k, ts), inv_imag.get(k, ts)
        cf, cg = er * sf + ei * sg, er * sg - ei * sf
        result.put(k, ts, cf)
        result.put(L + k, ts, cg)
    xf, xg = cf, cg
    for k in range(L - 1, -1, -1):
        if k < L - 1:
            ln = link.get(k, ts)
            pf, pg = ln * xf, ln * xg
            er, ei = inv_real.get(k, ts), inv_imag.get(k, ts)
            xf = result.get(k, ts) + (er * pf + ei * pg)
            xg = result.get(L + k, ts) + (er * pg - ei * pf)
            result.put(k, ts, xf)
            result.put(L + k, ts, xg)
        if also is not None:
            copy, rows = also
            for i, t in enumerate(ts):
                if t in rows:
                    copy.put(k, [t], xf[i : i + 1])
                    copy.put(L + k, [t], xg[i : i + 1])


def lanes():
    return lax.broadcasted_iota(jnp.int32, TILE, 1)


def cross_masks():
    lane = lanes()
    sub = lax.broadcasted_iota(jnp.int32, TILE, 0)
    first, last = lane == 0, lane == 127
    return first, last, first & (sub == 7), last & (sub == 0)


def cross(s, masks):
    first, last, first_end, last_end = masks
    up = jnp.where(first, pltpu.roll(s, 7, 0), s)
    up = jnp.where(first_end, 0.0, up)
    down = jnp.where(last, pltpu.roll(s, 1, 0), s)
    down = jnp.where(last_end, 0.0, down)
    return pltpu.roll(up, 127, 1) + pltpu.roll(down, 1, 1)


def stencil(ts, known, s, masks):
    for t in ts:
        total = cross(s[t], masks)
        for m in range(1, REACH + 1):
            near = [s[q] for q in (t - m, t + m) if q in known]
            if near:
                both = near[0] + near[1] if len(near) == 2 else near[0]
                weight = reach_weights[m - 1]
                total = total + (both if weight == 1.0 else weight * both)
        yield t, total


def halo_sum(total, distance, halo):
    for q in range(1, REACH + 1 - distance):
        weight = reach_weights[distance + q - 1]
        value = halo(q - 1)
        total = total + (value if weight == 1.0 else weight * value)
    return total


def loop_sums(pairs, step):
    pairs = list(pairs)

    def run(plane, carry):
        sums = dict(zip(pairs, carry))

        def add(pair, value):
            sums[pair] = sums[pair] + value

        step(plane, add)
        return tuple(sums[pair] for pair in pairs)

    zero = jnp.zeros(TILE, F32)
    return dict(zip(pairs, lax.fori_loop(0, PLANES, run, (zero,) * len(pairs))))


def with_all(add, b, value, plane, t, us):
    for a in range(b):
        add((a, b), value * us[a].row(plane, t))
    add((b, b), value * value)


def pairs_of(*bs):
    return [(a, b) for a, b in GRAM if b in bs]


def raw_reader(r, core, ts):
    places = [place_of(core, t) for t in ts]

    def rows(ref, plane):
        return jnp.stack([raw_row(ref, plane, place) for place in places])

    active = rows(r.iceraw, 0) > 0
    drag = jnp.where(rows(r.groundraw, 0) > 0, rows(r.fricraw, 0), 0.0)
    return (
        lambda k: rows(r.vraw, k),
        active,
        rows(r.nuraw, 0),
        drag,
        rows(r.rotraw, 0),
    )


def raw_source(fraw, core):
    return lambda plane, ts: jnp.stack([raw_row(fraw, plane, place_of(core, t)) for t in ts])


def load_kernel(r):
    core = lax.axis_index(CORE)
    edge = jnp.where(core == 1, 2, 0)
    small = [
        pltpu.make_async_copy(getattr(r, n), getattr(r, n + "raw"), r.sems.at[i])
        for i, n in enumerate(("nu", "fric", "rot", "ice", "ground"))
    ]
    v_copy = [
        pltpu.make_async_copy(r.v.at[:, tile], r.vraw.at[:, tile], r.sems.at[5 + i])
        for i, tile in enumerate((edge, 1, 2 - edge))
    ]
    f_copy = [
        pltpu.make_async_copy(r.f.at[:, tile], r.fraw.at[:, tile], r.sems.at[8 + i])
        for i, tile in enumerate((edge, 1, 2 - edge))
    ]
    for copy in small + v_copy[:2] + f_copy[:2] + [v_copy[2], f_copy[2]]:
        copy.start()
    for copy in small + v_copy[:2]:
        copy.wait()
    er, ei, link, nu = (Field(part(x, HALF, ROWS)) for x in (r.er, r.ei, r.link, r.nuh))
    packed = Field(mirrored(r.p1, 0, REACH))
    for start in (12, 18):
        ts = span(start, start + 6)
        read = raw_reader(r, core, ts)
        factor(ts, read, er, ei, link, nu)
        vert, active, nu_row, drag, rot = read
        for i, t in enumerate(ts):
            if t >= ROWS - REACH:
                for k in range(L - 1):
                    packed.put(PLANES + k, [t], vert(k)[i : i + 1])
                packed.put(PLANES + L - 1, [t], jnp.where(active, nu_row, 0.0)[i : i + 1])
                packed.put(PLANES + L, [t], drag[i : i + 1])
                packed.put(PLANES + L + 1, [t], rot[i : i + 1])
    for copy in f_copy[:2]:
        copy.wait()
    source = raw_source(r.fraw, core)
    s0 = Field(part(r.s0, HALF, ROWS))
    for start in (12, 18):
        ts = span(start, start + 6)
        solve(ts, source, er, ei, link, s0, (packed, span(ROWS - REACH, ROWS)))
    v_copy[2].wait()
    f_copy[2].wait()


def ahead_kernel(r):
    masks = cross_masks()
    s0 = Field(part(r.s0, HALF, ROWS))
    nu = Field(part(r.nuh, HALF, ROWS))
    sums = Field(mirrored(r.p2, 0, REACH))
    known = span(HALF, ROWS)
    u1 = Field(part(r.u1, 16, 20))

    def step(plane, carry):
        s = {t: s0.row(plane, t) for t in known}
        for t, total in stencil(span(16, 24), known, s, masks):
            if t < 20:
                u1.put(plane, [t], (nu.row(0, t) * total)[None])
            else:
                sums.put(plane, [t], total[None])
        return carry

    lax.fori_loop(0, PLANES, step, 0)
    er, ei, link = (Field(part(x, HALF, ROWS)) for x in (r.er, r.ei, r.link))
    packed = Field(mirrored(r.p2, REACH, 2 * REACH, PLANES))
    solve(span(16, 20), u1.get, er, ei, link, Field(part(r.s1, 16, 20)), (packed, span(16, 20)))


def rest_kernel(r):
    core = lax.axis_index(CORE)
    er, ei, link, nu = (Field(part(x, 0, HALF)) for x in (r.er, r.ei, r.link, r.nuh))
    for start in (0, 6):
        ts = span(start, start + 6)
        factor(ts, raw_reader(r, core, ts), er, ei, link, nu)
    places = [place_of(core, t) for t in range(ROWS)]

    def spread(plane, carry):
        for t in range(ROWS):
            r.u0[plane, t] = raw_row(r.fraw, plane, places[t])
        return carry

    lax.fori_loop(0, PLANES, spread, 0)
    u0 = Field(part(r.u0, 0, ROWS))
    s0 = Field(part(r.s0, 0, HALF))
    for start in (0, 6):
        solve(span(start, start + 6), u0.get, er, ei, link, s0, (Field(part(r.sa, 0, REACH)), span(0, REACH)))


def both_halves(r, name):
    return Field(part(getattr(r, name + "_a"), 0, HALF), part(getattr(r, name + "_b"), HALF, ROWS))


def inner1_kernel(r):
    masks = cross_masks()
    s0, nu = both_halves(r, "s0"), both_halves(r, "nuh")
    known = span(0, 20)

    def step(plane, carry):
        s = {t: s0.row(plane, t) for t in known}
        for t, total in stencil(span(0, 16), known, s, masks):
            if t < REACH:
                r.nsum[plane, t] = total
            else:
                r.u1[plane, t - REACH] = nu.row(0, t) * total
        return carry

    lax.fori_loop(0, PLANES, step, 0)


def edge_a_kernel(r):
    nu = Field(part(r.nuh_a, 0, HALF))
    er, ei, link = (both_halves(r, n) for n in ("er", "ei", "link"))
    edge = Field(part(r.u_edge, 0, REACH))
    inner = Field(part(r.u_in, REACH, 16))

    def source(plane, ts):
        rows = []
        for t in ts:
            if t < REACH:
                value = halo_sum(r.nsum[plane, t], t, lambda q: r.ha[plane, q])
                value = nu.row(0, t) * value
                edge.put(plane, [t], value[None])
            else:
                value = inner.row(plane, t)
            rows.append(value)
        return jnp.stack(rows)

    result = Field(part(r.s, 0, 16))
    sa = Field(part(r.sa, 0, REACH))
    for start in (0, 8):
        solve(span(start, start + 8), source, er, ei, link, result, (sa, span(0, REACH)))


def write_sums(ref, sums):
    zero = jnp.zeros(TILE, F32)
    for i, pair in enumerate(GRAM):
        ref[i] = sums.get(pair, zero)


def inner2_kernel(r):
    masks = cross_masks()
    s1 = Field(part(r.s1_a, 0, 16), part(r.s1_m, 16, 20))
    nu = both_halves(r, "nuh")
    u0 = Field(part(r.u0, 0, ROWS))
    u1 = Field(part(r.u1_e, 0, REACH), part(r.u1_i, REACH, 16), part(r.u1_m, 16, 20))
    known = span(0, 20)

    def step(plane, add):
        s = {t: s1.row(plane, t) for t in known}
        for t, total in stencil(span(0, 16), known, s, masks):
            if t < REACH:
                r.nsum[plane, t] = total
            else:
                value = nu.row(0, t) * total
                r.u2[plane, t - REACH] = value
                with_all(add, 2, value, plane, t, (u0, u1))
        for t in span(0, ROWS):
            value = u0.row(plane, t)
            add((0, 0), value * value)
            if t < 20:
                with_all(add, 1, u1.row(plane, t), plane, t, (u0,))

    write_sums(r.sums, loop_sums(pairs_of(0, 1, 2), step))


def inner3_kernel(r):
    masks = cross_masks()
    s2 = Field(part(r.s2, 0, 16))
    nu = Field(part(r.nuh_a, 0, HALF))
    u0 = Field(part(r.u0, 0, ROWS))
    u1 = Field(part(r.u1_e, 0, REACH), part(r.u1_i, REACH, 16))
    u2 = Field(part(r.u2_e, 0, REACH), part(r.u2_i, REACH, 16))
    known = span(0, 16)

    def step(plane, add):
        s = {t: s2.row(plane, t) for t in known}
        for t, total in stencil(span(0, HALF), known, s, masks):
            if t < REACH:
                r.nsum[plane, t] = total
                with_all(add, 2, u2.row(plane, t), plane, t, (u0, u1))
            else:
                value = nu.row(0, t) * total
                r.u3[plane, t - REACH] = value
                with_all(add, 3, value, plane, t, (u0, u1, u2))

    write_sums(r.sums, loop_sums(pairs_of(2, 3), step))


def beyond_kernel(r):
    nu_a = Field(part(r.nuh_a, 0, HALF))
    nu_b = Field(part(r.nuh_b, HALF, ROWS))
    u0 = Field(part(r.u0, 0, ROWS))
    u1 = Field(part(r.u1_e, 0, REACH))
    u2 = Field(part(r.u2_e, 0, REACH))
    ts = span(ROWS, ROWS + REACH)
    nu = r.p1[PLANES + L - 1]
    read = (
        lambda k: r.p1[PLANES + k],
        nu > 0.0,
        nu,
        r.p1[PLANES + L],
        r.p1[PLANES + L + 1],
    )
    er, ei, link = (Field(part(x, ROWS, ROWS + REACH)) for x in (r.er, r.ei, r.link))
    factor(ts, read, er, ei, link, None)

    def step(plane, add):
        for t in range(REACH):
            value = halo_sum(r.nsum[plane, t], t, lambda q: r.ha[plane, q])
            value = nu_a.row(0, t) * value
            r.u3[plane, t] = value
            with_all(add, 3, value, plane, t, (u0, u1, u2))
        for d in range(REACH):
            t = ROWS - 1 - d
            value = nu_b.row(0, t) * halo_sum(r.p2s[plane, d], d, lambda q: r.p1[plane, q])
            r.u1[plane, t - 20] = value
            with_all(add, 1, value, plane, t, (u0,))

    write_sums(r.sums, loop_sums(pairs_of(1, 3), step))


def band_kernel(r):
    masks = cross_masks()
    nu_b = Field(part(r.nuh_b, HALF, ROWS))
    nu = Field(part(r.nuh_b, HALF, ROWS), part(r.p1, ROWS, ROWS + REACH, PLANES + L - 1))
    er, ei, link = (
        Field(part(getattr(r, n + "_b"), HALF, ROWS), part(getattr(r, n + "_h"), ROWS, ROWS + REACH))
        for n in ("er", "ei", "link")
    )
    s0 = Field(part(r.s0_b, HALF, ROWS))
    u1 = Field(part(r.u1_i, REACH, 16), part(r.u1_m, 16, 20), part(r.u1_b, 20, ROWS))

    def source(plane, ts):
        rows = []
        for t in ts:
            if t < ROWS:
                rows.append(u1.row(plane, t))
            else:
                j = t - ROWS
                value = halo_sum(r.p2[plane, j], j, lambda q: s0.row(plane, ROWS - 1 - q))
                rows.append(nu.row(0, t) * value)
        return jnp.stack(rows)

    s1_b = part(r.s1, 20, 28)
    solve(span(20, 28), source, er, ei, link, Field(s1_b))
    s1 = Field(
        part(r.s1_a, 0, 16), part(r.s1_m, 16, 20), s1_b, part(r.p2, 28, 32, PLANES)
    )
    u0 = Field(part(r.u0, 0, ROWS))
    u2_b = part(r.u2, 16, 28)
    u2 = Field(part(r.u2_i, REACH, 16), u2_b)
    known = span(12, 32)

    def step(plane, add):
        s = {t: s1.row(plane, t) for t in known}
        for t, total in stencil(span(16, 28), known, s, masks):
            value = nu.row(0, t) * total
            u2.put(plane, [t], value[None])
            if t < ROWS:
                with_all(add, 2, value, plane, t, (u0, u1))

    sums = loop_sums(pairs_of(2), step)
    s2_b = part(r.s2, 16, 28)
    for start in (16, 22):
        solve(span(start, start + 6), u2.get, er, ei, link, Field(s2_b))
    s2 = Field(part(r.s2_a, 0, 16), s2_b)
    known3 = span(8, 28)

    def last(plane, add):
        s = {t: s2.row(plane, t) for t in known3}
        for t, total in stencil(span(12, 24), known3, s, masks):
            value = nu_b.row(0, t) * total
            r.u3[plane, t - 12] = value
            with_all(add, 3, value, plane, t, (u0, u1, u2))

    sums.update(loop_sums(pairs_of(3), last))
    lane = lanes()
    out = jnp.zeros(TILE, F32)
    for i, pair in enumerate(GRAM):
        value = r.sums2[i] + r.sums3[i] + r.sums4[i]
        if pair in sums:
            value = value + sums[pair]
        value = jnp.sum(jnp.sum(value, axis=0, keepdims=True), axis=1, keepdims=True)
        out = out + jnp.where(lane == i, value, 0.0)
    for i in range(r.payload.shape[0] // 8):
        r.payload[pl.ds(8 * i, 8), :] = out


def least_squares(columns, start):
    count_cols = len(columns)
    givens_rhs = [start] + [start * 0.0 for _ in range(count_cols)]
    cosines, sines, upper_cols = ([], [], [])
    for column_index, column_in in enumerate(columns):
        column = list(column_in)
        for row_index in range(column_index):
            rotated_a = (
                cosines[row_index] * column[row_index] + sines[row_index] * column[row_index + 1]
            )
            rotated_b = (
                -sines[row_index] * column[row_index] + cosines[row_index] * column[row_index + 1]
            )
            column[row_index] = rotated_a
            column[row_index + 1] = rotated_b
        radius = jnp.sqrt(
            column[column_index] * column[column_index]
            + column[column_index + 1] * column[column_index + 1]
        )
        inverse = 1.0 / radius
        cosine = column[column_index] * inverse
        sine_value = column[column_index + 1] * inverse
        column[column_index] = inverse
        cosines.append(cosine)
        sines.append(sine_value)
        upper_cols.append(column)
        next_rhs = -sine_value * givens_rhs[column_index]
        givens_rhs[column_index] = cosine * givens_rhs[column_index]
        givens_rhs[column_index + 1] = next_rhs
    factors = [None] * count_cols
    for column_index in range(count_cols - 1, -1, -1):
        accum = givens_rhs[column_index]
        for later in range(column_index + 1, count_cols):
            accum = accum - upper_cols[later][column_index] * factors[later]
        factors[column_index] = accum * upper_cols[column_index][column_index]
    return factors


def dot(left, right):
    total = left[0] * right[0]
    for a, b in zip(left[1:], right[1:]):
        total = total + a * b
    return total


def coefficients(gram):
    size = 4
    upper = {}
    for a in range(size):
        square = gram[(a, a)]
        for p in range(a):
            square = square - upper[(p, a)] * upper[(p, a)]
        square = jnp.maximum(square, 0.0)
        length = jnp.sqrt(square)
        inverse = jnp.where(length > 0.0, 1.0 / jnp.where(length > 0.0, length, 1.0), 0.0)
        upper[(a, a)] = length
        for b in range(a + 1, size):
            value = gram[(a, b)]
            for p in range(a):
                value = value - upper[(p, a)] * upper[(p, b)]
            upper[(a, b)] = value * inverse
    beta = jnp.sqrt(gram[(0, 0)] + epsilon)
    inverse = 1.0 / beta
    basis = [[inverse]]
    ortho = [[upper[(0, 0)] * inverse]]
    columns = []
    for j in range(3):
        current = basis[j]
        w = [current[0]]
        for i in range(1, j + 1):
            w.append(current[i] - current[i - 1])
        w.append(-current[j])
        q = [dot([upper[(i, m)] for m in range(i, j + 2)], w[i:]) for i in range(j + 2)]
        column = []
        for i in range(j + 1):
            h = dot(q[: i + 1], ortho[i])
            for m in range(i + 1):
                q[m] = q[m] - h * ortho[i][m]
                w[m] = w[m] - h * basis[i][m]
            column.append(h)
        length = jnp.sqrt(dot(q, q) + epsilon)
        column.append(length)
        columns.append(column)
        if j < 2:
            inverse = 1.0 / length
            basis.append([value * inverse for value in w])
            ortho.append([value * inverse for value in q])
    y = least_squares(columns, beta)
    return [dot(y[i:], [basis[j][i] for j in range(i, 3)]) for i in range(3)]


def final_kernel(r):
    total = r.gathered[pl.ds(0, 8), :]
    for i in range(1, r.gathered.shape[0] // 8):
        total = total + r.gathered[pl.ds(8 * i, 8), :]
    total = jnp.sum(total, axis=0, keepdims=True)
    total = jnp.broadcast_to(total, TILE)
    lane = lanes()
    gram = {}
    for i, pair in enumerate(GRAM):
        value = jnp.sum(jnp.where(lane == i, total, 0.0), axis=1, keepdims=True)
        gram[pair] = jnp.broadcast_to(value, TILE)
    c0, c1, c2 = coefficients(gram)
    e0, e1, e2 = 1.0 - c0, c0 - c1, c1 - c2
    core = lax.axis_index(CORE)
    places = [place_of(core, t) for t in range(ROWS)]
    s0 = both_halves(r, "s0")
    s1 = Field(part(r.s1_a, 0, 16), part(r.s1_m, 16, 20), part(r.s1_b, 20, 28))
    s2 = Field(part(r.s2_a, 0, 16), part(r.s2_b, 16, 28))
    u0 = Field(part(r.u0, 0, ROWS))
    u1 = Field(
        part(r.u1_e, 0, 4), part(r.u1_i, 4, 16), part(r.u1_m, 16, 20), part(r.u1_b, 20, 24)
    )
    u2 = Field(part(r.u2_e, 0, 4), part(r.u2_i, 4, 16), part(r.u2_b, 16, 28))
    u3 = Field(part(r.u3_e, 0, 4), part(r.u3_i, 4, 12), part(r.u3_b, 12, 24))

    def step(plane, carry):
        for t in range(ROWS):
            s = [x.row(plane, t) for x in (s0, s1, s2)]
            u = [x.row(plane, t) for x in (u0, u1, u2, u3)]
            tile, sub = places[t]
            r.buf_s[plane, tile, pl.ds(sub, 8, stride=8), :] = c0 * s[0] + c1 * s[1] + c2 * s[2]
            r.buf_r[plane, tile, pl.ds(sub, 8, stride=8), :] = (
                e0 * u[0] + e1 * u[1] + (e2 * u[2] + c2 * u[3])
            )
        pltpu.make_async_copy(r.buf_s.at[plane], r.out_s.at[plane], r.sem_s).start()
        pltpu.make_async_copy(r.buf_r.at[plane], r.out_r.at[plane], r.sem_r).start()
        return carry

    lax.fori_loop(0, PLANES, step, 0)
    pltpu.make_async_copy(r.buf_s, r.out_s, r.sem_s).wait()
    pltpu.make_async_copy(r.buf_r, r.out_r, r.sem_r).wait()


def tiled(x):
    x = x.reshape(-1, ROWS // 8, 8, 8, 128)
    return x.transpose(0, 1, 3, 2, 4).reshape(-1, ROWS // 8, 64, 128)


def untiled(x):
    x = x.reshape(PLANES, ROWS // 8, 8, 8, 128).transpose(0, 1, 3, 2, 4)
    return x.reshape(2, L, ROWS, 1024)


class Refs:
    def __init__(self, names, refs):
        self.__dict__.update(zip(names, refs))


def call(kernel, ins, outs, scratch={}, in_specs=None, out_specs=None, limit=4 << 20):
    names = [*ins, *outs, *scratch]

    def run(*refs):
        kernel(Refs(names, refs))

    results = pl.pallas_call(
        run,
        out_shape=list(outs.values()),
        in_specs=[in_specs or VM] * len(ins),
        out_specs=[out_specs or VM] * len(outs),
        scratch_shapes=list(scratch.values()),
        compiler_params=pltpu.CompilerParams(vmem_limit_bytes=limit),
    )(*ins.values())
    return dict(zip(outs, results))


def within(x):
    return lax.ppermute(x, FLOW, [(i, i ^ 1) for i in range(128)])


def across(x):
    pairs = [(i, i + 1) for i in range(1, 127, 2)]
    return lax.ppermute(x, FLOW, pairs + [(b, a) for a, b in pairs])


def body(forcing, viscosity, friction, rotation, vertical, ice_mask, grounded):
    names = ("f", "v", "nu", "fric", "rot", "ice", "ground")
    arrays = (forcing, vertical, viscosity, friction, rotation, ice_mask, grounded)
    ins = {
        n: pltpu.with_memory_space_constraint(tiled(x), pltpu.HBM) for n, x in zip(names, arrays)
    }
    raws = {n + "raw": pltpu.VMEM(x.shape, x.dtype) for n, x in ins.items()}

    def factors(rows):
        return {"er": vmem(L, rows), "ei": vmem(L, rows), "link": vmem(L - 1, rows)}

    def pick(src, tag, *keys):
        return {k + tag: src[k] for k in keys}

    edge = vmem(PLANES, REACH)
    k0 = call(
        load_kernel,
        ins,
        {
            **factors(HALF),
            "nuh": vmem(1, HALF),
            "s0": vmem(PLANES, HALF),
            "p1": vmem(PLANES + L + 2, REACH),
            **raws,
        },
        {"sems": pltpu.SemaphoreType.DMA((11,))},
        in_specs=HB,
    )
    p1 = across(k0["p1"])
    ahead = call(
        ahead_kernel,
        pick(k0, "", "s0", "nuh", "er", "ei", "link"),
        {"u1": edge, "s1": edge, "p2": vmem(2 * PLANES, REACH)},
    )
    p2 = across(ahead["p2"])
    k1 = call(
        rest_kernel,
        {**pick(k0, "", *raws), "order": ahead["p2"]},
        {
            **factors(HALF),
            "nuh": vmem(1, HALF),
            "s0": vmem(PLANES, HALF),
            "u0": vmem(PLANES, ROWS),
            "sa": edge,
        },
    )
    halves = {}
    for key in ("er", "ei", "link", "nuh", "s0"):
        halves[key + "_a"], halves[key + "_b"] = k1[key], k0[key]
    u0 = {"u0": k1["u0"]}

    def some(*keys):
        return {k: halves[k] for k in keys}

    operator = some("er_a", "er_b", "ei_a", "ei_b", "link_a", "link_b", "nuh_a")
    solved = {"u_edge": edge, "s": vmem(PLANES, 16), "sa": edge}
    ha = within(k1["sa"])
    n1 = call(
        inner1_kernel,
        some("s0_a", "s0_b", "nuh_a", "nuh_b"),
        {"nsum": edge, "u1": vmem(PLANES, HALF)},
    )
    e1 = call(edge_a_kernel, {"ha": ha, "nsum": n1["nsum"], "u_in": n1["u1"], **operator}, solved)
    ha = within(e1["sa"])
    first = {"u1_e": e1["u_edge"], "u1_i": n1["u1"]}
    middle = {"u1_m": ahead["u1"]}
    s1 = {"s1_a": e1["s"], "s1_m": ahead["s1"]}
    n2 = call(
        inner2_kernel,
        {**s1, **some("nuh_a", "nuh_b"), **u0, **first, **middle},
        {"nsum": edge, "u2": vmem(PLANES, HALF), "sums": vmem(10)},
    )
    e2 = call(edge_a_kernel, {"ha": ha, "nsum": n2["nsum"], "u_in": n2["u2"], **operator}, solved)
    ha = within(e2["sa"])
    second = {"u2_e": e2["u_edge"], "u2_i": n2["u2"]}
    n3 = call(
        inner3_kernel,
        {"s2": e2["s"], **some("nuh_a"), **u0, **first, **second},
        {"nsum": edge, "u3": vmem(PLANES, 8), "sums": vmem(10)},
    )
    b1 = call(
        beyond_kernel,
        {
            "ha": ha,
            "nsum": n3["nsum"],
            "p1": p1,
            "p2s": ahead["p2"],
            **some("nuh_a", "nuh_b"),
            **u0,
            "u1_e": first["u1_e"],
            "u2_e": second["u2_e"],
        },
        {**factors(REACH), "u1": edge, "u3": edge, "sums": vmem(10)},
    )
    b2 = call(
        band_kernel,
        {
            "p1": p1,
            "p2": p2,
            **some("er_b", "ei_b", "link_b", "nuh_b", "s0_b"),
            **pick(b1, "_h", "er", "ei", "link"),
            **u0,
            "u1_i": n1["u1"],
            **middle,
            "u1_b": b1["u1"],
            **s1,
            "u2_i": n2["u2"],
            "s2_a": e2["s"],
            "sums2": n2["sums"],
            "sums3": n3["sums"],
            "sums4": b1["sums"],
        },
        {
            "s1": vmem(PLANES, 8),
            "u2": vmem(PLANES, HALF),
            "s2": vmem(PLANES, HALF),
            "u3": vmem(PLANES, HALF),
            "payload": jax.ShapeDtypeStruct((128, 128), F32),
        },
    )
    gathered = lax.all_to_all(b2["payload"], FLOW, split_axis=0, concat_axis=0, tiled=True)
    shape = (PLANES, ROWS // 8, 64, 128)
    outs = call(
        final_kernel,
        {
            "gathered": gathered,
            **some("s0_a", "s0_b"),
            **s1,
            "s1_b": b2["s1"],
            "s2_a": e2["s"],
            "s2_b": b2["s2"],
            **u0,
            **first,
            **middle,
            "u1_b": b1["u1"],
            **second,
            "u2_b": b2["u2"],
            "u3_e": b1["u3"],
            "u3_i": n3["u3"],
            "u3_b": b2["u3"],
        },
        {"out_s": jax.ShapeDtypeStruct(shape, F32), "out_r": jax.ShapeDtypeStruct(shape, F32)},
        {
            "buf_s": pltpu.VMEM(shape, F32),
            "buf_r": pltpu.VMEM(shape, F32),
            "sem_s": pltpu.SemaphoreType.DMA,
            "sem_r": pltpu.SemaphoreType.DMA,
        },
        out_specs=HB,
        limit=8 << 20,
    )
    return untiled(outs["out_s"]), untiled(outs["out_r"])


def solution(mesh):
    finer = Mesh(mesh.devices.reshape(4, 4, 4, 2), FLOW)

    return jax.shard_map(
        body,
        mesh=finer,
        in_specs=(
            P(None, None, FLOW, None),
            P(FLOW, None),
            P(FLOW, None),
            P(FLOW, None),
            P(None, FLOW, None),
            P(FLOW, None),
            P(FLOW, None),
        ),
        out_specs=(P(None, None, FLOW, None), P(None, None, FLOW, None)),
        check_vma=False,
    )
```

```python
import jax
import jax.numpy as jnp
from jax import lax
from jax.experimental import pallas as pl
from jax.experimental.pallas import tpu as pltpu
from jax.sharding import Mesh
from jax.sharding import PartitionSpec as P


FLOW = ("flow_0", "flow_1", "flow_2", "flow_3")
CORE = "flow_3"
epsilon = 1e-06
relaxation = 0.5
reach_weights = (1.0, 0.6, 0.35, 0.2)
horiz_total = 2.0 * sum(reach_weights) + 2.0

L = 12
PLANES = 2 * L
ROWS = 24
REACH = 4
HALF = 12
GROUP = 4
COEFS = 2 * PLANES
F32 = jnp.float32
TILE = (8, 128)
GRAM = [(a, b) for b in range(4) for a in range(b + 1)]

VM = pl.BlockSpec(memory_space=pltpu.VMEM)
HB = pl.BlockSpec(memory_space=pltpu.HBM)


def vmem(*lead):
    return pltpu.VMEM((*lead, *TILE), F32)


def span(start, stop):
    return list(range(start, stop))


def place_of(core, t):
    tile, sub = t // 8, t % 8
    return (
        jnp.where(core == 1, tile, 2 - tile),
        jnp.where(core == 1, sub, 7 - sub),
    )


def raw_row(ref, plane, place):
    tile, sub = place
    return ref[plane, tile, pl.ds(sub, 8, stride=8), :]


class Field:
    def __init__(self, *parts):
        self.parts = parts

    def find(self, t):
        for ref, first, index in self.parts:
            if t in index:
                return ref, first, index[t]
        raise KeyError(t)

    def row(self, plane, t):
        ref, first, i = self.find(t)
        return ref[first + plane, i]

    def get(self, plane, ts):
        return jnp.stack([self.row(plane, t) for t in ts])

    def put(self, plane, ts, value):
        for i, t in enumerate(ts):
            ref, first, j = self.find(t)
            ref[first + plane, j] = value[i]


def part(ref, start, stop, first=0):
    return (ref, first, {t: t - start for t in range(start, stop)})


def mirrored(ref, start, stop, first=0):
    return (ref, first, {ROWS - 1 - d: d - start for d in range(start, stop)})


def factor(ts, read, inv_real, inv_imag, link, nu_out):
    vert, active, nu, drag, rot = read
    imag = jnp.where(active, rot, 0.0)
    base = (relaxation + horiz_total) * nu
    if nu_out is not None:
        nu_out.put(0, ts, jnp.where(active, nu, 0.0))
    below = er = ei = None
    for k in range(L):
        real = base + (drag if k == 0 else below)
        if k < L - 1:
            above = vert(k)
            real = real + above
        real = jnp.where(active, real, 1.0)
        pivot_imag = imag
        if k > 0:
            ln = jnp.where(active, below, 0.0)
            link.put(k - 1, ts, ln)
            square = ln * ln
            real = real - square * er
            pivot_imag = imag - square * ei
        inverse = 1.0 / (real * real + pivot_imag * pivot_imag)
        er = real * inverse
        ei = -(pivot_imag * inverse)
        inv_real.put(k, ts, er)
        inv_imag.put(k, ts, ei)
        if k < L - 1:
            below = above


def solve(ts, source, inv_real, inv_imag, link, result, also=None):
    cf = cg = None
    for k in range(L):
        sf, sg = source(k, ts), source(L + k, ts)
        if k > 0:
            ln = link.get(k - 1, ts)
            sf = sf + ln * cf
            sg = sg + ln * cg
        er, ei = inv_real.get(k, ts), inv_imag.get(k, ts)
        cf, cg = er * sf + ei * sg, er * sg - ei * sf
        result.put(k, ts, cf)
        result.put(L + k, ts, cg)
    xf, xg = cf, cg
    for k in range(L - 1, -1, -1):
        if k < L - 1:
            ln = link.get(k, ts)
            pf, pg = ln * xf, ln * xg
            er, ei = inv_real.get(k, ts), inv_imag.get(k, ts)
            xf = result.get(k, ts) + (er * pf + ei * pg)
            xg = result.get(L + k, ts) + (er * pg - ei * pf)
            result.put(k, ts, xf)
            result.put(L + k, ts, xg)
        if also is not None:
            copy, rows = also
            for i, t in enumerate(ts):
                if t in rows:
                    copy.put(k, [t], xf[i : i + 1])
                    copy.put(L + k, [t], xg[i : i + 1])


def lanes():
    return lax.broadcasted_iota(jnp.int32, TILE, 1)


def cross_masks():
    lane = lanes()
    sub = lax.broadcasted_iota(jnp.int32, TILE, 0)
    first, last = lane == 0, lane == 127
    return first, last, first & (sub == 7), last & (sub == 0)


def cross(s, masks):
    first, last, first_end, last_end = masks
    up = jnp.where(first, pltpu.roll(s, 7, 0), s)
    up = jnp.where(first_end, 0.0, up)
    down = jnp.where(last, pltpu.roll(s, 1, 0), s)
    down = jnp.where(last_end, 0.0, down)
    return pltpu.roll(up, 127, 1) + pltpu.roll(down, 1, 1)


def stencil(ts, known, s, masks):
    for t in ts:
        total = cross(s[t], masks)
        for m in range(1, REACH + 1):
            near = [s[q] for q in (t - m, t + m) if q in known]
            if near:
                both = near[0] + near[1] if len(near) == 2 else near[0]
                weight = reach_weights[m - 1]
                total = total + (both if weight == 1.0 else weight * both)
        yield t, total


def halo_sum(total, distance, halo):
    for q in range(1, REACH + 1 - distance):
        weight = reach_weights[distance + q - 1]
        value = halo(q - 1)
        total = total + (value if weight == 1.0 else weight * value)
    return total


def over_planes(step, together=GROUP):
    def run(group, carry):
        for i in range(together):
            step(group * together + i)
        return carry

    lax.fori_loop(0, PLANES // together, run, 0)


def loop_sums(pairs, step, together=GROUP):
    pairs = list(pairs)

    def run(group, carry):
        sums = dict(zip(pairs, carry))

        def add(pair, value):
            sums[pair] = sums[pair] + value

        for i in range(together):
            step(group * together + i, add)
        return tuple(sums[pair] for pair in pairs)

    zero = jnp.zeros(TILE, F32)
    return dict(zip(pairs, lax.fori_loop(0, PLANES // together, run, (zero,) * len(pairs))))


def with_all(add, b, value, plane, t, us):
    for a in range(b):
        add((a, b), value * us[a].row(plane, t))
    add((b, b), value * value)


def pairs_of(*bs):
    return [(a, b) for a, b in GRAM if b in bs]


def raw_reader(r, core, ts):
    places = [place_of(core, t) for t in ts]

    def rows(ref, plane):
        return jnp.stack([raw_row(ref, plane, place) for place in places])

    active = rows(r.iceraw, 0) > 0
    drag = jnp.where(rows(r.groundraw, 0) > 0, rows(r.fricraw, 0), 0.0)
    return (
        lambda k: rows(r.vraw, k),
        active,
        rows(r.nuraw, 0),
        drag,
        rows(r.rotraw, 0),
    )


def raw_source(fraw, core):
    return lambda plane, ts: jnp.stack([raw_row(fraw, plane, place_of(core, t)) for t in ts])


def load_kernel(r):
    core = lax.axis_index(CORE)
    edge = jnp.where(core == 1, 2, 0)
    small = [
        pltpu.make_async_copy(getattr(r, n), getattr(r, n + "raw"), r.sems.at[i])
        for i, n in enumerate(("nu", "fric", "rot", "ice", "ground"))
    ]
    v_copy = [
        pltpu.make_async_copy(r.v.at[:, tile], r.vraw.at[:, tile], r.sems.at[5 + i])
        for i, tile in enumerate((edge, 1, 2 - edge))
    ]
    f_copy = [
        pltpu.make_async_copy(r.f.at[:, tile], r.fraw.at[:, tile], r.sems.at[8 + i])
        for i, tile in enumerate((edge, 1, 2 - edge))
    ]
    for copy in small + v_copy[:2] + f_copy[:2] + [v_copy[2], f_copy[2]]:
        copy.start()
    for copy in small + v_copy[:2]:
        copy.wait()
    er, ei, link, nu = (Field(part(x, HALF, ROWS)) for x in (r.er, r.ei, r.link, r.nuh))
    packed = Field(mirrored(r.p1, 0, REACH), mirrored(r.p1, REACH, 2 * REACH, PLANES))
    for start in (12, 18):
        ts = span(start, start + 6)
        read = raw_reader(r, core, ts)
        factor(ts, read, er, ei, link, nu)
        vert, active, nu_row, drag, rot = read
        for i, t in enumerate(ts):
            if t >= ROWS - REACH:
                for k in range(L - 1):
                    packed.put(COEFS + k, [t], vert(k)[i : i + 1])
                packed.put(COEFS + L - 1, [t], jnp.where(active, nu_row, 0.0)[i : i + 1])
                packed.put(COEFS + L, [t], drag[i : i + 1])
                packed.put(COEFS + L + 1, [t], rot[i : i + 1])
    for copy in f_copy[:2]:
        copy.wait()
    source = raw_source(r.fraw, core)
    s0 = Field(part(r.s0, HALF, ROWS))
    for start in (12, 18):
        ts = span(start, start + 6)
        solve(ts, source, er, ei, link, s0, (packed, span(ROWS - 2 * REACH, ROWS)))
    v_copy[2].wait()
    f_copy[2].wait()


def ahead_kernel(r):
    masks = cross_masks()
    s0 = Field(part(r.s0, HALF, ROWS))
    nu = Field(part(r.nuh, HALF, ROWS))
    known = span(HALF, ROWS)
    u1 = Field(part(r.u1, 16, 20))

    def step(plane):
        s = {t: s0.row(plane, t) for t in known}
        for t, total in stencil(span(16, 20), known, s, masks):
            u1.put(plane, [t], (nu.row(0, t) * total)[None])

    over_planes(step, 8)
    er, ei, link = (Field(part(x, HALF, ROWS)) for x in (r.er, r.ei, r.link))
    packed = Field(mirrored(r.p2, REACH, 2 * REACH))
    solve(span(16, 20), u1.get, er, ei, link, Field(part(r.s1, 16, 20)), (packed, span(16, 20)))


def rest_kernel(r):
    core = lax.axis_index(CORE)
    er, ei, link, nu = (Field(part(x, 0, HALF)) for x in (r.er, r.ei, r.link, r.nuh))
    for start in (0, 6):
        ts = span(start, start + 6)
        factor(ts, raw_reader(r, core, ts), er, ei, link, nu)
    places = [place_of(core, t) for t in range(ROWS)]

    def spread(plane):
        for t in range(ROWS):
            r.u0[plane, t] = raw_row(r.fraw, plane, places[t])

    over_planes(spread, 2)
    u0 = Field(part(r.u0, 0, ROWS))
    s0 = Field(part(r.s0, 0, HALF))
    for start in (0, 6):
        solve(span(start, start + 6), u0.get, er, ei, link, s0, (Field(part(r.sa, 0, REACH)), span(0, REACH)))


def both_halves(r, name):
    return Field(part(getattr(r, name + "_a"), 0, HALF), part(getattr(r, name + "_b"), HALF, ROWS))


def inner1_kernel(r):
    masks = cross_masks()
    s0, nu = both_halves(r, "s0"), both_halves(r, "nuh")
    known = span(0, 20)

    def step(plane):
        s = {t: s0.row(plane, t) for t in known}
        for t, total in stencil(span(0, 16), known, s, masks):
            if t < REACH:
                r.nsum[plane, t] = total
            else:
                r.u1[plane, t - REACH] = nu.row(0, t) * total

    over_planes(step)


def edge_a_kernel(r):
    nu = Field(part(r.nuh_a, 0, HALF))
    er, ei, link = (both_halves(r, n) for n in ("er", "ei", "link"))
    edge = Field(part(r.u_edge, 0, REACH))
    inner = Field(part(r.u_in, REACH, 16))

    def source(plane, ts):
        rows = []
        for t in ts:
            if t < REACH:
                value = halo_sum(r.nsum[plane, t], t, lambda q: r.ha[plane, q])
                value = nu.row(0, t) * value
                edge.put(plane, [t], value[None])
            else:
                value = inner.row(plane, t)
            rows.append(value)
        return jnp.stack(rows)

    result = Field(part(r.s, 0, 16))
    sa = Field(part(r.sa, 0, REACH))
    for start in (0, 8):
        solve(span(start, start + 8), source, er, ei, link, result, (sa, span(0, REACH)))


def write_sums(ref, sums):
    zero = jnp.zeros(TILE, F32)
    for i, pair in enumerate(GRAM):
        ref[i] = sums.get(pair, zero)


def inner2_kernel(r):
    masks = cross_masks()
    s1 = Field(part(r.s1_a, 0, 16), part(r.s1_m, 16, 20))
    nu = both_halves(r, "nuh")
    u0 = Field(part(r.u0, 0, ROWS))
    u1 = Field(part(r.u1_e, 0, REACH), part(r.u1_i, REACH, 16), part(r.u1_m, 16, 20))
    known = span(0, 20)

    def step(plane, add):
        s = {t: s1.row(plane, t) for t in known}
        for t, total in stencil(span(0, 16), known, s, masks):
            if t < REACH:
                r.nsum[plane, t] = total
            else:
                value = nu.row(0, t) * total
                r.u2[plane, t - REACH] = value
                with_all(add, 2, value, plane, t, (u0, u1))
        for t in span(0, ROWS):
            value = u0.row(plane, t)
            add((0, 0), value * value)
            if t < 20:
                with_all(add, 1, u1.row(plane, t), plane, t, (u0,))

    write_sums(r.sums, loop_sums(pairs_of(0, 1, 2), step))


def inner3_kernel(r):
    masks = cross_masks()
    s2 = Field(part(r.s2, 0, 16))
    nu = Field(part(r.nuh_a, 0, HALF))
    u0 = Field(part(r.u0, 0, ROWS))
    u1 = Field(part(r.u1_e, 0, REACH), part(r.u1_i, REACH, 16))
    u2 = Field(part(r.u2_e, 0, REACH), part(r.u2_i, REACH, 16))
    known = span(0, 16)

    def step(plane, add):
        s = {t: s2.row(plane, t) for t in known}
        for t, total in stencil(span(0, HALF), known, s, masks):
            if t < REACH:
                r.nsum[plane, t] = total
                with_all(add, 2, u2.row(plane, t), plane, t, (u0, u1))
            else:
                value = nu.row(0, t) * total
                r.u3[plane, t - REACH] = value
                with_all(add, 3, value, plane, t, (u0, u1, u2))

    write_sums(r.sums, loop_sums(pairs_of(2, 3), step))


def last_a_kernel(r):
    nu = Field(part(r.nuh_a, 0, HALF))
    u0 = Field(part(r.u0, 0, ROWS))
    u1 = Field(part(r.u1_e, 0, REACH))
    u2 = Field(part(r.u2_e, 0, REACH))

    def step(plane, add):
        for t in range(REACH):
            value = halo_sum(r.nsum[plane, t], t, lambda q: r.ha[plane, q])
            value = nu.row(0, t) * value
            r.u3[plane, t] = value
            with_all(add, 3, value, plane, t, (u0, u1, u2))

    write_sums(r.sums, loop_sums(pairs_of(3), step))


def band_kernel(r):
    masks = cross_masks()
    beyond = span(ROWS, ROWS + REACH)
    nu_b = Field(part(r.nuh_b, HALF, ROWS))
    nu = Field(part(r.nuh_b, HALF, ROWS), part(r.p1, ROWS, ROWS + REACH, COEFS + L - 1))
    er_h, ei_h, link_h = (part(x, ROWS, ROWS + REACH) for x in (r.er_h, r.ei_h, r.link_h))
    nu_h = r.p1[COEFS + L - 1]
    read = (
        lambda k: r.p1[COEFS + k],
        nu_h > 0.0,
        nu_h,
        r.p1[COEFS + L],
        r.p1[COEFS + L + 1],
    )
    factor(beyond, read, Field(er_h), Field(ei_h), Field(link_h), None)
    er = Field(part(r.er_b, HALF, ROWS), er_h)
    ei = Field(part(r.ei_b, HALF, ROWS), ei_h)
    link = Field(part(r.link_b, HALF, ROWS), link_h)
    s0 = Field(
        part(r.s0_b, HALF, ROWS), part(r.p1, 24, 28), part(r.p1, 28, 32, PLANES)
    )
    u1_b = part(r.u1_b, 20, 28)
    known1 = span(16, 32)

    def first(plane):
        s = {t: s0.row(plane, t) for t in known1}
        for t, total in stencil(span(20, 28), known1, s, masks):
            r.u1_b[plane, t - 20] = nu.row(0, t) * total

    over_planes(first)
    s1_b = part(r.s1, 20, 28)
    solve(span(20, 28), Field(u1_b).get, er, ei, link, Field(s1_b))
    s1 = Field(part(r.s1_a, 0, 16), part(r.s1_m, 16, 20), s1_b, part(r.p2, 28, 32))
    u1 = Field(part(r.u1_i, REACH, 16), part(r.u1_m, 16, 20), u1_b)
    u0 = Field(part(r.u0, 0, ROWS))
    u2_b = part(r.u2, 16, 28)
    u2 = Field(part(r.u2_i, REACH, 16), u2_b)
    known = span(12, 32)

    def step(plane, add):
        s = {t: s1.row(plane, t) for t in known}
        for t, total in stencil(span(16, 28), known, s, masks):
            value = nu.row(0, t) * total
            u2.put(plane, [t], value[None])
            if t < ROWS:
                with_all(add, 2, value, plane, t, (u0, u1))
        for t in span(20, ROWS):
            with_all(add, 1, u1.row(plane, t), plane, t, (u0,))

    sums = loop_sums(pairs_of(1, 2), step)
    s2_b = part(r.s2, 16, 28)
    for start in (16, 22):
        solve(span(start, start + 6), u2.get, er, ei, link, Field(s2_b))
    s2 = Field(part(r.s2_a, 0, 16), s2_b)
    known3 = span(8, 28)

    def last(plane, add):
        s = {t: s2.row(plane, t) for t in known3}
        for t, total in stencil(span(12, 24), known3, s, masks):
            value = nu_b.row(0, t) * total
            r.u3[plane, t - 12] = value
            with_all(add, 3, value, plane, t, (u0, u1, u2))

    sums.update(loop_sums(pairs_of(3), last))
    lane = lanes()
    out = jnp.zeros(TILE, F32)
    for i, pair in enumerate(GRAM):
        value = r.sums2[i] + r.sums3[i] + r.sums4[i]
        if pair in sums:
            value = value + sums[pair]
        value = jnp.sum(jnp.sum(value, axis=0, keepdims=True), axis=1, keepdims=True)
        out = out + jnp.where(lane == i, value, 0.0)
    for i in range(r.payload.shape[0] // 8):
        r.payload[pl.ds(8 * i, 8), :] = out


def least_squares(columns, start):
    count_cols = len(columns)
    givens_rhs = [start] + [start * 0.0 for _ in range(count_cols)]
    cosines, sines, upper_cols = ([], [], [])
    for column_index, column_in in enumerate(columns):
        column = list(column_in)
        for row_index in range(column_index):
            rotated_a = (
                cosines[row_index] * column[row_index] + sines[row_index] * column[row_index + 1]
            )
            rotated_b = (
                -sines[row_index] * column[row_index] + cosines[row_index] * column[row_index + 1]
            )
            column[row_index] = rotated_a
            column[row_index + 1] = rotated_b
        radius = jnp.sqrt(
            column[column_index] * column[column_index]
            + column[column_index + 1] * column[column_index + 1]
        )
        inverse = 1.0 / radius
        cosine = column[column_index] * inverse
        sine_value = column[column_index + 1] * inverse
        column[column_index] = inverse
        cosines.append(cosine)
        sines.append(sine_value)
        upper_cols.append(column)
        next_rhs = -sine_value * givens_rhs[column_index]
        givens_rhs[column_index] = cosine * givens_rhs[column_index]
        givens_rhs[column_index + 1] = next_rhs
    factors = [None] * count_cols
    for column_index in range(count_cols - 1, -1, -1):
        accum = givens_rhs[column_index]
        for later in range(column_index + 1, count_cols):
            accum = accum - upper_cols[later][column_index] * factors[later]
        factors[column_index] = accum * upper_cols[column_index][column_index]
    return factors


def dot(left, right):
    total = left[0] * right[0]
    for a, b in zip(left[1:], right[1:]):
        total = total + a * b
    return total


def coefficients(gram):
    size = 4
    upper = {}
    for a in range(size):
        square = gram[(a, a)]
        for p in range(a):
            square = square - upper[(p, a)] * upper[(p, a)]
        square = jnp.maximum(square, 0.0)
        length = jnp.sqrt(square)
        inverse = jnp.where(length > 0.0, 1.0 / jnp.where(length > 0.0, length, 1.0), 0.0)
        upper[(a, a)] = length
        for b in range(a + 1, size):
            value = gram[(a, b)]
            for p in range(a):
                value = value - upper[(p, a)] * upper[(p, b)]
            upper[(a, b)] = value * inverse
    beta = jnp.sqrt(gram[(0, 0)] + epsilon)
    inverse = 1.0 / beta
    basis = [[inverse]]
    ortho = [[upper[(0, 0)] * inverse]]
    columns = []
    for j in range(3):
        current = basis[j]
        w = [current[0]]
        for i in range(1, j + 1):
            w.append(current[i] - current[i - 1])
        w.append(-current[j])
        q = [dot([upper[(i, m)] for m in range(i, j + 2)], w[i:]) for i in range(j + 2)]
        column = []
        for i in range(j + 1):
            h = dot(q[: i + 1], ortho[i])
            for m in range(i + 1):
                q[m] = q[m] - h * ortho[i][m]
                w[m] = w[m] - h * basis[i][m]
            column.append(h)
        length = jnp.sqrt(dot(q, q) + epsilon)
        column.append(length)
        columns.append(column)
        if j < 2:
            inverse = 1.0 / length
            basis.append([value * inverse for value in w])
            ortho.append([value * inverse for value in q])
    y = least_squares(columns, beta)
    return [dot(y[i:], [basis[j][i] for j in range(i, 3)]) for i in range(3)]


def final_kernel(r):
    total = r.gathered[pl.ds(0, 8), :]
    for i in range(1, r.gathered.shape[0] // 8):
        total = total + r.gathered[pl.ds(8 * i, 8), :]
    total = jnp.sum(total, axis=0, keepdims=True)
    total = jnp.broadcast_to(total, TILE)
    lane = lanes()
    gram = {}
    for i, pair in enumerate(GRAM):
        value = jnp.sum(jnp.where(lane == i, total, 0.0), axis=1, keepdims=True)
        gram[pair] = jnp.broadcast_to(value, TILE)
    c0, c1, c2 = coefficients(gram)
    e0, e1, e2 = 1.0 - c0, c0 - c1, c1 - c2
    core = lax.axis_index(CORE)
    places = [place_of(core, t) for t in range(ROWS)]
    s0 = both_halves(r, "s0")
    s1 = Field(part(r.s1_a, 0, 16), part(r.s1_m, 16, 20), part(r.s1_b, 20, 28))
    s2 = Field(part(r.s2_a, 0, 16), part(r.s2_b, 16, 28))
    u0 = Field(part(r.u0, 0, ROWS))
    u1 = Field(
        part(r.u1_e, 0, 4), part(r.u1_i, 4, 16), part(r.u1_m, 16, 20), part(r.u1_b, 20, 28)
    )
    u2 = Field(part(r.u2_e, 0, 4), part(r.u2_i, 4, 16), part(r.u2_b, 16, 28))
    u3 = Field(part(r.u3_e, 0, 4), part(r.u3_i, 4, 12), part(r.u3_b, 12, 24))

    def step(plane):
        for t in range(ROWS):
            s = [x.row(plane, t) for x in (s0, s1, s2)]
            u = [x.row(plane, t) for x in (u0, u1, u2, u3)]
            tile, sub = places[t]
            r.buf_s[plane, tile, pl.ds(sub, 8, stride=8), :] = c0 * s[0] + c1 * s[1] + c2 * s[2]
            r.buf_r[plane, tile, pl.ds(sub, 8, stride=8), :] = (
                e0 * u[0] + e1 * u[1] + (e2 * u[2] + c2 * u[3])
            )
        pltpu.make_async_copy(r.buf_s.at[plane], r.out_s.at[plane], r.sem_s).start()
        pltpu.make_async_copy(r.buf_r.at[plane], r.out_r.at[plane], r.sem_r).start()

    over_planes(step, 2)
    pltpu.make_async_copy(r.buf_s, r.out_s, r.sem_s).wait()
    pltpu.make_async_copy(r.buf_r, r.out_r, r.sem_r).wait()


def tiled(x):
    x = x.reshape(-1, ROWS // 8, 8, 8, 128)
    return x.transpose(0, 1, 3, 2, 4).reshape(-1, ROWS // 8, 64, 128)


def untiled(x):
    x = x.reshape(PLANES, ROWS // 8, 8, 8, 128).transpose(0, 1, 3, 2, 4)
    return x.reshape(2, L, ROWS, 1024)


class Refs:
    def __init__(self, names, refs):
        self.__dict__.update(zip(names, refs))


def call(kernel, ins, outs, scratch={}, in_specs=None, out_specs=None, limit=4 << 20):
    names = [*ins, *outs, *scratch]

    def run(*refs):
        kernel(Refs(names, refs))

    results = pl.pallas_call(
        run,
        out_shape=list(outs.values()),
        in_specs=[in_specs or VM] * len(ins),
        out_specs=[out_specs or VM] * len(outs),
        scratch_shapes=list(scratch.values()),
        compiler_params=pltpu.CompilerParams(vmem_limit_bytes=limit),
    )(*ins.values())
    return dict(zip(outs, results))


def within(x):
    return lax.ppermute(x, FLOW, [(i, i ^ 1) for i in range(128)])


def across(x):
    pairs = [(i, i + 1) for i in range(1, 127, 2)]
    return lax.ppermute(x, FLOW, pairs + [(b, a) for a, b in pairs])


def body(forcing, viscosity, friction, rotation, vertical, ice_mask, grounded):
    names = ("f", "v", "nu", "fric", "rot", "ice", "ground")
    arrays = (forcing, vertical, viscosity, friction, rotation, ice_mask, grounded)
    ins = {
        n: pltpu.with_memory_space_constraint(tiled(x), pltpu.HBM) for n, x in zip(names, arrays)
    }
    raws = {n + "raw": pltpu.VMEM(x.shape, x.dtype) for n, x in ins.items()}

    def factors(rows):
        return {"er": vmem(L, rows), "ei": vmem(L, rows), "link": vmem(L - 1, rows)}

    def pick(src, tag, *keys):
        return {k + tag: src[k] for k in keys}

    edge = vmem(PLANES, REACH)
    k0 = call(
        load_kernel,
        ins,
        {
            **factors(HALF),
            "nuh": vmem(1, HALF),
            "s0": vmem(PLANES, HALF),
            "p1": vmem(COEFS + L + 2, REACH),
            **raws,
        },
        {"sems": pltpu.SemaphoreType.DMA((11,))},
        in_specs=HB,
    )
    p1 = across(k0["p1"])
    ahead = call(
        ahead_kernel,
        pick(k0, "", "s0", "nuh", "er", "ei", "link"),
        {"u1": edge, "s1": edge, "p2": edge},
    )
    p2 = across(ahead["p2"])
    k1 = call(
        rest_kernel,
        {**pick(k0, "", *raws), "order": ahead["p2"]},
        {
            **factors(HALF),
            "nuh": vmem(1, HALF),
            "s0": vmem(PLANES, HALF),
            "u0": vmem(PLANES, ROWS),
            "sa": edge,
        },
    )
    halves = {}
    for key in ("er", "ei", "link", "nuh", "s0"):
        halves[key + "_a"], halves[key + "_b"] = k1[key], k0[key]
    u0 = {"u0": k1["u0"]}

    def some(*keys):
        return {k: halves[k] for k in keys}

    operator = some("er_a", "er_b", "ei_a", "ei_b", "link_a", "link_b", "nuh_a")
    solved = {"u_edge": edge, "s": vmem(PLANES, 16), "sa": edge}
    ha = within(k1["sa"])
    n1 = call(
        inner1_kernel,
        some("s0_a", "s0_b", "nuh_a", "nuh_b"),
        {"nsum": edge, "u1": vmem(PLANES, HALF)},
    )
    e1 = call(edge_a_kernel, {"ha": ha, "nsum": n1["nsum"], "u_in": n1["u1"], **operator}, solved)
    ha = within(e1["sa"])
    first = {"u1_e": e1["u_edge"], "u1_i": n1["u1"]}
    middle = {"u1_m": ahead["u1"]}
    s1 = {"s1_a": e1["s"], "s1_m": ahead["s1"]}
    n2 = call(
        inner2_kernel,
        {**s1, **some("nuh_a", "nuh_b"), **u0, **first, **middle},
        {"nsum": edge, "u2": vmem(PLANES, HALF), "sums": vmem(10)},
    )
    e2 = call(edge_a_kernel, {"ha": ha, "nsum": n2["nsum"], "u_in": n2["u2"], **operator}, solved)
    ha = within(e2["sa"])
    second = {"u2_e": e2["u_edge"], "u2_i": n2["u2"]}
    n3 = call(
        inner3_kernel,
        {"s2": e2["s"], **some("nuh_a"), **u0, **first, **second},
        {"nsum": edge, "u3": vmem(PLANES, 8), "sums": vmem(10)},
    )
    a3 = call(
        last_a_kernel,
        {
            "ha": ha,
            "nsum": n3["nsum"],
            **some("nuh_a"),
            **u0,
            "u1_e": first["u1_e"],
            "u2_e": second["u2_e"],
        },
        {"u3": edge, "sums": vmem(10)},
    )
    b2 = call(
        band_kernel,
        {
            "p1": p1,
            "p2": p2,
            **some("er_b", "ei_b", "link_b", "nuh_b", "s0_b"),
            **u0,
            "u1_i": n1["u1"],
            **middle,
            **s1,
            "u2_i": n2["u2"],
            "s2_a": e2["s"],
            "sums2": n2["sums"],
            "sums3": n3["sums"],
            "sums4": a3["sums"],
        },
        {
            "u1_b": vmem(PLANES, 8),
            "s1": vmem(PLANES, 8),
            "u2": vmem(PLANES, HALF),
            "s2": vmem(PLANES, HALF),
            "u3": vmem(PLANES, HALF),
            "payload": jax.ShapeDtypeStruct((128, 128), F32),
        },
        {"er_h": vmem(L, REACH), "ei_h": vmem(L, REACH), "link_h": vmem(L - 1, REACH)},
    )
    gathered = lax.all_to_all(b2["payload"], FLOW, split_axis=0, concat_axis=0, tiled=True)
    shape = (PLANES, ROWS // 8, 64, 128)
    outs = call(
        final_kernel,
        {
            "gathered": gathered,
            **some("s0_a", "s0_b"),
            **s1,
            "s1_b": b2["s1"],
            "s2_a": e2["s"],
            "s2_b": b2["s2"],
            **u0,
            **first,
            **middle,
            "u1_b": b2["u1_b"],
            **second,
            "u2_b": b2["u2"],
            "u3_e": a3["u3"],
            "u3_i": n3["u3"],
            "u3_b": b2["u3"],
        },
        {"out_s": jax.ShapeDtypeStruct(shape, F32), "out_r": jax.ShapeDtypeStruct(shape, F32)},
        {
            "buf_s": pltpu.VMEM(shape, F32),
            "buf_r": pltpu.VMEM(shape, F32),
            "sem_s": pltpu.SemaphoreType.DMA,
            "sem_r": pltpu.SemaphoreType.DMA,
        },
        out_specs=HB,
        limit=8 << 20,
    )
    return untiled(outs["out_s"]), untiled(outs["out_r"])


def solution(mesh):
    finer = Mesh(mesh.devices.reshape(4, 4, 4, 2), FLOW)

    return jax.shard_map(
        body,
        mesh=finer,
        in_specs=(
            P(None, None, FLOW, None),
            P(FLOW, None),
            P(FLOW, None),
            P(FLOW, None),
            P(None, FLOW, None),
            P(FLOW, None),
            P(FLOW, None),
        ),
        out_specs=(P(None, None, FLOW, None), P(None, None, FLOW, None)),
        check_vma=False,
    )
```

```python
import jax
import jax.numpy as jnp
from jax import lax
from jax.experimental import pallas as pl
from jax.experimental.pallas import tpu as pltpu
from jax.sharding import Mesh
from jax.sharding import PartitionSpec as P


FLOW = ("flow_0", "flow_1", "flow_2", "flow_3")
CORE = "flow_3"
epsilon = 1e-06
TINY = 1e-37
relaxation = 0.5
reach_weights = (1.0, 0.6, 0.35, 0.2)
horiz_total = 2.0 * sum(reach_weights) + 2.0

L = 12
PLANES = 2 * L
ROWS = 24
REACH = 4
HALF = 12
BAND = 16
GROUP = 4
COEFS = 2 * PLANES
F32 = jnp.float32
TILE = (8, 128)
GRAM = [(a, b) for b in range(4) for a in range(b + 1)]

VM = pl.BlockSpec(memory_space=pltpu.VMEM)
HB = pl.BlockSpec(memory_space=pltpu.HBM)


def vmem(*lead):
    return pltpu.VMEM((*lead, *TILE), F32)


def span(start, stop):
    return list(range(start, stop))


def place_of(core, t):
    tile, sub = t // 8, t % 8
    return (
        jnp.where(core == 1, tile, 2 - tile),
        jnp.where(core == 1, sub, 7 - sub),
    )


def raw_row(ref, plane, place):
    tile, sub = place
    return ref[plane, tile, pl.ds(sub, 8, stride=8), :]


class Field:
    def __init__(self, *parts):
        self.parts = parts

    def find(self, t):
        for ref, first, index in self.parts:
            if t in index:
                return ref, first, index[t]
        raise KeyError(t)

    def row(self, plane, t):
        ref, first, i = self.find(t)
        return ref[first + plane, i]

    def get(self, plane, ts):
        return jnp.stack([self.row(plane, t) for t in ts])

    def put(self, plane, ts, value):
        for i, t in enumerate(ts):
            ref, first, j = self.find(t)
            ref[first + plane, j] = value[i]


def part(ref, start, stop, first=0):
    return (ref, first, {t: t - start for t in range(start, stop)})


def mirrored(ref, start, stop, first=0):
    return (ref, first, {ROWS - 1 - d: d - start for d in range(start, stop)})


def factor(ts, read, inv_real, inv_imag, link, nu_out):
    vert, active, nu, drag, rot = read
    imag = jnp.where(active, rot, 0.0)
    base = (relaxation + horiz_total) * nu
    if nu_out is not None:
        nu_out.put(0, ts, jnp.where(active, nu, 0.0))
    below = er = ei = None
    for k in range(L):
        real = base + (drag if k == 0 else below)
        if k < L - 1:
            above = vert(k)
            real = real + above
        real = jnp.where(active, real, 1.0)
        pivot_imag = imag
        if k > 0:
            ln = jnp.where(active, below, 0.0)
            link.put(k - 1, ts, ln)
            square = ln * ln
            real = real - square * er
            pivot_imag = imag - square * ei
        inverse = 1.0 / (real * real + pivot_imag * pivot_imag)
        er = real * inverse
        ei = -(pivot_imag * inverse)
        inv_real.put(k, ts, er)
        inv_imag.put(k, ts, ei)
        if k < L - 1:
            below = above


def solve(ts, source, inv_real, inv_imag, link, result, also=None):
    cf = cg = None
    for k in range(L):
        sf, sg = source(k, ts), source(L + k, ts)
        if k > 0:
            ln = link.get(k - 1, ts)
            sf = sf + ln * cf
            sg = sg + ln * cg
        er, ei = inv_real.get(k, ts), inv_imag.get(k, ts)
        cf, cg = er * sf + ei * sg, er * sg - ei * sf
        result.put(k, ts, cf)
        result.put(L + k, ts, cg)
    xf, xg = cf, cg
    for k in range(L - 1, -1, -1):
        if k < L - 1:
            ln = link.get(k, ts)
            pf, pg = ln * xf, ln * xg
            er, ei = inv_real.get(k, ts), inv_imag.get(k, ts)
            xf = result.get(k, ts) + (er * pf + ei * pg)
            xg = result.get(L + k, ts) + (er * pg - ei * pf)
            result.put(k, ts, xf)
            result.put(L + k, ts, xg)
        if also is not None:
            copy, rows = also
            for i, t in enumerate(ts):
                if t in rows:
                    copy.put(k, [t], xf[i : i + 1])
                    copy.put(L + k, [t], xg[i : i + 1])


def lanes():
    return lax.broadcasted_iota(jnp.int32, TILE, 1)


def cross_masks():
    lane = lanes()
    sub = lax.broadcasted_iota(jnp.int32, TILE, 0)
    first, last = lane == 0, lane == 127
    return first, last, first & (sub == 7), last & (sub == 0)


def cross(s, masks):
    first, last, first_end, last_end = masks
    up = jnp.where(first, pltpu.roll(s, 7, 0), s)
    up = jnp.where(first_end, 0.0, up)
    down = jnp.where(last, pltpu.roll(s, 1, 0), s)
    down = jnp.where(last_end, 0.0, down)
    return pltpu.roll(up, 127, 1) + pltpu.roll(down, 1, 1)


def stencil(ts, known, s, masks):
    for t in ts:
        total = cross(s[t], masks)
        for m in range(1, REACH + 1):
            near = [s[q] for q in (t - m, t + m) if q in known]
            if near:
                both = near[0] + near[1] if len(near) == 2 else near[0]
                weight = reach_weights[m - 1]
                total = total + (both if weight == 1.0 else weight * both)
        yield t, total


def halo_sum(total, distance, halo):
    for q in range(1, REACH + 1 - distance):
        weight = reach_weights[distance + q - 1]
        value = halo(q - 1)
        total = total + (value if weight == 1.0 else weight * value)
    return total


def over_planes(step, together=GROUP):
    def run(group, carry):
        for i in range(together):
            step(group * together + i)
        return carry

    lax.fori_loop(0, PLANES // together, run, 0)


def loop_sums(pairs, step, together=GROUP):
    pairs = list(pairs)

    def run(group, carry):
        sums = dict(zip(pairs, carry))

        def add(pair, value):
            sums[pair] = sums[pair] + value

        for i in range(together):
            step(group * together + i, add)
        return tuple(sums[pair] for pair in pairs)

    zero = jnp.zeros(TILE, F32)
    return dict(zip(pairs, lax.fori_loop(0, PLANES // together, run, (zero,) * len(pairs))))


def with_all(add, b, value, plane, t, us):
    for a in range(b):
        add((a, b), value * us[a].row(plane, t))
    add((b, b), value * value)


def pairs_of(*bs):
    return [(a, b) for a, b in GRAM if b in bs]


def raw_reader(r, core, ts):
    places = [place_of(core, t) for t in ts]

    def rows(ref, plane):
        return jnp.stack([raw_row(ref, plane, place) for place in places])

    active = rows(r.iceraw, 0) > 0
    drag = jnp.where(rows(r.groundraw, 0) > 0, rows(r.fricraw, 0), 0.0)
    return (
        lambda k: rows(r.vraw, k),
        active,
        rows(r.nuraw, 0),
        drag,
        rows(r.rotraw, 0),
    )


def raw_source(fraw, core):
    return lambda plane, ts: jnp.stack([raw_row(fraw, plane, place_of(core, t)) for t in ts])


def load_kernel(r):
    core = lax.axis_index(CORE)
    edge = jnp.where(core == 1, 2, 0)
    names = ("nu", "fric", "rot", "ice", "ground", "v", "f")
    copies = {}
    for i, tile in enumerate((edge, 1, 2 - edge)):
        for j, n in enumerate(names):
            copies[n, i] = pltpu.make_async_copy(
                getattr(r, n).at[:, tile], getattr(r, n + "raw").at[:, tile], r.sems.at[i, j]
            )
            copies[n, i].start()
    for n in names[:-1]:
        copies[n, 0].wait()
    er, ei, link, nu = (Field(part(x, BAND, ROWS)) for x in (r.er, r.ei, r.link, r.nuh))
    packed = Field(mirrored(r.p1, 0, REACH), mirrored(r.p1, REACH, 2 * REACH, PLANES))
    ts = span(BAND, ROWS)
    read = raw_reader(r, core, ts)
    factor(ts, read, er, ei, link, nu)
    vert, active, nu_row, drag, rot = read
    for i, t in enumerate(ts):
        if t >= ROWS - REACH:
            for k in range(L - 1):
                packed.put(COEFS + k, [t], vert(k)[i : i + 1])
            packed.put(COEFS + L - 1, [t], jnp.where(active, nu_row, 0.0)[i : i + 1])
            packed.put(COEFS + L, [t], drag[i : i + 1])
            packed.put(COEFS + L + 1, [t], rot[i : i + 1])
    copies["f", 0].wait()
    solve(ts, raw_source(r.fraw, core), er, ei, link, Field(part(r.s0, BAND, ROWS)), (packed, ts))
    for i in (1, 2):
        for n in names:
            copies[n, i].wait()


def ahead_kernel(r):
    core = lax.axis_index(CORE)
    masks = cross_masks()
    middle = span(HALF, BAND)
    er_m, ei_m, link_m, nu_m = (part(x, HALF, BAND) for x in (r.er, r.ei, r.link, r.nuh))
    s0_m = part(r.s0, HALF, BAND)
    solver = (Field(er_m), Field(ei_m), Field(link_m))
    factor(middle, raw_reader(r, core, middle), *solver, Field(nu_m))
    solve(middle, raw_source(r.fraw, core), *solver, Field(s0_m))
    s0 = Field(s0_m, part(r.s0_b, BAND, ROWS))
    nu = Field(part(r.nuh_b, BAND, ROWS))
    known = span(HALF, ROWS)
    ts = span(16, 20)
    u1 = Field(part(r.u1, 16, 20))

    def step(plane):
        s = {t: s0.row(plane, t) for t in known}
        for t, total in stencil(ts, known, s, masks):
            u1.put(plane, [t], (nu.row(0, t) * total)[None])

    over_planes(step, 8)
    solver = tuple(Field(part(x, BAND, ROWS)) for x in (r.er_b, r.ei_b, r.link_b))
    packed = Field(mirrored(r.p2, REACH, 2 * REACH))
    solve(ts, u1.get, *solver, Field(part(r.s1, 16, 20)), (packed, ts))


def rest_kernel(r):
    core = lax.axis_index(CORE)
    er, ei, link, nu = (Field(part(x, 0, HALF)) for x in (r.er, r.ei, r.link, r.nuh))
    for start in (0, 6):
        ts = span(start, start + 6)
        factor(ts, raw_reader(r, core, ts), er, ei, link, nu)
    places = [place_of(core, t) for t in range(ROWS)]

    def spread(plane):
        for t in range(ROWS):
            r.u0[plane, t] = raw_row(r.fraw, plane, places[t])

    over_planes(spread, 2)
    u0 = Field(part(r.u0, 0, ROWS))
    s0 = Field(part(r.s0, 0, HALF))
    for start in (0, 6):
        solve(span(start, start + 6), u0.get, er, ei, link, s0, (Field(part(r.sa, 0, REACH)), span(0, REACH)))


def both_halves(r, name):
    starts = (("_a", 0, HALF), ("_m", HALF, BAND), ("_b", BAND, ROWS))
    return Field(*(part(getattr(r, name + tag), a, b) for tag, a, b in starts if hasattr(r, name + tag)))


def inner1_kernel(r):
    masks = cross_masks()
    s0, nu = both_halves(r, "s0"), both_halves(r, "nuh")
    known = span(0, 20)

    def step(plane):
        s = {t: s0.row(plane, t) for t in known}
        for t, total in stencil(span(0, 16), known, s, masks):
            if t < REACH:
                r.nsum[plane, t] = total
            else:
                r.u1[plane, t - REACH] = nu.row(0, t) * total

    over_planes(step)


def edge_a_kernel(r):
    nu = Field(part(r.nuh_a, 0, HALF))
    er, ei, link = (both_halves(r, n) for n in ("er", "ei", "link"))
    edge = Field(part(r.u_edge, 0, REACH))
    inner = Field(part(r.u_in, REACH, 16))

    def source(plane, ts):
        rows = []
        for t in ts:
            if t < REACH:
                value = halo_sum(r.nsum[plane, t], t, lambda q: r.ha[plane, q])
                value = nu.row(0, t) * value
                edge.put(plane, [t], value[None])
            else:
                value = inner.row(plane, t)
            rows.append(value)
        return jnp.stack(rows)

    result = Field(part(r.s, 0, 16))
    sa = Field(part(r.sa, 0, REACH))
    for start in (0, 8):
        solve(span(start, start + 8), source, er, ei, link, result, (sa, span(0, REACH)))


def write_sums(ref, sums):
    zero = jnp.zeros(TILE, F32)
    for i, pair in enumerate(GRAM):
        ref[i] = sums.get(pair, zero)


def inner2_kernel(r):
    masks = cross_masks()
    s1 = Field(part(r.s1_a, 0, 16), part(r.s1_m, 16, 20))
    nu = both_halves(r, "nuh")
    u0 = Field(part(r.u0, 0, ROWS))
    u1 = Field(part(r.u1_e, 0, REACH), part(r.u1_i, REACH, 16), part(r.u1_m, 16, 20))
    known = span(0, 20)

    def step(plane, add):
        s = {t: s1.row(plane, t) for t in known}
        for t, total in stencil(span(0, 16), known, s, masks):
            if t < REACH:
                r.nsum[plane, t] = total
            else:
                value = nu.row(0, t) * total
                r.u2[plane, t - REACH] = value
                with_all(add, 2, value, plane, t, (u0, u1))
        for t in span(0, ROWS):
            value = u0.row(plane, t)
            add((0, 0), value * value)
            if t < 20:
                with_all(add, 1, u1.row(plane, t), plane, t, (u0,))

    write_sums(r.sums, loop_sums(pairs_of(0, 1, 2), step))


def inner3_kernel(r):
    masks = cross_masks()
    s2 = Field(part(r.s2, 0, 16))
    nu = Field(part(r.nuh_a, 0, HALF))
    u0 = Field(part(r.u0, 0, ROWS))
    u1 = Field(part(r.u1_e, 0, REACH), part(r.u1_i, REACH, 16))
    u2 = Field(part(r.u2_e, 0, REACH), part(r.u2_i, REACH, 16))
    known = span(0, 16)

    def step(plane, add):
        s = {t: s2.row(plane, t) for t in known}
        for t, total in stencil(span(0, HALF), known, s, masks):
            if t < REACH:
                r.nsum[plane, t] = total
                with_all(add, 2, u2.row(plane, t), plane, t, (u0, u1))
            else:
                value = nu.row(0, t) * total
                r.u3[plane, t - REACH] = value
                with_all(add, 3, value, plane, t, (u0, u1, u2))

    write_sums(r.sums, loop_sums(pairs_of(2, 3), step))


def last_a_kernel(r):
    nu = Field(part(r.nuh_a, 0, HALF))
    u0 = Field(part(r.u0, 0, ROWS))
    u1 = Field(part(r.u1_e, 0, REACH))
    u2 = Field(part(r.u2_e, 0, REACH))

    def step(plane, add):
        for t in range(REACH):
            value = halo_sum(r.nsum[plane, t], t, lambda q: r.ha[plane, q])
            value = nu.row(0, t) * value
            r.u3[plane, t] = value
            with_all(add, 3, value, plane, t, (u0, u1, u2))

    write_sums(r.sums, loop_sums(pairs_of(3), step))


def band_kernel(r):
    masks = cross_masks()
    beyond = span(ROWS, ROWS + REACH)
    nu_own = both_halves(r, "nuh")
    nu = Field(part(r.nuh_b, BAND, ROWS), part(r.p1, ROWS, ROWS + REACH, COEFS + L - 1))
    er_h, ei_h, link_h = (part(x, ROWS, ROWS + REACH) for x in (r.er_h, r.ei_h, r.link_h))
    nu_h = r.p1[COEFS + L - 1]
    read = (
        lambda k: r.p1[COEFS + k],
        nu_h > 0.0,
        nu_h,
        r.p1[COEFS + L],
        r.p1[COEFS + L + 1],
    )
    factor(beyond, read, Field(er_h), Field(ei_h), Field(link_h), None)
    er = Field(part(r.er_b, BAND, ROWS), er_h)
    ei = Field(part(r.ei_b, BAND, ROWS), ei_h)
    link = Field(part(r.link_b, BAND, ROWS), link_h)
    s0 = Field(
        part(r.s0_b, BAND, ROWS), part(r.p1, 24, 28), part(r.p1, 28, 32, PLANES)
    )
    u1_b = part(r.u1_b, 20, 28)
    known1 = span(16, 32)

    def first(plane):
        s = {t: s0.row(plane, t) for t in known1}
        for t, total in stencil(span(20, 28), known1, s, masks):
            r.u1_b[plane, t - 20] = nu.row(0, t) * total

    over_planes(first)
    s1_b = part(r.s1, 20, 28)
    solve(span(20, 28), Field(u1_b).get, er, ei, link, Field(s1_b))
    s1 = Field(part(r.s1_a, 0, 16), part(r.s1_m, 16, 20), s1_b)
    u1 = Field(part(r.u1_i, REACH, 16), part(r.u1_m, 16, 20), u1_b)
    u0 = Field(part(r.u0, 0, ROWS))
    u2_b = part(r.u2, 16, 24)
    known2 = span(12, 28)

    def second(plane, add):
        s = {t: s1.row(plane, t) for t in known2}
        for t, total in stencil(span(16, 28), known2, s, masks):
            if t < ROWS:
                value = nu.row(0, t) * total
                r.u2[plane, t - 16] = value
                with_all(add, 2, value, plane, t, (u0, u1))
            else:
                r.nsum2[plane, t - ROWS] = total
        for t in span(20, ROWS):
            with_all(add, 1, u1.row(plane, t), plane, t, (u0,))

    sums = loop_sums(pairs_of(1, 2), second)
    s2_b = part(r.s2, 16, 24)
    solve(span(16, 24), Field(u2_b).get, er, ei, link, Field(s2_b))
    s2 = Field(part(r.s2_a, 0, 16), s2_b)
    u2 = Field(part(r.u2_i, REACH, 16), u2_b)
    known3 = span(8, 24)

    def third(plane, add):
        s = {t: s2.row(plane, t) for t in known3}
        for t, total in stencil(span(12, 24), known3, s, masks):
            if t < 20:
                value = nu_own.row(0, t) * total
                r.u3[plane, t - 12] = value
                with_all(add, 3, value, plane, t, (u0, u1, u2))
            else:
                r.nsum3[plane, t - 20] = total

    sums.update(loop_sums(pairs_of(3), third))
    zero = jnp.zeros(TILE, F32)
    for i, pair in enumerate(GRAM):
        r.sums[i] = r.sums2[i] + r.sums3[i] + r.sums4[i] + sums.get(pair, zero)


def last_b_kernel(r):
    beyond = span(ROWS, ROWS + REACH)
    solver = tuple(Field(part(x, ROWS, ROWS + REACH)) for x in (r.er_h, r.ei_h, r.link_h))
    nu_b = Field(part(r.nuh_b, BAND, ROWS))

    def source(plane, ts):
        rows = []
        for j in range(REACH):
            value = r.nsum2[plane, j]
            for q in range(j + 1):
                value = value + reach_weights[REACH - 1 - j + q] * r.p2[plane, q]
            rows.append(r.p1[COEFS + L - 1, j] * value)
        return jnp.stack(rows)

    solve(beyond, source, *solver, Field(part(r.s2_h, ROWS, ROWS + REACH)))
    u0 = Field(part(r.u0, 0, ROWS))
    u1 = Field(part(r.u1_b, 20, 28))
    u2 = Field(part(r.u2_b, 16, 24))

    def step(plane, add):
        for t in span(20, ROWS):
            d = ROWS - 1 - t
            value = halo_sum(r.nsum3[plane, t - 20], d, lambda q: r.s2_h[plane, q])
            value = nu_b.row(0, t) * value
            r.u3[plane, t - 20] = value
            with_all(add, 3, value, plane, t, (u0, u1, u2))

    sums = loop_sums(pairs_of(3), step, 6)
    lane = lanes()
    out = jnp.zeros(TILE, F32)
    for i, pair in enumerate(GRAM):
        value = r.sums[i]
        if pair in sums:
            value = value + sums[pair]
        value = jnp.sum(jnp.sum(value, axis=0, keepdims=True), axis=1, keepdims=True)
        out = out + jnp.where(lane == i, value, 0.0)
    for i in range(r.payload.shape[0] // 8):
        r.payload[pl.ds(8 * i, 8), :] = out


def least_squares(columns, start):
    count_cols = len(columns)
    givens_rhs = [start] + [start * 0.0 for _ in range(count_cols)]
    cosines, sines, upper_cols = ([], [], [])
    for column_index, column_in in enumerate(columns):
        column = list(column_in)
        for row_index in range(column_index):
            rotated_a = (
                cosines[row_index] * column[row_index] + sines[row_index] * column[row_index + 1]
            )
            rotated_b = (
                -sines[row_index] * column[row_index] + cosines[row_index] * column[row_index + 1]
            )
            column[row_index] = rotated_a
            column[row_index + 1] = rotated_b
        inverse = lax.rsqrt(
            column[column_index] * column[column_index]
            + column[column_index + 1] * column[column_index + 1]
        )
        cosine = column[column_index] * inverse
        sine_value = column[column_index + 1] * inverse
        column[column_index] = inverse
        cosines.append(cosine)
        sines.append(sine_value)
        upper_cols.append(column)
        next_rhs = -sine_value * givens_rhs[column_index]
        givens_rhs[column_index] = cosine * givens_rhs[column_index]
        givens_rhs[column_index + 1] = next_rhs
    factors = [None] * count_cols
    for column_index in range(count_cols - 1, -1, -1):
        accum = givens_rhs[column_index]
        for later in range(column_index + 1, count_cols):
            accum = accum - upper_cols[later][column_index] * factors[later]
        factors[column_index] = accum * upper_cols[column_index][column_index]
    return factors


def dot(left, right):
    total = left[0] * right[0]
    for a, b in zip(left[1:], right[1:]):
        total = total + a * b
    return total


def coefficients(gram):
    size = 4
    upper = {}
    for a in range(size):
        square = gram[(a, a)]
        for p in range(a):
            square = square - upper[(p, a)] * upper[(p, a)]
        inverse = jnp.where(square > 0.0, lax.rsqrt(jnp.maximum(square, TINY)), 0.0)
        upper[(a, a)] = square * inverse
        for b in range(a + 1, size):
            value = gram[(a, b)]
            for p in range(a):
                value = value - upper[(p, a)] * upper[(p, b)]
            upper[(a, b)] = value * inverse
    square = gram[(0, 0)] + epsilon
    inverse = lax.rsqrt(square)
    beta = square * inverse
    basis = [[inverse]]
    ortho = [[upper[(0, 0)] * inverse]]
    columns = []
    for j in range(3):
        current = basis[j]
        w = [current[0]]
        for i in range(1, j + 1):
            w.append(current[i] - current[i - 1])
        w.append(-current[j])
        q = [dot([upper[(i, m)] for m in range(i, j + 2)], w[i:]) for i in range(j + 2)]
        column = []
        for i in range(j + 1):
            h = dot(q[: i + 1], ortho[i])
            for m in range(i + 1):
                q[m] = q[m] - h * ortho[i][m]
                w[m] = w[m] - h * basis[i][m]
            column.append(h)
        square = dot(q, q) + epsilon
        inverse = lax.rsqrt(square)
        column.append(square * inverse)
        columns.append(column)
        if j < 2:
            basis.append([value * inverse for value in w])
            ortho.append([value * inverse for value in q])
    y = least_squares(columns, beta)
    return [dot(y[i:], [basis[j][i] for j in range(i, 3)]) for i in range(3)]


def final_kernel(r):
    total = r.gathered[pl.ds(0, 8), :]
    for i in range(1, r.gathered.shape[0] // 8):
        total = total + r.gathered[pl.ds(8 * i, 8), :]
    total = jnp.sum(total, axis=0, keepdims=True)
    total = jnp.broadcast_to(total, TILE)
    lane = lanes()
    gram = {}
    for i, pair in enumerate(GRAM):
        value = jnp.sum(jnp.where(lane == i, total, 0.0), axis=1, keepdims=True)
        gram[pair] = jnp.broadcast_to(value, TILE)
    c0, c1, c2 = coefficients(gram)
    e0, e1, e2 = 1.0 - c0, c0 - c1, c1 - c2
    core = lax.axis_index(CORE)
    places = [place_of(core, t) for t in range(ROWS)]
    s0 = both_halves(r, "s0")
    s1 = Field(part(r.s1_a, 0, 16), part(r.s1_m, 16, 20), part(r.s1_b, 20, 28))
    s2 = Field(part(r.s2_a, 0, 16), part(r.s2_b, 16, 24))
    u0 = Field(part(r.u0, 0, ROWS))
    u1 = Field(
        part(r.u1_e, 0, 4), part(r.u1_i, 4, 16), part(r.u1_m, 16, 20), part(r.u1_b, 20, 28)
    )
    u2 = Field(part(r.u2_e, 0, 4), part(r.u2_i, 4, 16), part(r.u2_b, 16, 24))
    u3 = Field(
        part(r.u3_e, 0, 4), part(r.u3_i, 4, 12), part(r.u3_b, 12, 20), part(r.u3_h, 20, 24)
    )

    def step(plane):
        for t in range(ROWS):
            s = [x.row(plane, t) for x in (s0, s1, s2)]
            u = [x.row(plane, t) for x in (u0, u1, u2, u3)]
            tile, sub = places[t]
            r.buf_s[plane, tile, pl.ds(sub, 8, stride=8), :] = c0 * s[0] + c1 * s[1] + c2 * s[2]
            r.buf_r[plane, tile, pl.ds(sub, 8, stride=8), :] = (
                e0 * u[0] + e1 * u[1] + (e2 * u[2] + c2 * u[3])
            )
        pltpu.make_async_copy(r.buf_s.at[plane], r.out_s.at[plane], r.sem_s).start()
        pltpu.make_async_copy(r.buf_r.at[plane], r.out_r.at[plane], r.sem_r).start()

    over_planes(step, 2)
    pltpu.make_async_copy(r.buf_s, r.out_s, r.sem_s).wait()
    pltpu.make_async_copy(r.buf_r, r.out_r, r.sem_r).wait()


def tiled(x):
    x = x.reshape(-1, ROWS // 8, 8, 8, 128)
    return x.transpose(0, 1, 3, 2, 4).reshape(-1, ROWS // 8, 64, 128)


def untiled(x):
    x = x.reshape(PLANES, ROWS // 8, 8, 8, 128).transpose(0, 1, 3, 2, 4)
    return x.reshape(2, L, ROWS, 1024)


class Refs:
    def __init__(self, names, refs):
        self.__dict__.update(zip(names, refs))


def call(kernel, ins, outs, scratch={}, in_specs=None, out_specs=None, limit=4 << 20):
    names = [*ins, *outs, *scratch]

    def run(*refs):
        kernel(Refs(names, refs))

    results = pl.pallas_call(
        run,
        out_shape=list(outs.values()),
        in_specs=[in_specs or VM] * len(ins),
        out_specs=[out_specs or VM] * len(outs),
        scratch_shapes=list(scratch.values()),
        compiler_params=pltpu.CompilerParams(vmem_limit_bytes=limit),
    )(*ins.values())
    return dict(zip(outs, results))


def within(x):
    return lax.ppermute(x, FLOW, [(i, i ^ 1) for i in range(128)])


def across(x):
    pairs = [(i, i + 1) for i in range(1, 127, 2)]
    return lax.ppermute(x, FLOW, pairs + [(b, a) for a, b in pairs])


def body(forcing, viscosity, friction, rotation, vertical, ice_mask, grounded):
    names = ("f", "v", "nu", "fric", "rot", "ice", "ground")
    arrays = (forcing, vertical, viscosity, friction, rotation, ice_mask, grounded)
    ins = {
        n: pltpu.with_memory_space_constraint(tiled(x), pltpu.HBM) for n, x in zip(names, arrays)
    }
    raws = {n + "raw": pltpu.VMEM(x.shape, x.dtype) for n, x in ins.items()}

    def factors(rows):
        return {"er": vmem(L, rows), "ei": vmem(L, rows), "link": vmem(L - 1, rows)}

    def pick(src, tag, *keys):
        return {k + tag: src[k] for k in keys}

    edge = vmem(PLANES, REACH)
    rows_b, rows_m = ROWS - BAND, BAND - HALF
    k0 = call(
        load_kernel,
        ins,
        {
            **factors(rows_b),
            "nuh": vmem(1, rows_b),
            "s0": vmem(PLANES, rows_b),
            "p1": vmem(COEFS + L + 2, REACH),
            **raws,
        },
        {"sems": pltpu.SemaphoreType.DMA((3, 7))},
        in_specs=HB,
    )
    p1 = across(k0["p1"])
    raw = pick(k0, "", *raws)
    ahead = call(
        ahead_kernel,
        {**pick(k0, "_b", "s0", "nuh", "er", "ei", "link"), **raw},
        {
            **factors(rows_m),
            "nuh": vmem(1, rows_m),
            "s0": vmem(PLANES, rows_m),
            "u1": edge,
            "s1": edge,
            "p2": edge,
        },
    )
    p2 = across(ahead["p2"])
    k1 = call(
        rest_kernel,
        {**raw, "order": ahead["p2"]},
        {
            **factors(HALF),
            "nuh": vmem(1, HALF),
            "s0": vmem(PLANES, HALF),
            "u0": vmem(PLANES, ROWS),
            "sa": edge,
        },
    )
    halves = {}
    for key in ("er", "ei", "link", "nuh", "s0"):
        halves[key + "_a"], halves[key + "_m"], halves[key + "_b"] = k1[key], ahead[key], k0[key]
    u0 = {"u0": k1["u0"]}

    def some(*keys):
        return {k: halves[k] for k in keys}

    operator = some("er_a", "er_m", "ei_a", "ei_m", "link_a", "link_m", "nuh_a")
    solved = {"u_edge": edge, "s": vmem(PLANES, 16), "sa": edge}
    ha = within(k1["sa"])
    n1 = call(
        inner1_kernel,
        some("s0_a", "s0_m", "s0_b", "nuh_a", "nuh_m"),
        {"nsum": edge, "u1": vmem(PLANES, HALF)},
    )
    e1 = call(edge_a_kernel, {"ha": ha, "nsum": n1["nsum"], "u_in": n1["u1"], **operator}, solved)
    ha = within(e1["sa"])
    first = {"u1_e": e1["u_edge"], "u1_i": n1["u1"]}
    middle = {"u1_m": ahead["u1"]}
    s1 = {"s1_a": e1["s"], "s1_m": ahead["s1"]}
    n2 = call(
        inner2_kernel,
        {**s1, **some("nuh_a", "nuh_m"), **u0, **first, **middle},
        {"nsum": edge, "u2": vmem(PLANES, HALF), "sums": vmem(10)},
    )
    e2 = call(edge_a_kernel, {"ha": ha, "nsum": n2["nsum"], "u_in": n2["u2"], **operator}, solved)
    ha = within(e2["sa"])
    second = {"u2_e": e2["u_edge"], "u2_i": n2["u2"]}
    n3 = call(
        inner3_kernel,
        {"s2": e2["s"], **some("nuh_a"), **u0, **first, **second},
        {"nsum": edge, "u3": vmem(PLANES, 8), "sums": vmem(10)},
    )
    a3 = call(
        last_a_kernel,
        {
            "ha": ha,
            "nsum": n3["nsum"],
            **some("nuh_a"),
            **u0,
            "u1_e": first["u1_e"],
            "u2_e": second["u2_e"],
        },
        {"u3": edge, "sums": vmem(10)},
    )
    b1 = call(
        band_kernel,
        {
            "p1": p1,
            **some("er_b", "ei_b", "link_b", "nuh_m", "nuh_b", "s0_b"),
            **u0,
            "u1_i": n1["u1"],
            **middle,
            **s1,
            "u2_i": n2["u2"],
            "s2_a": e2["s"],
            "sums2": n2["sums"],
            "sums3": n3["sums"],
            "sums4": a3["sums"],
        },
        {
            **{k + "_h": x for k, x in factors(REACH).items()},
            "u1_b": vmem(PLANES, 8),
            "s1": vmem(PLANES, 8),
            "u2": vmem(PLANES, 8),
            "nsum2": edge,
            "s2": vmem(PLANES, 8),
            "u3": vmem(PLANES, 8),
            "nsum3": edge,
            "sums": vmem(10),
        },
    )
    b2 = call(
        last_b_kernel,
        {
            "p1": p1,
            "p2": p2,
            **some("nuh_b"),
            **u0,
            **pick(b1, "", "er_h", "ei_h", "link_h", "nsum2", "nsum3", "u1_b", "sums"),
            "u2_b": b1["u2"],
        },
        {"u3": edge, "payload": jax.ShapeDtypeStruct((128, 128), F32)},
        {"s2_h": edge},
    )
    gathered = lax.all_to_all(b2["payload"], FLOW, split_axis=0, concat_axis=0, tiled=True)
    shape = (PLANES, ROWS // 8, 64, 128)
    outs = call(
        final_kernel,
        {
            "gathered": gathered,
            **some("s0_a", "s0_m", "s0_b"),
            **s1,
            "s1_b": b1["s1"],
            "s2_a": e2["s"],
            "s2_b": b1["s2"],
            **u0,
            **first,
            **middle,
            "u1_b": b1["u1_b"],
            **second,
            "u2_b": b1["u2"],
            "u3_e": a3["u3"],
            "u3_i": n3["u3"],
            "u3_b": b1["u3"],
            "u3_h": b2["u3"],
        },
        {"out_s": jax.ShapeDtypeStruct(shape, F32), "out_r": jax.ShapeDtypeStruct(shape, F32)},
        {
            "buf_s": pltpu.VMEM(shape, F32),
            "buf_r": pltpu.VMEM(shape, F32),
            "sem_s": pltpu.SemaphoreType.DMA,
            "sem_r": pltpu.SemaphoreType.DMA,
        },
        out_specs=HB,
        limit=8 << 20,
    )
    return untiled(outs["out_s"]), untiled(outs["out_r"])


def solution(mesh):
    finer = Mesh(mesh.devices.reshape(4, 4, 4, 2), FLOW)

    return jax.shard_map(
        body,
        mesh=finer,
        in_specs=(
            P(None, None, FLOW, None),
            P(FLOW, None),
            P(FLOW, None),
            P(FLOW, None),
            P(None, FLOW, None),
            P(FLOW, None),
            P(FLOW, None),
        ),
        out_specs=(P(None, None, FLOW, None), P(None, None, FLOW, None)),
        check_vma=False,
    )
```

```python
import jax
import jax.numpy as jnp
from jax import lax
from jax.experimental import pallas as pl
from jax.experimental.pallas import tpu as pltpu
from jax.sharding import Mesh
from jax.sharding import PartitionSpec as P


FLOW = ("flow_0", "flow_1", "flow_2", "flow_3")
CORE = "flow_3"
epsilon = 1e-06
TINY = 1e-37
relaxation = 0.5
reach_weights = (1.0, 0.6, 0.35, 0.2)
horiz_total = 2.0 * sum(reach_weights) + 2.0

L = 12
PLANES = 2 * L
ROWS = 24
REACH = 4
HALF = 12
BAND = 16
GROUP = 4
COEFS = 2 * PLANES
F32 = jnp.float32
TILE = (8, 128)
GRAM = [(a, b) for b in range(4) for a in range(b + 1)]

VM = pl.BlockSpec(memory_space=pltpu.VMEM)
HB = pl.BlockSpec(memory_space=pltpu.HBM)


def vmem(*lead):
    return pltpu.VMEM((*lead, *TILE), F32)


def span(start, stop):
    return list(range(start, stop))


def place_of(core, t):
    tile, sub = t // 8, t % 8
    return (
        jnp.where(core == 1, tile, 2 - tile),
        jnp.where(core == 1, sub, 7 - sub),
    )


def raw_row(ref, plane, place):
    tile, sub = place
    return ref[plane, tile, pl.ds(sub, 8, stride=8), :]


class Field:
    def __init__(self, *parts):
        self.parts = parts

    def find(self, t):
        for ref, first, index in self.parts:
            if t in index:
                return ref, first, index[t]
        raise KeyError(t)

    def row(self, plane, t):
        ref, first, i = self.find(t)
        return ref[first + plane, i]

    def get(self, plane, ts):
        return jnp.stack([self.row(plane, t) for t in ts])

    def put(self, plane, ts, value):
        for i, t in enumerate(ts):
            ref, first, j = self.find(t)
            ref[first + plane, j] = value[i]


def part(ref, start, stop, first=0):
    return (ref, first, {t: t - start for t in range(start, stop)})


def mirrored(ref, start, stop, first=0):
    return (ref, first, {ROWS - 1 - d: d - start for d in range(start, stop)})


def factor(ts, read, inv_real, inv_imag, link, nu_out):
    vert, active, nu, drag, rot = read
    imag = jnp.where(active, rot, 0.0)
    base = (relaxation + horiz_total) * nu
    if nu_out is not None:
        nu_out.put(0, ts, jnp.where(active, nu, 0.0))
    below = er = ei = None
    for k in range(L):
        real = base + (drag if k == 0 else below)
        if k < L - 1:
            above = vert(k)
            real = real + above
        real = jnp.where(active, real, 1.0)
        pivot_imag = imag
        if k > 0:
            ln = jnp.where(active, below, 0.0)
            link.put(k - 1, ts, ln)
            square = ln * ln
            real = real - square * er
            pivot_imag = imag - square * ei
        inverse = 1.0 / (real * real + pivot_imag * pivot_imag)
        er = real * inverse
        ei = -(pivot_imag * inverse)
        inv_real.put(k, ts, er)
        inv_imag.put(k, ts, ei)
        if k < L - 1:
            below = above


def solve(ts, source, inv_real, inv_imag, link, result, also=None):
    cf = cg = None
    for k in range(L):
        sf, sg = source(k, ts), source(L + k, ts)
        if k > 0:
            ln = link.get(k - 1, ts)
            sf = sf + ln * cf
            sg = sg + ln * cg
        er, ei = inv_real.get(k, ts), inv_imag.get(k, ts)
        cf, cg = er * sf + ei * sg, er * sg - ei * sf
        result.put(k, ts, cf)
        result.put(L + k, ts, cg)
    xf, xg = cf, cg
    for k in range(L - 1, -1, -1):
        if k < L - 1:
            ln = link.get(k, ts)
            pf, pg = ln * xf, ln * xg
            er, ei = inv_real.get(k, ts), inv_imag.get(k, ts)
            xf = result.get(k, ts) + (er * pf + ei * pg)
            xg = result.get(L + k, ts) + (er * pg - ei * pf)
            result.put(k, ts, xf)
            result.put(L + k, ts, xg)
        if also is not None:
            copy, rows = also
            for i, t in enumerate(ts):
                if t in rows:
                    copy.put(k, [t], xf[i : i + 1])
                    copy.put(L + k, [t], xg[i : i + 1])


def lanes():
    return lax.broadcasted_iota(jnp.int32, TILE, 1)


def cross_masks():
    lane = lanes()
    sub = lax.broadcasted_iota(jnp.int32, TILE, 0)
    first, last = lane == 0, lane == 127
    return first, last, (first & (sub == 0)) | (last & (sub == 7))


def cross(s, masks):
    first, last, ends = masks
    inside = jnp.where(ends, 0.0, s)
    up = jnp.where(first, pltpu.roll(inside, 7, 0), s)
    down = jnp.where(last, pltpu.roll(inside, 1, 0), s)
    return pltpu.roll(up, 127, 1) + pltpu.roll(down, 1, 1)


def stencil(ts, known, s, masks):
    for t in ts:
        total = cross(s[t], masks)
        for m in range(1, REACH + 1):
            near = [s[q] for q in (t - m, t + m) if q in known]
            if near:
                both = near[0] + near[1] if len(near) == 2 else near[0]
                weight = reach_weights[m - 1]
                total = total + (both if weight == 1.0 else weight * both)
        yield t, total


def halo_sum(total, distance, halo):
    for q in range(1, REACH + 1 - distance):
        weight = reach_weights[distance + q - 1]
        value = halo(q - 1)
        total = total + (value if weight == 1.0 else weight * value)
    return total


def over_planes(step, together=GROUP):
    def run(group, carry):
        for i in range(together):
            step(group * together + i)
        return carry

    lax.fori_loop(0, PLANES // together, run, 0)


def loop_sums(pairs, step, together=GROUP):
    pairs = list(pairs)

    def run(group, carry):
        sums = dict(zip(pairs, carry))

        def add(pair, value):
            sums[pair] = sums[pair] + value

        for i in range(together):
            step(group * together + i, add)
        return tuple(sums[pair] for pair in pairs)

    zero = jnp.zeros(TILE, F32)
    return dict(zip(pairs, lax.fori_loop(0, PLANES // together, run, (zero,) * len(pairs))))


def with_all(add, b, value, plane, t, us):
    for a in range(b):
        add((a, b), value * us[a].row(plane, t))
    add((b, b), value * value)


def pairs_of(*bs):
    return [(a, b) for a, b in GRAM if b in bs]


def raw_reader(r, core, ts):
    places = [place_of(core, t) for t in ts]

    def rows(ref, plane):
        return jnp.stack([raw_row(ref, plane, place) for place in places])

    active = rows(r.iceraw, 0) > 0
    drag = jnp.where(rows(r.groundraw, 0) > 0, rows(r.fricraw, 0), 0.0)
    return (
        lambda k: rows(r.vraw, k),
        active,
        rows(r.nuraw, 0),
        drag,
        rows(r.rotraw, 0),
    )


def raw_source(fraw, core):
    return lambda plane, ts: jnp.stack([raw_row(fraw, plane, place_of(core, t)) for t in ts])


def load_kernel(r):
    core = lax.axis_index(CORE)
    edge = jnp.where(core == 1, 2, 0)
    names = ("f", "v", "nu", "fric", "rot", "ice", "ground")
    copies = {}
    for i, tile in enumerate((edge, 1, 2 - edge)):
        for j, n in enumerate(names):
            copies[n, i] = pltpu.make_async_copy(
                getattr(r, n).at[:, tile], getattr(r, n + "raw").at[:, tile], r.sems.at[i, j]
            )
            copies[n, i].start()
    for n in names:
        copies[n, 0].wait()
    er, ei, link, nu = (Field(part(x, BAND, ROWS)) for x in (r.er, r.ei, r.link, r.nuh))
    packed = Field(mirrored(r.p1, 0, REACH), mirrored(r.p1, REACH, 2 * REACH, PLANES))
    ts = span(BAND, ROWS)
    read = raw_reader(r, core, ts)
    factor(ts, read, er, ei, link, nu)
    vert, active, nu_row, drag, rot = read
    for i, t in enumerate(ts):
        if t >= ROWS - REACH:
            for k in range(L - 1):
                packed.put(COEFS + k, [t], vert(k)[i : i + 1])
            packed.put(COEFS + L - 1, [t], jnp.where(active, nu_row, 0.0)[i : i + 1])
            packed.put(COEFS + L, [t], drag[i : i + 1])
            packed.put(COEFS + L + 1, [t], rot[i : i + 1])
    solve(ts, raw_source(r.fraw, core), er, ei, link, Field(part(r.s0, BAND, ROWS)), (packed, ts))
    for i in (1, 2):
        for n in names:
            copies[n, i].wait()


def ahead_kernel(r):
    core = lax.axis_index(CORE)
    masks = cross_masks()
    middle = span(HALF, BAND)
    er_m, ei_m, link_m, nu_m = (part(x, HALF, BAND) for x in (r.er, r.ei, r.link, r.nuh))
    s0_m = part(r.s0, HALF, BAND)
    solver = (Field(er_m), Field(ei_m), Field(link_m))
    factor(middle, raw_reader(r, core, middle), *solver, Field(nu_m))
    solve(middle, raw_source(r.fraw, core), *solver, Field(s0_m))
    s0 = Field(s0_m, part(r.s0_b, BAND, ROWS))
    nu = Field(part(r.nuh_b, BAND, ROWS))
    known = span(HALF, ROWS)
    ts = span(16, 20)
    u1 = Field(part(r.u1, 16, 20))

    def step(plane):
        s = {t: s0.row(plane, t) for t in known}
        for t, total in stencil(ts, known, s, masks):
            u1.put(plane, [t], (nu.row(0, t) * total)[None])

    over_planes(step, 8)
    solver = tuple(Field(part(x, BAND, ROWS)) for x in (r.er_b, r.ei_b, r.link_b))
    packed = Field(mirrored(r.p2, REACH, 2 * REACH))
    solve(ts, u1.get, *solver, Field(part(r.s1, 16, 20)), (packed, ts))


def rest_kernel(r):
    core = lax.axis_index(CORE)
    er, ei, link, nu = (Field(part(x, 0, HALF)) for x in (r.er, r.ei, r.link, r.nuh))
    for start in (0, 6):
        ts = span(start, start + 6)
        factor(ts, raw_reader(r, core, ts), er, ei, link, nu)
    places = [place_of(core, t) for t in range(ROWS)]

    def spread(plane):
        for t in range(ROWS):
            r.u0[plane, t] = raw_row(r.fraw, plane, places[t])

    over_planes(spread, 2)
    u0 = Field(part(r.u0, 0, ROWS))
    s0 = Field(part(r.s0, 0, HALF))
    for start in (0, 6):
        solve(span(start, start + 6), u0.get, er, ei, link, s0, (Field(part(r.sa, 0, REACH)), span(0, REACH)))


def both_halves(r, name):
    starts = (("_a", 0, HALF), ("_m", HALF, BAND), ("_b", BAND, ROWS))
    return Field(*(part(getattr(r, name + tag), a, b) for tag, a, b in starts if hasattr(r, name + tag)))


def inner1_kernel(r):
    masks = cross_masks()
    s0, nu = both_halves(r, "s0"), both_halves(r, "nuh")
    known = span(0, 20)

    def step(plane):
        s = {t: s0.row(plane, t) for t in known}
        for t, total in stencil(span(0, 16), known, s, masks):
            if t < REACH:
                r.nsum[plane, t] = total
            else:
                r.u1[plane, t - REACH] = nu.row(0, t) * total

    over_planes(step)


def edge_a_kernel(r):
    nu = Field(part(r.nuh_a, 0, HALF))
    er, ei, link = (both_halves(r, n) for n in ("er", "ei", "link"))
    edge = Field(part(r.u_edge, 0, REACH))
    inner = Field(part(r.u_in, REACH, 16))

    def source(plane, ts):
        rows = []
        for t in ts:
            if t < REACH:
                value = halo_sum(r.nsum[plane, t], t, lambda q: r.ha[plane, q])
                value = nu.row(0, t) * value
                edge.put(plane, [t], value[None])
            else:
                value = inner.row(plane, t)
            rows.append(value)
        return jnp.stack(rows)

    result = Field(part(r.s, 0, 16))
    sa = Field(part(r.sa, 0, REACH))
    for start in (0, 8):
        solve(span(start, start + 8), source, er, ei, link, result, (sa, span(0, REACH)))


def write_sums(ref, sums):
    zero = jnp.zeros(TILE, F32)
    for i, pair in enumerate(GRAM):
        ref[i] = sums.get(pair, zero)


def inner2_kernel(r):
    masks = cross_masks()
    s1 = Field(part(r.s1_a, 0, 16), part(r.s1_m, 16, 20))
    nu = both_halves(r, "nuh")
    u0 = Field(part(r.u0, 0, ROWS))
    u1 = Field(part(r.u1_e, 0, REACH), part(r.u1_i, REACH, 16), part(r.u1_m, 16, 20))
    known = span(0, 20)

    def step(plane, add):
        s = {t: s1.row(plane, t) for t in known}
        for t, total in stencil(span(0, 16), known, s, masks):
            if t < REACH:
                r.nsum[plane, t] = total
            else:
                value = nu.row(0, t) * total
                r.u2[plane, t - REACH] = value
                with_all(add, 2, value, plane, t, (u0, u1))
        for t in span(0, ROWS):
            value = u0.row(plane, t)
            add((0, 0), value * value)
            if t < 20:
                with_all(add, 1, u1.row(plane, t), plane, t, (u0,))

    write_sums(r.sums, loop_sums(pairs_of(0, 1, 2), step))


def inner3_kernel(r):
    masks = cross_masks()
    s2 = Field(part(r.s2, 0, 16))
    nu = Field(part(r.nuh_a, 0, HALF))
    u0 = Field(part(r.u0, 0, ROWS))
    u1 = Field(part(r.u1_e, 0, REACH), part(r.u1_i, REACH, 16))
    u2 = Field(part(r.u2_e, 0, REACH), part(r.u2_i, REACH, 16))
    known = span(0, 16)

    def step(plane, add):
        s = {t: s2.row(plane, t) for t in known}
        for t, total in stencil(span(0, HALF), known, s, masks):
            if t < REACH:
                r.nsum[plane, t] = total
                with_all(add, 2, u2.row(plane, t), plane, t, (u0, u1))
            else:
                value = nu.row(0, t) * total
                r.u3[plane, t - REACH] = value
                with_all(add, 3, value, plane, t, (u0, u1, u2))

    write_sums(r.sums, loop_sums(pairs_of(2, 3), step))


def last_a_kernel(r):
    nu = Field(part(r.nuh_a, 0, HALF))
    u0 = Field(part(r.u0, 0, ROWS))
    u1 = Field(part(r.u1_e, 0, REACH))
    u2 = Field(part(r.u2_e, 0, REACH))

    def step(plane, add):
        for t in range(REACH):
            value = halo_sum(r.nsum[plane, t], t, lambda q: r.ha[plane, q])
            value = nu.row(0, t) * value
            r.u3[plane, t] = value
            with_all(add, 3, value, plane, t, (u0, u1, u2))

    write_sums(r.sums, loop_sums(pairs_of(3), step))


def band_kernel(r):
    masks = cross_masks()
    beyond = span(ROWS, ROWS + REACH)
    nu_own = both_halves(r, "nuh")
    nu = Field(part(r.nuh_b, BAND, ROWS), part(r.p1, ROWS, ROWS + REACH, COEFS + L - 1))
    er_h, ei_h, link_h = (part(x, ROWS, ROWS + REACH) for x in (r.er_h, r.ei_h, r.link_h))
    nu_h = r.p1[COEFS + L - 1]
    read = (
        lambda k: r.p1[COEFS + k],
        nu_h > 0.0,
        nu_h,
        r.p1[COEFS + L],
        r.p1[COEFS + L + 1],
    )
    factor(beyond, read, Field(er_h), Field(ei_h), Field(link_h), None)
    er = Field(part(r.er_b, BAND, ROWS), er_h)
    ei = Field(part(r.ei_b, BAND, ROWS), ei_h)
    link = Field(part(r.link_b, BAND, ROWS), link_h)
    s0 = Field(
        part(r.s0_b, BAND, ROWS), part(r.p1, 24, 28), part(r.p1, 28, 32, PLANES)
    )
    u1_b = part(r.u1_b, 20, 28)
    known1 = span(16, 32)

    def first(plane):
        s = {t: s0.row(plane, t) for t in known1}
        for t, total in stencil(span(20, 28), known1, s, masks):
            r.u1_b[plane, t - 20] = nu.row(0, t) * total

    over_planes(first)
    s1_b = part(r.s1, 20, 28)
    solve(span(20, 28), Field(u1_b).get, er, ei, link, Field(s1_b))
    s1 = Field(part(r.s1_a, 0, 16), part(r.s1_m, 16, 20), s1_b)
    u1 = Field(part(r.u1_i, REACH, 16), part(r.u1_m, 16, 20), u1_b)
    u0 = Field(part(r.u0, 0, ROWS))
    u2_b = part(r.u2, 16, 24)
    known2 = span(12, 28)

    def second(plane, add):
        s = {t: s1.row(plane, t) for t in known2}
        for t, total in stencil(span(16, 28), known2, s, masks):
            if t < ROWS:
                value = nu.row(0, t) * total
                r.u2[plane, t - 16] = value
                with_all(add, 2, value, plane, t, (u0, u1))
            else:
                r.nsum2[plane, t - ROWS] = total
        for t in span(20, ROWS):
            with_all(add, 1, u1.row(plane, t), plane, t, (u0,))

    sums = loop_sums(pairs_of(1, 2), second)
    s2_b = part(r.s2, 16, 24)
    solve(span(16, 24), Field(u2_b).get, er, ei, link, Field(s2_b))
    s2 = Field(part(r.s2_a, 0, 16), s2_b)
    u2 = Field(part(r.u2_i, REACH, 16), u2_b)
    known3 = span(8, 24)

    def third(plane, add):
        s = {t: s2.row(plane, t) for t in known3}
        for t, total in stencil(span(12, 24), known3, s, masks):
            if t < 20:
                value = nu_own.row(0, t) * total
                r.u3[plane, t - 12] = value
                with_all(add, 3, value, plane, t, (u0, u1, u2))
            else:
                r.nsum3[plane, t - 20] = total

    sums.update(loop_sums(pairs_of(3), third))
    zero = jnp.zeros(TILE, F32)
    for i, pair in enumerate(GRAM):
        r.sums[i] = r.sums2[i] + r.sums3[i] + r.sums4[i] + sums.get(pair, zero)


def last_b_kernel(r):
    beyond = span(ROWS, ROWS + REACH)
    solver = tuple(Field(part(x, ROWS, ROWS + REACH)) for x in (r.er_h, r.ei_h, r.link_h))
    nu_b = Field(part(r.nuh_b, BAND, ROWS))

    def source(plane, ts):
        rows = []
        for j in range(REACH):
            value = r.nsum2[plane, j]
            for q in range(j + 1):
                value = value + reach_weights[REACH - 1 - j + q] * r.p2[plane, q]
            rows.append(r.p1[COEFS + L - 1, j] * value)
        return jnp.stack(rows)

    solve(beyond, source, *solver, Field(part(r.s2_h, ROWS, ROWS + REACH)))
    u0 = Field(part(r.u0, 0, ROWS))
    u1 = Field(part(r.u1_b, 20, 28))
    u2 = Field(part(r.u2_b, 16, 24))

    def step(plane, add):
        for t in span(20, ROWS):
            d = ROWS - 1 - t
            value = halo_sum(r.nsum3[plane, t - 20], d, lambda q: r.s2_h[plane, q])
            value = nu_b.row(0, t) * value
            r.u3[plane, t - 20] = value
            with_all(add, 3, value, plane, t, (u0, u1, u2))

    sums = loop_sums(pairs_of(3), step, 12)
    lane = lanes()
    out = jnp.zeros(TILE, F32)
    for i, pair in enumerate(GRAM):
        value = r.sums[i]
        if pair in sums:
            value = value + sums[pair]
        value = jnp.sum(jnp.sum(value, axis=0, keepdims=True), axis=1, keepdims=True)
        out = out + jnp.where(lane == i, value, 0.0)
    for i in range(r.payload.shape[0] // 8):
        r.payload[pl.ds(8 * i, 8), :] = out


def least_squares(columns, start):
    count_cols = len(columns)
    givens_rhs = [start] + [start * 0.0 for _ in range(count_cols)]
    cosines, sines, upper_cols = ([], [], [])
    for column_index, column_in in enumerate(columns):
        column = list(column_in)
        for row_index in range(column_index):
            rotated_a = (
                cosines[row_index] * column[row_index] + sines[row_index] * column[row_index + 1]
            )
            rotated_b = (
                -sines[row_index] * column[row_index] + cosines[row_index] * column[row_index + 1]
            )
            column[row_index] = rotated_a
            column[row_index + 1] = rotated_b
        inverse = lax.rsqrt(
            column[column_index] * column[column_index]
            + column[column_index + 1] * column[column_index + 1]
        )
        cosine = column[column_index] * inverse
        sine_value = column[column_index + 1] * inverse
        column[column_index] = inverse
        cosines.append(cosine)
        sines.append(sine_value)
        upper_cols.append(column)
        next_rhs = -sine_value * givens_rhs[column_index]
        givens_rhs[column_index] = cosine * givens_rhs[column_index]
        givens_rhs[column_index + 1] = next_rhs
    factors = [None] * count_cols
    for column_index in range(count_cols - 1, -1, -1):
        accum = givens_rhs[column_index]
        for later in range(column_index + 1, count_cols):
            accum = accum - upper_cols[later][column_index] * factors[later]
        factors[column_index] = accum * upper_cols[column_index][column_index]
    return factors


def dot(left, right):
    total = left[0] * right[0]
    for a, b in zip(left[1:], right[1:]):
        total = total + a * b
    return total


def coefficients(gram):
    size = 4
    upper = {}
    for a in range(size):
        square = gram[(a, a)]
        for p in range(a):
            square = square - upper[(p, a)] * upper[(p, a)]
        inverse = jnp.where(square > 0.0, lax.rsqrt(jnp.maximum(square, TINY)), 0.0)
        upper[(a, a)] = square * inverse
        for b in range(a + 1, size):
            value = gram[(a, b)]
            for p in range(a):
                value = value - upper[(p, a)] * upper[(p, b)]
            upper[(a, b)] = value * inverse
    square = gram[(0, 0)] + epsilon
    inverse = lax.rsqrt(square)
    beta = square * inverse
    basis = [[inverse]]
    ortho = [[upper[(0, 0)] * inverse]]
    columns = []
    for j in range(3):
        current = basis[j]
        w = [current[0]]
        for i in range(1, j + 1):
            w.append(current[i] - current[i - 1])
        w.append(-current[j])
        q = [dot([upper[(i, m)] for m in range(i, j + 2)], w[i:]) for i in range(j + 2)]
        column = []
        for i in range(j + 1):
            h = dot(q[: i + 1], ortho[i])
            for m in range(i + 1):
                q[m] = q[m] - h * ortho[i][m]
                w[m] = w[m] - h * basis[i][m]
            column.append(h)
        square = dot(q, q) + epsilon
        inverse = lax.rsqrt(square)
        column.append(square * inverse)
        columns.append(column)
        if j < 2:
            basis.append([value * inverse for value in w])
            ortho.append([value * inverse for value in q])
    y = least_squares(columns, beta)
    return [dot(y[i:], [basis[j][i] for j in range(i, 3)]) for i in range(3)]


def final_kernel(r):
    total = r.gathered[pl.ds(0, 8), :]
    for i in range(1, r.gathered.shape[0] // 8):
        total = total + r.gathered[pl.ds(8 * i, 8), :]
    total = jnp.sum(total, axis=0, keepdims=True)
    total = jnp.broadcast_to(total, TILE)
    lane = lanes()
    gram = {}
    for i, pair in enumerate(GRAM):
        value = jnp.sum(jnp.where(lane == i, total, 0.0), axis=1, keepdims=True)
        gram[pair] = jnp.broadcast_to(value, TILE)
    c0, c1, c2 = coefficients(gram)
    e0, e1, e2 = 1.0 - c0, c0 - c1, c1 - c2
    core = lax.axis_index(CORE)
    places = [place_of(core, t) for t in range(ROWS)]
    s0 = both_halves(r, "s0")
    s1 = Field(part(r.s1_a, 0, 16), part(r.s1_m, 16, 20), part(r.s1_b, 20, 28))
    s2 = Field(part(r.s2_a, 0, 16), part(r.s2_b, 16, 24))
    u0 = Field(part(r.u0, 0, ROWS))
    u1 = Field(
        part(r.u1_e, 0, 4), part(r.u1_i, 4, 16), part(r.u1_m, 16, 20), part(r.u1_b, 20, 28)
    )
    u2 = Field(part(r.u2_e, 0, 4), part(r.u2_i, 4, 16), part(r.u2_b, 16, 24))
    u3 = Field(
        part(r.u3_e, 0, 4), part(r.u3_i, 4, 12), part(r.u3_b, 12, 20), part(r.u3_h, 20, 24)
    )

    def step(plane):
        for t in range(ROWS):
            s = [x.row(plane, t) for x in (s0, s1, s2)]
            u = [x.row(plane, t) for x in (u0, u1, u2, u3)]
            tile, sub = places[t]
            r.buf_s[plane, tile, pl.ds(sub, 8, stride=8), :] = c0 * s[0] + c1 * s[1] + c2 * s[2]
            r.buf_r[plane, tile, pl.ds(sub, 8, stride=8), :] = (
                e0 * u[0] + e1 * u[1] + (e2 * u[2] + c2 * u[3])
            )
        pltpu.make_async_copy(r.buf_s.at[plane], r.out_s.at[plane], r.sem_s).start()
        pltpu.make_async_copy(r.buf_r.at[plane], r.out_r.at[plane], r.sem_r).start()

    over_planes(step, 2)
    pltpu.make_async_copy(r.buf_s, r.out_s, r.sem_s).wait()
    pltpu.make_async_copy(r.buf_r, r.out_r, r.sem_r).wait()


def tiled(x):
    x = x.reshape(-1, ROWS // 8, 8, 8, 128)
    return x.transpose(0, 1, 3, 2, 4).reshape(-1, ROWS // 8, 64, 128)


def untiled(x):
    x = x.reshape(PLANES, ROWS // 8, 8, 8, 128).transpose(0, 1, 3, 2, 4)
    return x.reshape(2, L, ROWS, 1024)


class Refs:
    def __init__(self, names, refs):
        self.__dict__.update(zip(names, refs))


def call(kernel, ins, outs, scratch={}, in_specs=None, out_specs=None, limit=4 << 20):
    names = [*ins, *outs, *scratch]

    def run(*refs):
        kernel(Refs(names, refs))

    results = pl.pallas_call(
        run,
        out_shape=list(outs.values()),
        in_specs=[in_specs or VM] * len(ins),
        out_specs=[out_specs or VM] * len(outs),
        scratch_shapes=list(scratch.values()),
        compiler_params=pltpu.CompilerParams(vmem_limit_bytes=limit),
    )(*ins.values())
    return dict(zip(outs, results))


def within(x):
    return lax.ppermute(x, FLOW, [(i, i ^ 1) for i in range(128)])


def across(x):
    pairs = [(i, i + 1) for i in range(1, 127, 2)]
    return lax.ppermute(x, FLOW, pairs + [(b, a) for a, b in pairs])


def body(forcing, viscosity, friction, rotation, vertical, ice_mask, grounded):
    names = ("f", "v", "nu", "fric", "rot", "ice", "ground")
    arrays = (forcing, vertical, viscosity, friction, rotation, ice_mask, grounded)
    ins = {
        n: pltpu.with_memory_space_constraint(tiled(x), pltpu.HBM) for n, x in zip(names, arrays)
    }
    raws = {n + "raw": pltpu.VMEM(x.shape, x.dtype) for n, x in ins.items()}

    def factors(rows):
        return {"er": vmem(L, rows), "ei": vmem(L, rows), "link": vmem(L - 1, rows)}

    def pick(src, tag, *keys):
        return {k + tag: src[k] for k in keys}

    edge = vmem(PLANES, REACH)
    rows_b, rows_m = ROWS - BAND, BAND - HALF
    k0 = call(
        load_kernel,
        ins,
        {
            **factors(rows_b),
            "nuh": vmem(1, rows_b),
            "s0": vmem(PLANES, rows_b),
            "p1": vmem(COEFS + L + 2, REACH),
            **raws,
        },
        {"sems": pltpu.SemaphoreType.DMA((3, 7))},
        in_specs=HB,
    )
    p1 = across(k0["p1"])
    raw = pick(k0, "", *raws)
    ahead = call(
        ahead_kernel,
        {**pick(k0, "_b", "s0", "nuh", "er", "ei", "link"), **raw},
        {
            **factors(rows_m),
            "nuh": vmem(1, rows_m),
            "s0": vmem(PLANES, rows_m),
            "u1": edge,
            "s1": edge,
            "p2": edge,
        },
    )
    p2 = across(ahead["p2"])
    k1 = call(
        rest_kernel,
        {**raw, "order": ahead["p2"]},
        {
            **factors(HALF),
            "nuh": vmem(1, HALF),
            "s0": vmem(PLANES, HALF),
            "u0": vmem(PLANES, ROWS),
            "sa": edge,
        },
    )
    halves = {}
    for key in ("er", "ei", "link", "nuh", "s0"):
        halves[key + "_a"], halves[key + "_m"], halves[key + "_b"] = k1[key], ahead[key], k0[key]
    u0 = {"u0": k1["u0"]}

    def some(*keys):
        return {k: halves[k] for k in keys}

    operator = some("er_a", "er_m", "ei_a", "ei_m", "link_a", "link_m", "nuh_a")
    solved = {"u_edge": edge, "s": vmem(PLANES, 16), "sa": edge}
    ha = within(k1["sa"])
    n1 = call(
        inner1_kernel,
        some("s0_a", "s0_m", "s0_b", "nuh_a", "nuh_m"),
        {"nsum": edge, "u1": vmem(PLANES, HALF)},
    )
    e1 = call(edge_a_kernel, {"ha": ha, "nsum": n1["nsum"], "u_in": n1["u1"], **operator}, solved)
    ha = within(e1["sa"])
    first = {"u1_e": e1["u_edge"], "u1_i": n1["u1"]}
    middle = {"u1_m": ahead["u1"]}
    s1 = {"s1_a": e1["s"], "s1_m": ahead["s1"]}
    n2 = call(
        inner2_kernel,
        {**s1, **some("nuh_a", "nuh_m"), **u0, **first, **middle},
        {"nsum": edge, "u2": vmem(PLANES, HALF), "sums": vmem(10)},
    )
    e2 = call(edge_a_kernel, {"ha": ha, "nsum": n2["nsum"], "u_in": n2["u2"], **operator}, solved)
    ha = within(e2["sa"])
    second = {"u2_e": e2["u_edge"], "u2_i": n2["u2"]}
    n3 = call(
        inner3_kernel,
        {"s2": e2["s"], **some("nuh_a"), **u0, **first, **second},
        {"nsum": edge, "u3": vmem(PLANES, 8), "sums": vmem(10)},
    )
    a3 = call(
        last_a_kernel,
        {
            "ha": ha,
            "nsum": n3["nsum"],
            **some("nuh_a"),
            **u0,
            "u1_e": first["u1_e"],
            "u2_e": second["u2_e"],
        },
        {"u3": edge, "sums": vmem(10)},
    )
    b1 = call(
        band_kernel,
        {
            "p1": p1,
            **some("er_b", "ei_b", "link_b", "nuh_m", "nuh_b", "s0_b"),
            **u0,
            "u1_i": n1["u1"],
            **middle,
            **s1,
            "u2_i": n2["u2"],
            "s2_a": e2["s"],
            "sums2": n2["sums"],
            "sums3": n3["sums"],
            "sums4": a3["sums"],
        },
        {
            **{k + "_h": x for k, x in factors(REACH).items()},
            "u1_b": vmem(PLANES, 8),
            "s1": vmem(PLANES, 8),
            "u2": vmem(PLANES, 8),
            "nsum2": edge,
            "s2": vmem(PLANES, 8),
            "u3": vmem(PLANES, 8),
            "nsum3": edge,
            "sums": vmem(10),
        },
    )
    b2 = call(
        last_b_kernel,
        {
            "p1": p1,
            "p2": p2,
            **some("nuh_b"),
            **u0,
            **pick(b1, "", "er_h", "ei_h", "link_h", "nsum2", "nsum3", "u1_b", "sums"),
            "u2_b": b1["u2"],
        },
        {"u3": edge, "payload": jax.ShapeDtypeStruct((128, 128), F32)},
        {"s2_h": edge},
    )
    gathered = lax.all_to_all(b2["payload"], FLOW, split_axis=0, concat_axis=0, tiled=True)
    shape = (PLANES, ROWS // 8, 64, 128)
    outs = call(
        final_kernel,
        {
            "gathered": gathered,
            **some("s0_a", "s0_m", "s0_b"),
            **s1,
            "s1_b": b1["s1"],
            "s2_a": e2["s"],
            "s2_b": b1["s2"],
            **u0,
            **first,
            **middle,
            "u1_b": b1["u1_b"],
            **second,
            "u2_b": b1["u2"],
            "u3_e": a3["u3"],
            "u3_i": n3["u3"],
            "u3_b": b1["u3"],
            "u3_h": b2["u3"],
        },
        {"out_s": jax.ShapeDtypeStruct(shape, F32), "out_r": jax.ShapeDtypeStruct(shape, F32)},
        {
            "buf_s": pltpu.VMEM(shape, F32),
            "buf_r": pltpu.VMEM(shape, F32),
            "sem_s": pltpu.SemaphoreType.DMA,
            "sem_r": pltpu.SemaphoreType.DMA,
        },
        out_specs=HB,
        limit=8 << 20,
    )
    return untiled(outs["out_s"]), untiled(outs["out_r"])


def solution(mesh):
    finer = Mesh(mesh.devices.reshape(4, 4, 4, 2), FLOW)

    return jax.shard_map(
        body,
        mesh=finer,
        in_specs=(
            P(None, None, FLOW, None),
            P(FLOW, None),
            P(FLOW, None),
            P(FLOW, None),
            P(None, FLOW, None),
            P(FLOW, None),
            P(FLOW, None),
        ),
        out_specs=(P(None, None, FLOW, None), P(None, None, FLOW, None)),
        check_vma=False,
    )
```

```python
import jax
import jax.numpy as jnp
from jax import lax
from jax.experimental import pallas as pl
from jax.experimental.pallas import tpu as pltpu
from jax.sharding import Mesh
from jax.sharding import PartitionSpec as P


FLOW = ("flow_0", "flow_1", "flow_2", "flow_3")
CORE = "flow_3"
epsilon = 1e-06
TINY = 1e-37
relaxation = 0.5
reach_weights = (1.0, 0.6, 0.35, 0.2)
horiz_total = 2.0 * sum(reach_weights) + 2.0

L = 12
PLANES = 2 * L
ROWS = 24
REACH = 4
HALF = 12
BAND = 16
GROUP = 4
COEFS = 2 * PLANES
F32 = jnp.float32
TILE = (8, 128)
GRAM = [(a, b) for b in range(4) for a in range(b + 1)]

VM = pl.BlockSpec(memory_space=pltpu.VMEM)
HB = pl.BlockSpec(memory_space=pltpu.HBM)


def vmem(*lead):
    return pltpu.VMEM((*lead, *TILE), F32)


def span(start, stop):
    return list(range(start, stop))


def place_of(core, t):
    tile, sub = t // 8, t % 8
    return (
        jnp.where(core == 1, tile, 2 - tile),
        jnp.where(core == 1, sub, 7 - sub),
    )


def raw_row(ref, plane, place):
    tile, sub = place
    return ref[plane, tile, pl.ds(sub, 8, stride=8), :]


class Field:
    def __init__(self, *parts):
        self.parts = parts

    def find(self, t):
        for ref, first, index in self.parts:
            if t in index:
                return ref, first, index[t]
        raise KeyError(t)

    def row(self, plane, t):
        ref, first, i = self.find(t)
        return ref[first + plane, i]

    def get(self, plane, ts):
        return jnp.stack([self.row(plane, t) for t in ts])

    def put(self, plane, ts, value):
        for i, t in enumerate(ts):
            ref, first, j = self.find(t)
            ref[first + plane, j] = value[i]


def part(ref, start, stop, first=0):
    return (ref, first, {t: t - start for t in range(start, stop)})


def mirrored(ref, start, stop, first=0):
    return (ref, first, {ROWS - 1 - d: d - start for d in range(start, stop)})


def factor(ts, read, inv_real, inv_imag, link, nu_out):
    vert, active, nu, drag, rot = read
    imag = jnp.where(active, rot, 0.0)
    base = (relaxation + horiz_total) * nu
    if nu_out is not None:
        nu_out.put(0, ts, jnp.where(active, nu, 0.0))
    below = er = ei = None
    for k in range(L):
        real = base + (drag if k == 0 else below)
        if k < L - 1:
            above = vert(k)
            real = real + above
        real = jnp.where(active, real, 1.0)
        pivot_imag = imag
        if k > 0:
            ln = jnp.where(active, below, 0.0)
            link.put(k - 1, ts, ln)
            square = ln * ln
            real = real - square * er
            pivot_imag = imag - square * ei
        inverse = 1.0 / (real * real + pivot_imag * pivot_imag)
        er = real * inverse
        ei = -(pivot_imag * inverse)
        inv_real.put(k, ts, er)
        inv_imag.put(k, ts, ei)
        if k < L - 1:
            below = above


def solve(ts, source, inv_real, inv_imag, link, result, also=None):
    cf = cg = None
    for k in range(L):
        sf, sg = source(k, ts), source(L + k, ts)
        if k > 0:
            ln = link.get(k - 1, ts)
            sf = sf + ln * cf
            sg = sg + ln * cg
        er, ei = inv_real.get(k, ts), inv_imag.get(k, ts)
        cf, cg = er * sf + ei * sg, er * sg - ei * sf
        result.put(k, ts, cf)
        result.put(L + k, ts, cg)
    xf, xg = cf, cg
    for k in range(L - 1, -1, -1):
        if k < L - 1:
            ln = link.get(k, ts)
            pf, pg = ln * xf, ln * xg
            er, ei = inv_real.get(k, ts), inv_imag.get(k, ts)
            xf = result.get(k, ts) + (er * pf + ei * pg)
            xg = result.get(L + k, ts) + (er * pg - ei * pf)
            result.put(k, ts, xf)
            result.put(L + k, ts, xg)
        if also is not None:
            copy, rows = also
            for i, t in enumerate(ts):
                if t in rows:
                    copy.put(k, [t], xf[i : i + 1])
                    copy.put(L + k, [t], xg[i : i + 1])


def lanes():
    return lax.broadcasted_iota(jnp.int32, TILE, 1)


def cross_masks():
    lane = lanes()
    sub = lax.broadcasted_iota(jnp.int32, TILE, 0)
    first, last = lane == 0, lane == 127
    return first, last, (first & (sub == 0)) | (last & (sub == 7))


def cross(s, masks):
    first, last, ends = masks
    inside = jnp.where(ends, 0.0, s)
    up = jnp.where(first, pltpu.roll(inside, 7, 0), s)
    down = jnp.where(last, pltpu.roll(inside, 1, 0), s)
    return pltpu.roll(up, 127, 1) + pltpu.roll(down, 1, 1)


def stencil(ts, known, s, masks):
    for t in ts:
        total = cross(s[t], masks)
        for m in range(1, REACH + 1):
            near = [s[q] for q in (t - m, t + m) if q in known]
            if near:
                both = near[0] + near[1] if len(near) == 2 else near[0]
                weight = reach_weights[m - 1]
                total = total + (both if weight == 1.0 else weight * both)
        yield t, total


def halo_sum(total, distance, halo):
    for q in range(1, REACH + 1 - distance):
        weight = reach_weights[distance + q - 1]
        value = halo(q - 1)
        total = total + (value if weight == 1.0 else weight * value)
    return total


def over_planes(step, together=GROUP):
    def run(group, carry):
        for i in range(together):
            step(group * together + i)
        return carry

    lax.fori_loop(0, PLANES // together, run, 0)


def loop_sums(pairs, step, together=GROUP):
    pairs = list(pairs)

    def run(group, carry):
        sums = dict(zip(pairs, carry))

        def add(pair, value):
            sums[pair] = sums[pair] + value

        for i in range(together):
            step(group * together + i, add)
        return tuple(sums[pair] for pair in pairs)

    zero = jnp.zeros(TILE, F32)
    return dict(zip(pairs, lax.fori_loop(0, PLANES // together, run, (zero,) * len(pairs))))


def with_all(add, b, value, plane, t, us):
    for a in range(b):
        add((a, b), value * us[a].row(plane, t))
    add((b, b), value * value)


def pairs_of(*bs):
    return [(a, b) for a, b in GRAM if b in bs]


def raw_reader(r, core, ts):
    places = [place_of(core, t) for t in ts]

    def rows(ref, plane):
        return jnp.stack([raw_row(ref, plane, place) for place in places])

    active = rows(r.iceraw, 0) > 0
    drag = jnp.where(rows(r.groundraw, 0) > 0, rows(r.fricraw, 0), 0.0)
    return (
        lambda k: rows(r.vraw, k),
        active,
        rows(r.nuraw, 0),
        drag,
        rows(r.rotraw, 0),
    )


def raw_source(fraw, core):
    return lambda plane, ts: jnp.stack([raw_row(fraw, plane, place_of(core, t)) for t in ts])


def load_kernel(r):
    core = lax.axis_index(CORE)
    edge = jnp.where(core == 1, 2, 0)
    names = ("f", "v", "nu", "fric", "rot", "ice", "ground")
    copies = {}
    for i, tile in enumerate((edge, 1, 2 - edge)):
        for j, n in enumerate(names):
            copies[n, i] = pltpu.make_async_copy(
                getattr(r, n).at[:, tile], getattr(r, n + "raw").at[:, tile], r.sems.at[i, j]
            )
            copies[n, i].start()
    for n in names:
        copies[n, 0].wait()
    er, ei, link, nu = (Field(part(x, BAND, ROWS)) for x in (r.er, r.ei, r.link, r.nuh))
    packed = Field(mirrored(r.p1, 0, REACH), mirrored(r.p1, REACH, 2 * REACH, PLANES))
    ts = span(BAND, ROWS)
    read = raw_reader(r, core, ts)
    factor(ts, read, er, ei, link, nu)
    vert, active, nu_row, drag, rot = read
    for i, t in enumerate(ts):
        if t >= ROWS - REACH:
            for k in range(L - 1):
                packed.put(COEFS + k, [t], vert(k)[i : i + 1])
            packed.put(COEFS + L - 1, [t], jnp.where(active, nu_row, 0.0)[i : i + 1])
            packed.put(COEFS + L, [t], drag[i : i + 1])
            packed.put(COEFS + L + 1, [t], rot[i : i + 1])
    solve(ts, raw_source(r.fraw, core), er, ei, link, Field(part(r.s0, BAND, ROWS)), (packed, ts))
    for i in (1, 2):
        for n in names:
            copies[n, i].wait()


def ahead_kernel(r):
    core = lax.axis_index(CORE)
    masks = cross_masks()
    middle = span(HALF, BAND)
    er_m, ei_m, link_m, nu_m = (part(x, HALF, BAND) for x in (r.er, r.ei, r.link, r.nuh))
    s0_m = part(r.s0, HALF, BAND)
    solver = (Field(er_m), Field(ei_m), Field(link_m))
    factor(middle, raw_reader(r, core, middle), *solver, Field(nu_m))
    solve(middle, raw_source(r.fraw, core), *solver, Field(s0_m))
    s0 = Field(s0_m, part(r.s0_b, BAND, ROWS))
    nu = Field(part(r.nuh_b, BAND, ROWS))
    known = span(HALF, ROWS)
    ts = span(16, 20)
    u1 = Field(part(r.u1, 16, 20))

    def step(plane):
        s = {t: s0.row(plane, t) for t in known}
        for t, total in stencil(ts, known, s, masks):
            u1.put(plane, [t], (nu.row(0, t) * total)[None])

    over_planes(step, 8)
    solver = tuple(Field(part(x, BAND, ROWS)) for x in (r.er_b, r.ei_b, r.link_b))
    packed = Field(mirrored(r.p2, REACH, 2 * REACH))
    solve(ts, u1.get, *solver, Field(part(r.s1, 16, 20)), (packed, ts))


def rest_kernel(r):
    core = lax.axis_index(CORE)
    er, ei, link, nu = (Field(part(x, 0, HALF)) for x in (r.er, r.ei, r.link, r.nuh))
    for start in (0, 6):
        ts = span(start, start + 6)
        factor(ts, raw_reader(r, core, ts), er, ei, link, nu)
    places = [place_of(core, t) for t in range(ROWS)]

    def spread(plane):
        for t in range(ROWS):
            r.u0[plane, t] = raw_row(r.fraw, plane, places[t])

    over_planes(spread, 2)
    u0 = Field(part(r.u0, 0, ROWS))
    s0 = Field(part(r.s0, 0, HALF))
    for start in (0, 6):
        solve(span(start, start + 6), u0.get, er, ei, link, s0, (Field(part(r.sa, 0, REACH)), span(0, REACH)))


def both_halves(r, name):
    starts = (("_a", 0, HALF), ("_m", HALF, BAND), ("_b", BAND, ROWS))
    return Field(*(part(getattr(r, name + tag), a, b) for tag, a, b in starts if hasattr(r, name + tag)))


def inner1_kernel(r):
    masks = cross_masks()
    s0, nu = both_halves(r, "s0"), both_halves(r, "nuh")
    known = span(0, 20)

    def step(plane):
        s = {t: s0.row(plane, t) for t in known}
        for t, total in stencil(span(0, 16), known, s, masks):
            if t < REACH:
                r.nsum[plane, t] = total
            else:
                r.u1[plane, t - REACH] = nu.row(0, t) * total

    over_planes(step)


def edge_a_kernel(r):
    nu = Field(part(r.nuh_a, 0, HALF))
    er, ei, link = (both_halves(r, n) for n in ("er", "ei", "link"))
    edge = Field(part(r.u_edge, 0, REACH))
    inner = Field(part(r.u_in, REACH, 16))

    def source(plane, ts):
        rows = []
        for t in ts:
            if t < REACH:
                value = halo_sum(r.nsum[plane, t], t, lambda q: r.ha[plane, q])
                value = nu.row(0, t) * value
                edge.put(plane, [t], value[None])
            else:
                value = inner.row(plane, t)
            rows.append(value)
        return jnp.stack(rows)

    result = Field(part(r.s, 0, 16))
    sa = Field(part(r.sa, 0, REACH))
    for start in (0, 8):
        solve(span(start, start + 8), source, er, ei, link, result, (sa, span(0, REACH)))


def write_sums(ref, sums):
    zero = jnp.zeros(TILE, F32)
    for i, pair in enumerate(GRAM):
        ref[i] = sums.get(pair, zero)


def inner2_kernel(r):
    masks = cross_masks()
    s1 = Field(part(r.s1_a, 0, 16), part(r.s1_m, 16, 20))
    nu = both_halves(r, "nuh")
    u0 = Field(part(r.u0, 0, ROWS))
    u1 = Field(part(r.u1_e, 0, REACH), part(r.u1_i, REACH, 16), part(r.u1_m, 16, 20))
    known = span(0, 20)

    def step(plane, add):
        s = {t: s1.row(plane, t) for t in known}
        for t, total in stencil(span(0, 16), known, s, masks):
            if t < REACH:
                r.nsum[plane, t] = total
            else:
                value = nu.row(0, t) * total
                r.u2[plane, t - REACH] = value
                with_all(add, 2, value, plane, t, (u0, u1))
        for t in span(0, ROWS):
            value = u0.row(plane, t)
            add((0, 0), value * value)
            if t < 20:
                with_all(add, 1, u1.row(plane, t), plane, t, (u0,))

    write_sums(r.sums, loop_sums(pairs_of(0, 1, 2), step))


def inner3_kernel(r):
    masks = cross_masks()
    s2 = Field(part(r.s2, 0, 16))
    nu = Field(part(r.nuh_a, 0, HALF))
    u0 = Field(part(r.u0, 0, ROWS))
    u1 = Field(part(r.u1_e, 0, REACH), part(r.u1_i, REACH, 16))
    u2 = Field(part(r.u2_e, 0, REACH), part(r.u2_i, REACH, 16))
    known = span(0, 16)

    def step(plane, add):
        s = {t: s2.row(plane, t) for t in known}
        for t, total in stencil(span(0, HALF), known, s, masks):
            if t < REACH:
                r.nsum[plane, t] = total
                with_all(add, 2, u2.row(plane, t), plane, t, (u0, u1))
            else:
                value = nu.row(0, t) * total
                r.u3[plane, t - REACH] = value
                with_all(add, 3, value, plane, t, (u0, u1, u2))

    write_sums(r.sums, loop_sums(pairs_of(2, 3), step))


def last_a_kernel(r):
    nu = Field(part(r.nuh_a, 0, HALF))
    u0 = Field(part(r.u0, 0, ROWS))
    u1 = Field(part(r.u1_e, 0, REACH))
    u2 = Field(part(r.u2_e, 0, REACH))

    def step(plane, add):
        for t in range(REACH):
            value = halo_sum(r.nsum[plane, t], t, lambda q: r.ha[plane, q])
            value = nu.row(0, t) * value
            r.u3[plane, t] = value
            with_all(add, 3, value, plane, t, (u0, u1, u2))

    write_sums(r.sums, loop_sums(pairs_of(3), step))


def in_lane(out, i, value):
    value = jnp.sum(jnp.sum(value, axis=0, keepdims=True), axis=1, keepdims=True)
    return out + jnp.where(lanes() == i, value, 0.0)


def band_kernel(r):
    masks = cross_masks()
    beyond = span(ROWS, ROWS + REACH)
    nu_own = both_halves(r, "nuh")
    nu = Field(part(r.nuh_b, BAND, ROWS), part(r.p1, ROWS, ROWS + REACH, COEFS + L - 1))
    er_h, ei_h, link_h = (part(x, ROWS, ROWS + REACH) for x in (r.er_h, r.ei_h, r.link_h))
    nu_h = r.p1[COEFS + L - 1]
    read = (
        lambda k: r.p1[COEFS + k],
        nu_h > 0.0,
        nu_h,
        r.p1[COEFS + L],
        r.p1[COEFS + L + 1],
    )
    factor(beyond, read, Field(er_h), Field(ei_h), Field(link_h), None)
    er = Field(part(r.er_b, BAND, ROWS), er_h)
    ei = Field(part(r.ei_b, BAND, ROWS), ei_h)
    link = Field(part(r.link_b, BAND, ROWS), link_h)
    s0 = Field(
        part(r.s0_b, BAND, ROWS), part(r.p1, 24, 28), part(r.p1, 28, 32, PLANES)
    )
    u1_b = part(r.u1_b, 20, 28)
    known1 = span(16, 32)

    def first(plane):
        s = {t: s0.row(plane, t) for t in known1}
        for t, total in stencil(span(20, 28), known1, s, masks):
            r.u1_b[plane, t - 20] = nu.row(0, t) * total

    over_planes(first)
    s1_b = part(r.s1, 20, 28)
    solve(span(20, 28), Field(u1_b).get, er, ei, link, Field(s1_b))
    s1 = Field(part(r.s1_a, 0, 16), part(r.s1_m, 16, 20), s1_b)
    u1 = Field(part(r.u1_i, REACH, 16), part(r.u1_m, 16, 20), u1_b)
    u0 = Field(part(r.u0, 0, ROWS))
    u2_b = part(r.u2, 16, 24)
    known2 = span(12, 28)

    def second(plane, add):
        s = {t: s1.row(plane, t) for t in known2}
        for t, total in stencil(span(16, 28), known2, s, masks):
            if t < ROWS:
                value = nu.row(0, t) * total
                r.u2[plane, t - 16] = value
                with_all(add, 2, value, plane, t, (u0, u1))
            else:
                r.nsum2[plane, t - ROWS] = total
        for t in span(20, ROWS):
            with_all(add, 1, u1.row(plane, t), plane, t, (u0,))

    sums = loop_sums(pairs_of(1, 2), second)
    s2_b = part(r.s2, 16, 24)
    solve(span(16, 24), Field(u2_b).get, er, ei, link, Field(s2_b))
    s2 = Field(part(r.s2_a, 0, 16), s2_b)
    u2 = Field(part(r.u2_i, REACH, 16), u2_b)
    known3 = span(8, 24)

    def third(plane, add):
        s = {t: s2.row(plane, t) for t in known3}
        for t, total in stencil(span(12, 24), known3, s, masks):
            if t < 20:
                value = nu_own.row(0, t) * total
                r.u3[plane, t - 12] = value
                with_all(add, 3, value, plane, t, (u0, u1, u2))
            else:
                r.nsum3[plane, t - 20] = total

    sums.update(loop_sums(pairs_of(3), third))
    out = jnp.zeros(TILE, F32)
    for i, pair in enumerate(GRAM):
        value = r.sums2[i] + r.sums3[i] + r.sums4[i]
        if pair in sums:
            value = value + sums[pair]
        if pair[1] == 3:
            r.sums[pair[0]] = value
        else:
            out = in_lane(out, i, value)
    r.sums[4] = out


def last_b_kernel(r):
    beyond = span(ROWS, ROWS + REACH)
    solver = tuple(Field(part(x, ROWS, ROWS + REACH)) for x in (r.er_h, r.ei_h, r.link_h))
    nu_b = Field(part(r.nuh_b, BAND, ROWS))

    def source(plane, ts):
        rows = []
        for j in range(REACH):
            value = r.nsum2[plane, j]
            for q in range(j + 1):
                value = value + reach_weights[REACH - 1 - j + q] * r.p2[plane, q]
            rows.append(r.p1[COEFS + L - 1, j] * value)
        return jnp.stack(rows)

    solve(beyond, source, *solver, Field(part(r.s2_h, ROWS, ROWS + REACH)))
    u0 = Field(part(r.u0, 0, ROWS))
    u1 = Field(part(r.u1_b, 20, 28))
    u2 = Field(part(r.u2_b, 16, 24))

    def step(plane, add):
        for t in span(20, ROWS):
            d = ROWS - 1 - t
            value = halo_sum(r.nsum3[plane, t - 20], d, lambda q: r.s2_h[plane, q])
            value = nu_b.row(0, t) * value
            r.u3[plane, t - 20] = value
            with_all(add, 3, value, plane, t, (u0, u1, u2))

    sums = loop_sums(pairs_of(3), step, 6)
    out = r.sums[4]
    for i, pair in enumerate(GRAM):
        if pair[1] == 3:
            out = in_lane(out, i, r.sums[pair[0]] + sums[pair])
    for i in range(r.payload.shape[0] // 8):
        r.payload[pl.ds(8 * i, 8), :] = out


def least_squares(columns, start):
    count_cols = len(columns)
    givens_rhs = [start] + [start * 0.0 for _ in range(count_cols)]
    cosines, sines, upper_cols = ([], [], [])
    for column_index, column_in in enumerate(columns):
        column = list(column_in)
        for row_index in range(column_index):
            rotated_a = (
                cosines[row_index] * column[row_index] + sines[row_index] * column[row_index + 1]
            )
            rotated_b = (
                -sines[row_index] * column[row_index] + cosines[row_index] * column[row_index + 1]
            )
            column[row_index] = rotated_a
            column[row_index + 1] = rotated_b
        inverse = lax.rsqrt(
            column[column_index] * column[column_index]
            + column[column_index + 1] * column[column_index + 1]
        )
        cosine = column[column_index] * inverse
        sine_value = column[column_index + 1] * inverse
        column[column_index] = inverse
        cosines.append(cosine)
        sines.append(sine_value)
        upper_cols.append(column)
        next_rhs = -sine_value * givens_rhs[column_index]
        givens_rhs[column_index] = cosine * givens_rhs[column_index]
        givens_rhs[column_index + 1] = next_rhs
    factors = [None] * count_cols
    for column_index in range(count_cols - 1, -1, -1):
        accum = givens_rhs[column_index]
        for later in range(column_index + 1, count_cols):
            accum = accum - upper_cols[later][column_index] * factors[later]
        factors[column_index] = accum * upper_cols[column_index][column_index]
    return factors


def dot(left, right):
    total = left[0] * right[0]
    for a, b in zip(left[1:], right[1:]):
        total = total + a * b
    return total


def coefficients(gram):
    size = 4
    upper = {}
    for a in range(size):
        square = gram[(a, a)]
        for p in range(a):
            square = square - upper[(p, a)] * upper[(p, a)]
        inverse = jnp.where(square > 0.0, lax.rsqrt(jnp.maximum(square, TINY)), 0.0)
        upper[(a, a)] = square * inverse
        for b in range(a + 1, size):
            value = gram[(a, b)]
            for p in range(a):
                value = value - upper[(p, a)] * upper[(p, b)]
            upper[(a, b)] = value * inverse
    square = gram[(0, 0)] + epsilon
    inverse = lax.rsqrt(square)
    beta = square * inverse
    basis = [[inverse]]
    ortho = [[upper[(0, 0)] * inverse]]
    columns = []
    for j in range(3):
        current = basis[j]
        w = [current[0]]
        for i in range(1, j + 1):
            w.append(current[i] - current[i - 1])
        w.append(-current[j])
        q = [dot([upper[(i, m)] for m in range(i, j + 2)], w[i:]) for i in range(j + 2)]
        column = []
        for i in range(j + 1):
            h = dot(q[: i + 1], ortho[i])
            for m in range(i + 1):
                q[m] = q[m] - h * ortho[i][m]
                w[m] = w[m] - h * basis[i][m]
            column.append(h)
        square = dot(q, q) + epsilon
        inverse = lax.rsqrt(square)
        column.append(square * inverse)
        columns.append(column)
        if j < 2:
            basis.append([value * inverse for value in w])
            ortho.append([value * inverse for value in q])
    y = least_squares(columns, beta)
    return [dot(y[i:], [basis[j][i] for j in range(i, 3)]) for i in range(3)]


def final_kernel(r):
    total = r.gathered[pl.ds(0, 8), :]
    for i in range(1, r.gathered.shape[0] // 8):
        total = total + r.gathered[pl.ds(8 * i, 8), :]
    total = jnp.sum(total, axis=0, keepdims=True)
    total = jnp.broadcast_to(total, TILE)
    lane = lanes()
    gram = {}
    for i, pair in enumerate(GRAM):
        value = jnp.sum(jnp.where(lane == i, total, 0.0), axis=1, keepdims=True)
        gram[pair] = jnp.broadcast_to(value, TILE)
    c0, c1, c2 = coefficients(gram)
    e0, e1, e2 = 1.0 - c0, c0 - c1, c1 - c2
    core = lax.axis_index(CORE)
    places = [place_of(core, t) for t in range(ROWS)]
    s0 = both_halves(r, "s0")
    s1 = Field(part(r.s1_a, 0, 16), part(r.s1_m, 16, 20), part(r.s1_b, 20, 28))
    s2 = Field(part(r.s2_a, 0, 16), part(r.s2_b, 16, 24))
    u0 = Field(part(r.u0, 0, ROWS))
    u1 = Field(
        part(r.u1_e, 0, 4), part(r.u1_i, 4, 16), part(r.u1_m, 16, 20), part(r.u1_b, 20, 28)
    )
    u2 = Field(part(r.u2_e, 0, 4), part(r.u2_i, 4, 16), part(r.u2_b, 16, 24))
    u3 = Field(
        part(r.u3_e, 0, 4), part(r.u3_i, 4, 12), part(r.u3_b, 12, 20), part(r.u3_h, 20, 24)
    )

    def step(plane):
        for t in range(ROWS):
            s = [x.row(plane, t) for x in (s0, s1, s2)]
            u = [x.row(plane, t) for x in (u0, u1, u2, u3)]
            tile, sub = places[t]
            r.buf_s[plane, tile, pl.ds(sub, 8, stride=8), :] = c0 * s[0] + c1 * s[1] + c2 * s[2]
            r.buf_r[plane, tile, pl.ds(sub, 8, stride=8), :] = (
                e0 * u[0] + e1 * u[1] + (e2 * u[2] + c2 * u[3])
            )
        pltpu.make_async_copy(r.buf_s.at[plane], r.out_s.at[plane], r.sem_s).start()
        pltpu.make_async_copy(r.buf_r.at[plane], r.out_r.at[plane], r.sem_r).start()

    over_planes(step, 4)
    pltpu.make_async_copy(r.buf_s, r.out_s, r.sem_s).wait()
    pltpu.make_async_copy(r.buf_r, r.out_r, r.sem_r).wait()


def tiled(x):
    x = x.reshape(-1, ROWS // 8, 8, 8, 128)
    return x.transpose(0, 1, 3, 2, 4).reshape(-1, ROWS // 8, 64, 128)


def untiled(x):
    x = x.reshape(PLANES, ROWS // 8, 8, 8, 128).transpose(0, 1, 3, 2, 4)
    return x.reshape(2, L, ROWS, 1024)


class Refs:
    def __init__(self, names, refs):
        self.__dict__.update(zip(names, refs))


def call(kernel, ins, outs, scratch={}, in_specs=None, out_specs=None, limit=4 << 20):
    names = [*ins, *outs, *scratch]

    def run(*refs):
        kernel(Refs(names, refs))

    results = pl.pallas_call(
        run,
        out_shape=list(outs.values()),
        in_specs=[in_specs or VM] * len(ins),
        out_specs=[out_specs or VM] * len(outs),
        scratch_shapes=list(scratch.values()),
        compiler_params=pltpu.CompilerParams(vmem_limit_bytes=limit),
    )(*ins.values())
    return dict(zip(outs, results))


def within(x):
    return lax.ppermute(x, FLOW, [(i, i ^ 1) for i in range(128)])


def across(x):
    pairs = [(i, i + 1) for i in range(1, 127, 2)]
    return lax.ppermute(x, FLOW, pairs + [(b, a) for a, b in pairs])


def body(forcing, viscosity, friction, rotation, vertical, ice_mask, grounded):
    names = ("f", "v", "nu", "fric", "rot", "ice", "ground")
    arrays = (forcing, vertical, viscosity, friction, rotation, ice_mask, grounded)
    ins = {
        n: pltpu.with_memory_space_constraint(tiled(x), pltpu.HBM) for n, x in zip(names, arrays)
    }
    raws = {n + "raw": pltpu.VMEM(x.shape, x.dtype) for n, x in ins.items()}

    def factors(rows):
        return {"er": vmem(L, rows), "ei": vmem(L, rows), "link": vmem(L - 1, rows)}

    def pick(src, tag, *keys):
        return {k + tag: src[k] for k in keys}

    edge = vmem(PLANES, REACH)
    rows_b, rows_m = ROWS - BAND, BAND - HALF
    k0 = call(
        load_kernel,
        ins,
        {
            **factors(rows_b),
            "nuh": vmem(1, rows_b),
            "s0": vmem(PLANES, rows_b),
            "p1": vmem(COEFS + L + 2, REACH),
            **raws,
        },
        {"sems": pltpu.SemaphoreType.DMA((3, 7))},
        in_specs=HB,
    )
    p1 = across(k0["p1"])
    raw = pick(k0, "", *raws)
    ahead = call(
        ahead_kernel,
        {**pick(k0, "_b", "s0", "nuh", "er", "ei", "link"), **raw},
        {
            **factors(rows_m),
            "nuh": vmem(1, rows_m),
            "s0": vmem(PLANES, rows_m),
            "u1": edge,
            "s1": edge,
            "p2": edge,
        },
    )
    p2 = across(ahead["p2"])
    k1 = call(
        rest_kernel,
        {**raw, "order": ahead["p2"]},
        {
            **factors(HALF),
            "nuh": vmem(1, HALF),
            "s0": vmem(PLANES, HALF),
            "u0": vmem(PLANES, ROWS),
            "sa": edge,
        },
    )
    halves = {}
    for key in ("er", "ei", "link", "nuh", "s0"):
        halves[key + "_a"], halves[key + "_m"], halves[key + "_b"] = k1[key], ahead[key], k0[key]
    u0 = {"u0": k1["u0"]}

    def some(*keys):
        return {k: halves[k] for k in keys}

    operator = some("er_a", "er_m", "ei_a", "ei_m", "link_a", "link_m", "nuh_a")
    solved = {"u_edge": edge, "s": vmem(PLANES, 16), "sa": edge}
    ha = within(k1["sa"])
    n1 = call(
        inner1_kernel,
        some("s0_a", "s0_m", "s0_b", "nuh_a", "nuh_m"),
        {"nsum": edge, "u1": vmem(PLANES, HALF)},
    )
    e1 = call(edge_a_kernel, {"ha": ha, "nsum": n1["nsum"], "u_in": n1["u1"], **operator}, solved)
    ha = within(e1["sa"])
    first = {"u1_e": e1["u_edge"], "u1_i": n1["u1"]}
    middle = {"u1_m": ahead["u1"]}
    s1 = {"s1_a": e1["s"], "s1_m": ahead["s1"]}
    n2 = call(
        inner2_kernel,
        {**s1, **some("nuh_a", "nuh_m"), **u0, **first, **middle},
        {"nsum": edge, "u2": vmem(PLANES, HALF), "sums": vmem(10)},
    )
    e2 = call(edge_a_kernel, {"ha": ha, "nsum": n2["nsum"], "u_in": n2["u2"], **operator}, solved)
    ha = within(e2["sa"])
    second = {"u2_e": e2["u_edge"], "u2_i": n2["u2"]}
    n3 = call(
        inner3_kernel,
        {"s2": e2["s"], **some("nuh_a"), **u0, **first, **second},
        {"nsum": edge, "u3": vmem(PLANES, 8), "sums": vmem(10)},
    )
    a3 = call(
        last_a_kernel,
        {
            "ha": ha,
            "nsum": n3["nsum"],
            **some("nuh_a"),
            **u0,
            "u1_e": first["u1_e"],
            "u2_e": second["u2_e"],
        },
        {"u3": edge, "sums": vmem(10)},
    )
    b1 = call(
        band_kernel,
        {
            "p1": p1,
            **some("er_b", "ei_b", "link_b", "nuh_m", "nuh_b", "s0_b"),
            **u0,
            "u1_i": n1["u1"],
            **middle,
            **s1,
            "u2_i": n2["u2"],
            "s2_a": e2["s"],
            "sums2": n2["sums"],
            "sums3": n3["sums"],
            "sums4": a3["sums"],
        },
        {
            **{k + "_h": x for k, x in factors(REACH).items()},
            "u1_b": vmem(PLANES, 8),
            "s1": vmem(PLANES, 8),
            "u2": vmem(PLANES, 8),
            "nsum2": edge,
            "s2": vmem(PLANES, 8),
            "u3": vmem(PLANES, 8),
            "nsum3": edge,
            "sums": vmem(5),
        },
    )
    b2 = call(
        last_b_kernel,
        {
            "p1": p1,
            "p2": p2,
            **some("nuh_b"),
            **u0,
            **pick(b1, "", "er_h", "ei_h", "link_h", "nsum2", "nsum3", "u1_b", "sums"),
            "u2_b": b1["u2"],
        },
        {"u3": edge, "payload": jax.ShapeDtypeStruct((128, 128), F32)},
        {"s2_h": edge},
    )
    gathered = lax.all_to_all(b2["payload"], FLOW, split_axis=0, concat_axis=0, tiled=True)
    shape = (PLANES, ROWS // 8, 64, 128)
    outs = call(
        final_kernel,
        {
            "gathered": gathered,
            **some("s0_a", "s0_m", "s0_b"),
            **s1,
            "s1_b": b1["s1"],
            "s2_a": e2["s"],
            "s2_b": b1["s2"],
            **u0,
            **first,
            **middle,
            "u1_b": b1["u1_b"],
            **second,
            "u2_b": b1["u2"],
            "u3_e": a3["u3"],
            "u3_i": n3["u3"],
            "u3_b": b1["u3"],
            "u3_h": b2["u3"],
        },
        {"out_s": jax.ShapeDtypeStruct(shape, F32), "out_r": jax.ShapeDtypeStruct(shape, F32)},
        {
            "buf_s": pltpu.VMEM(shape, F32),
            "buf_r": pltpu.VMEM(shape, F32),
            "sem_s": pltpu.SemaphoreType.DMA,
            "sem_r": pltpu.SemaphoreType.DMA,
        },
        out_specs=HB,
        limit=8 << 20,
    )
    return untiled(outs["out_s"]), untiled(outs["out_r"])


def solution(mesh):
    finer = Mesh(mesh.devices.reshape(4, 4, 4, 2), FLOW)

    return jax.shard_map(
        body,
        mesh=finer,
        in_specs=(
            P(None, None, FLOW, None),
            P(FLOW, None),
            P(FLOW, None),
            P(FLOW, None),
            P(None, FLOW, None),
            P(FLOW, None),
            P(FLOW, None),
        ),
        out_specs=(P(None, None, FLOW, None), P(None, None, FLOW, None)),
        check_vma=False,
    )
```
